256 devices in a mesh: grp: 2 (over z), tp: 128 (over x, y, core).
Axes of the slice: x: 8, y: 8, z: 2, core: 2. Of those that a mesh axis runs over, the one named last changes fastest.
The devices are a block of a 8x8x16 slice.
Arguments:
- hidden_in: float32 [64, 4608], P('grp'), parts along dimension 0, may hold values from -6 to 6
- prefill_cache: bfloat16 [128, 1, 2, 4, 128, 8, 256], P('tp', None, None, 'grp'), parts along dimension 3, may hold values from -6 to 6
- lengths: int32 [64], P('grp'), parts along dimension 0, may hold values from 1 to 1023
- page_table: int32 [64, 128], P('grp'), parts along dimension 0, may hold values from 0 to 127, each once within a row
- qkv_weight: bfloat16 [1, 8192, 4608], P(None, 'tp'), may hold values from -0.09375 to 0.09375
- out_weight: bfloat16 [1, 4608, 4096], P(None, 'tp'), may hold values from -0.09375 to 0.09375
- gate_up_weight: bfloat16 [1, 2, 18432, 4608], P(None, None, 'tp'), may hold values from -0.09375 to 0.09375
- down_weight: bfloat16 [1, 18432, 4608], P(None, 'tp'), may hold values from -0.15625 to 0.15625
- norm_gains: float32 [1, 4, 4608], replicated, may hold values from 0.25 to 1.75
Outputs:
- hidden_out: float32 [64, 4608], P('grp', 'tp'), parts along dimension 0
- decode_cache: bfloat16 [128, 1, 2, 64, 8, 2048], P('tp', None, None, 'grp'), parts along dimension 3
The draws below stay inside these ranges and needn't reach their ends.
There are 2 independent parts, one for each index of `grp`. The reference program is written for one: setup_inputs(seed, part) draws one part's arguments, and reference() takes and returns one part's arrays. A program takes and returns all parts, laid end to end along the dimension named above; an argument that names none is the same for every part. Nothing has to cross between parts.
Inputs may be any that keep to these rules, and one draw needn't show every extreme that they name: Request r's new token takes position lengths[r]. Each row is a permutation of 0 to 127; page j of request r holds cache positions page_table[r, j] * 8 to page_table[r, j] * 8 + 7.
All inputs are finite; a program needn't handle non-finite values.
Results may differ from the reference program's by a relative error of at most 0.012.
The reference program's roundings to bfloat16 on the way (of `normed`, `projected`, `attended`, `mixed`, `ffn_in` and `active`) count: a program that leaves them out, or rounds other values in their place, can miss the bound.
Values may be sent and summed in bfloat16 or wider, within the bound.
No kernel may reach another device: no remote copies, remote signals or barrier semaphores. Data moves between devices by JAX's collectives and lax.ppermute only.
A program may use at most 64 MiB of HBM per device.

```python
import jax
import jax.numpy as jnp
from jax import lax

D = 4608
HEADS = 32
KV_HEADS = 16
HEAD_DIM = 128
FF = 18432
PREFILL_TP = 8
LAYERS = 1
REQ_GROUP = 2
CTX_DEV = 8
BATCH = 32
CTX = 1024
N_TP = 128


def touch_ends(entries, rng, smallest, high):
    spot = [jax.random.randint(jax.random.fold_in(rng, axis), (), 0, length) for axis, length in enumerate(entries.shape)]
    longest = entries.shape.index(max(entries.shape))
    next_to = spot[:longest] + [(spot[longest] + 1) % entries.shape[longest]] + spot[longest + 1:]
    return entries.at[tuple(spot)].set(smallest).at[tuple(next_to)].set(high)


def with_spikes(entries, own_key, source, target, blocks, factor):
    owner, partner = [(jnp.arange(entries.shape[axis_at]) // (entries.shape[axis_at] // blocks)).reshape([-1 if axis == axis_at else 1 for axis in range(entries.ndim)]) for axis_at in (source, target)]
    chosen = jax.random.permutation(own_key, blocks)[partner]
    strong = (owner == chosen) | (owner == (partner + blocks // 2) % blocks)
    return jnp.where(strong, factor * entries, entries)


def level_of(key, dims, pieces, smallest, largest):
    gain, own = 1.0, jax.random.fold_in(key, 6)
    for position, blocks in pieces:
        draws = jnp.exp(jax.random.uniform(jax.random.fold_in(own, position), (blocks,), jnp.float32, smallest / len(pieces), largest / len(pieces)))
        gain = gain * jnp.repeat(draws, dims[position] // blocks).reshape([-1 if axis == position else 1 for axis in range(len(dims))])
    return gain


def gaussian(stream_key, shape, width, most, cuts=(), kind=jnp.bfloat16):
    loudness = level_of(stream_key, shape, cuts, -0.22, 0.18) if cuts else 1.0
    drawn = jax.random.normal(stream_key, shape, jnp.float32) * width * loudness
    return jnp.minimum(jnp.maximum(drawn, -most), most).astype(kind)


def bell_draw_with(key, shape, deviation, reach, split, heavy, kind=jnp.bfloat16):
    array = deviation * jax.random.normal(key, shape, jnp.float32)
    if split:
        array = array * level_of(key, shape, split, -0.22, 0.18)
    return jnp.clip(with_spikes(array, jax.random.fold_in(key, 3), *heavy), -reach, reach).astype(kind)


def setup_inputs(seed: int = 0, part: int = 0) -> dict:
    key_list = jax.random.split(jax.random.key(seed), 10)
    own_keys = jax.random.split(jax.random.fold_in(key_list[9], part), 10)
    hidden_in = gaussian(own_keys[0], (BATCH, D), 1.0, 6.0, (), jnp.float32)
    prefill_cache = gaussian(own_keys[1], (N_TP, LAYERS, 2, REQ_GROUP, N_TP, CTX_DEV, KV_HEADS // PREFILL_TP * HEAD_DIM), 1.0, 6.0, ((0, 128),))
    lengths = touch_ends(jax.random.randint(own_keys[2], (BATCH,), 1, CTX), jax.random.fold_in(own_keys[2], 1), 1, CTX - 1).astype(jnp.int32)
    page_table = jax.vmap(lambda own: jax.random.permutation(own, N_TP))(jax.random.split(own_keys[3], BATCH)).reshape((BATCH, N_TP)).astype(jnp.int32)
    qkv_weight = gaussian(key_list[4], (LAYERS, (HEADS + 2 * KV_HEADS) * HEAD_DIM, D), D ** -0.5, 0.09375, ((1, 128),))
    out_weight = gaussian(key_list[5], (LAYERS, D, HEADS * HEAD_DIM), (HEADS * HEAD_DIM) ** -0.5, 0.09375, ((1, 128),))
    gate_up_weight = gaussian(key_list[6], (LAYERS, 2, FF, D), D ** -0.5, 0.09375, ((2, 128),))
    down_weight = bell_draw_with(key_list[7], (LAYERS, FF, D), FF ** -0.5, 0.15625, ((1, 128),), (1, 2, 128, 5.5))
    norm_gains = jnp.clip(1.0 + 0.15 * jax.random.normal(key_list[8], (LAYERS, 4, D), jnp.float32), 0.25, 1.75)
    return dict(hidden_in=hidden_in, prefill_cache=prefill_cache, lengths=lengths, page_table=page_table, qkv_weight=qkv_weight, out_weight=out_weight, gate_up_weight=gate_up_weight, down_weight=down_weight, norm_gains=norm_gains)


EPSILON = 1e-06
SOFTCAP = 50.0

def rms_scale(vector, gain_row):
    meansq = lax.optimization_barrier(jnp.mean(vector * vector, axis=-1, keepdims=True))
    return vector * lax.rsqrt(meansq + EPSILON) * (1.0 + gain_row)

def rotate(vector, positions):
    half_dim = vector.shape[-1] // 2
    exponent = jnp.arange(half_dim, dtype=jnp.float32) * (-2.0 / vector.shape[-1])
    frequency = jnp.power(jnp.float32(10000.0), exponent)
    angles = positions.astype(jnp.float32)[:, None, None] * frequency
    cosine = jnp.cos(angles)
    sine_term = jnp.sin(angles)
    front_half = vector[..., :half_dim]
    back_half = vector[..., half_dim:]
    return jnp.concatenate([front_half * cosine - back_half * sine_term, back_half * cosine + front_half * sine_term], axis=-1)

def capped(raw_scores):
    return SOFTCAP * jnp.tanh(raw_scores / SOFTCAP)

def round_back(vector):
    return lax.optimization_barrier(vector.astype(jnp.bfloat16)).astype(jnp.float32)

def reference(hidden_in, prefill_cache, lengths, page_table, qkv_weight, out_weight, gate_up_weight, down_weight, norm_gains):
    groups = N_TP // PREFILL_TP
    local_heads = KV_HEADS // PREFILL_TP
    head_share = HEADS // KV_HEADS
    score_scale = (D / HEADS) ** (-0.5)
    q_cols = HEADS * HEAD_DIM
    k_cols = KV_HEADS * HEAD_DIM
    blocks = prefill_cache.reshape(groups, PREFILL_TP, LAYERS, 2, REQ_GROUP, N_TP, CTX_DEV, local_heads, HEAD_DIM)
    by_request = blocks.transpose(2, 3, 0, 4, 5, 6, 1, 7, 8).reshape(LAYERS, 2, BATCH, N_TP, CTX_DEV, k_cols)
    page_ids = jnp.arange(N_TP, dtype=jnp.int32)
    onehot = (page_table[:, :, None] == page_ids[None, None, :]).astype(jnp.int32)
    inverse = lax.optimization_barrier(jnp.sum(onehot * page_ids[None, :, None], axis=1)).astype(jnp.int32)
    ordered = jnp.take_along_axis(by_request, inverse[None, None, :, :, None, None], axis=3)
    positions = page_ids[:, None] * CTX_DEV + jnp.arange(CTX_DEV, dtype=jnp.int32)[None, :]
    visible = positions[None, :, :] < lengths[:, None, None]
    fresh_slot = positions[None, :, :] == lengths[:, None, None]
    stream = hidden_in
    written = []
    for layer_index in range(LAYERS):
        normed = rms_scale(stream, norm_gains[layer_index, 0]).astype(jnp.bfloat16)
        projected = jnp.dot(normed, qkv_weight[layer_index].T, preferred_element_type=jnp.float32).astype(jnp.bfloat16)
        queries = rotate(projected[:, :q_cols].astype(jnp.float32).reshape(BATCH, HEADS, HEAD_DIM), lengths).astype(jnp.bfloat16)
        new_key = rotate(projected[:, q_cols:q_cols + k_cols].astype(jnp.float32).reshape(BATCH, KV_HEADS, HEAD_DIM), lengths).astype(jnp.bfloat16)
        new_value = projected[:, q_cols + k_cols:]
        key_layer = jnp.where(fresh_slot[:, :, :, None], new_key.reshape(BATCH, 1, 1, k_cols), ordered[layer_index, 0])
        value_layer = jnp.where(fresh_slot[:, :, :, None], new_value.reshape(BATCH, 1, 1, k_cols), ordered[layer_index, 1])
        written.append(jnp.stack([key_layer, value_layer], axis=0))
        shaped_q = queries.reshape(BATCH, KV_HEADS, head_share, HEAD_DIM).astype(jnp.float32)
        shaped_k = new_key.reshape(BATCH, KV_HEADS, 1, HEAD_DIM).astype(jnp.float32)
        shaped_v = new_value.reshape(BATCH, KV_HEADS, 1, HEAD_DIM).astype(jnp.float32)
        cached_keys = ordered[layer_index, 0].reshape(BATCH, N_TP, CTX_DEV, KV_HEADS, HEAD_DIM).astype(jnp.float32)
        cached_values = ordered[layer_index, 1].reshape(BATCH, N_TP, CTX_DEV, KV_HEADS, HEAD_DIM).astype(jnp.float32)
        raw_scores = jnp.einsum('bkmd,bjtkd->bkmjt', shaped_q, cached_keys) * score_scale
        weights = jnp.where(visible[:, None, None, :, :], jnp.exp(capped(raw_scores)), 0.0)
        own_weight = jnp.exp(capped(lax.optimization_barrier(jnp.sum(shaped_q * shaped_k, axis=-1)) * score_scale))
        denominator = lax.optimization_barrier(jnp.sum(weights, axis=(-2, -1))) + own_weight
        numerator = jnp.einsum('bkmjt,bjtkd->bkmd', round_back(weights), cached_values)
        numerator = numerator + round_back(own_weight)[..., None] * shaped_v
        attended = (numerator / denominator[..., None]).astype(jnp.bfloat16).reshape(BATCH, q_cols)
        mixed = jnp.dot(attended, out_weight[layer_index].T, preferred_element_type=jnp.float32).astype(jnp.bfloat16)
        stream = stream + rms_scale(mixed.astype(jnp.float32), norm_gains[layer_index, 1])
        ffn_in = rms_scale(stream, norm_gains[layer_index, 2]).astype(jnp.bfloat16)
        gate_proj = jnp.dot(ffn_in, gate_up_weight[layer_index, 0].T, preferred_element_type=jnp.float32)
        up_proj = jnp.dot(ffn_in, gate_up_weight[layer_index, 1].T, preferred_element_type=jnp.float32)
        active = (jax.nn.gelu(gate_proj, approximate=True) * up_proj).astype(jnp.bfloat16)
        branch = jnp.dot(active, down_weight[layer_index], preferred_element_type=jnp.float32)
        stream = stream + rms_scale(branch, norm_gains[layer_index, 3])
    decode_cache = jnp.stack(written, axis=0).transpose(3, 0, 1, 2, 4, 5)
    return (stream, decode_cache)
```

```python
import jax
import jax.numpy as jnp
from jax import lax
from jax.sharding import Mesh
from jax.sharding import PartitionSpec as P

D = 4608
HEADS = 32
KV_HEADS = 16
HEAD_DIM = 128
PREFILL_TP = 8
TP = ("tp_0", "tp_1", "tp_2")
XY = ("tp_0", "tp_1")


EPSILON = 1e-06
SOFTCAP = 50.0


def cut_along(shard, dim, size):
    before, after = (shard.shape[:dim], shard.shape[dim + 1 :])
    return jnp.moveaxis(shard.reshape(*before, size, -1, *after), dim, 0)


def joined_along(tiles, dim):
    tiles = jnp.moveaxis(tiles, 0, dim)
    shape = tiles.shape
    return tiles.reshape(*shape[:dim], shape[dim] * shape[dim + 1], *shape[dim + 2 :])


def turned_blocks(tiles, axes, turns):
    shape = [lax.axis_size(a) for a in axes]
    tiles = tiles.reshape(*shape, *tiles.shape[1:])
    for k in turns:
        tiles = lax.all_to_all(tiles, axes[k], split_axis=k, concat_axis=k, tiled=True)
    return tiles.reshape(-1, *tiles.shape[len(axes) :])


def exchange_by_chip(shard, groups, turns, split_dim, concat_dim):
    size = lax.axis_size(groups[0]) * lax.axis_size(groups[1])
    tiles = cut_along(shard, split_dim, size)
    return joined_along(turned_blocks(tiles, groups, turns), concat_dim)


def core_swap(shard):
    return lax.ppermute(shard, "tp_2", [(0, 1), (1, 0)])


def both_cores(mine):
    other = core_swap(mine)
    first = lax.axis_index("tp_2") == 0
    return jnp.stack([jnp.where(first, mine, other), jnp.where(first, other, mine)], axis=1)


def gather_chips(shard):
    size = lax.axis_size(XY)
    spread = jnp.broadcast_to(shard[None], (size, *shard.shape))
    return lax.all_to_all(spread, XY, 0, 0, tiled=True)


def gather_all(shard):
    return both_cores(gather_chips(shard)).reshape(-1, *shard.shape)


def scatter_sum(tiles):
    size = lax.axis_size(XY)
    core = lax.axis_index("tp_2")
    tiles = tiles.reshape(size, 2, *tiles.shape[1:])
    keep = lax.dynamic_index_in_dim(tiles, core, 1, False)
    send = lax.dynamic_index_in_dim(tiles, 1 - core, 1, False)
    chip = (keep + core_swap(send.astype(jnp.bfloat16)).astype(jnp.float32)).astype(jnp.bfloat16)
    return jnp.sum(lax.all_to_all(chip, XY, 0, 0, tiled=True).astype(jnp.float32), axis=0)


def rms_scale(vector, gain_row):
    meansq = jnp.mean(vector * vector, axis=-1, keepdims=True)
    return vector * lax.rsqrt(meansq + EPSILON) * (1.0 + gain_row)


def rotate(vector, positions):
    half_dim = vector.shape[-1] // 2
    exponent = jnp.arange(half_dim, dtype=jnp.float32) * (-2.0 / vector.shape[-1])
    frequency = jnp.power(jnp.float32(10000.0), exponent)
    angles = positions.astype(jnp.float32)[:, None, None] * frequency
    cosine = jnp.cos(angles)
    sine_term = jnp.sin(angles)
    front_half = vector[..., :half_dim]
    back_half = vector[..., half_dim:]
    return jnp.concatenate(
        [front_half * cosine - back_half * sine_term, back_half * cosine + front_half * sine_term],
        axis=-1,
    )


def capped(raw_scores):
    return SOFTCAP * jnp.tanh(raw_scores / SOFTCAP)


def round_back(vector):
    return lax.optimization_barrier(vector.astype(jnp.bfloat16)).astype(jnp.float32)


def pick_slot(vector, my_group, my_slot):
    inner = lax.dynamic_index_in_dim(vector, my_group, 0, False)
    return lax.dynamic_index_in_dim(inner, my_slot, 1, False)


def take_pages(page_block, page_order):
    return jnp.take(page_block, page_order, axis=2)


def project_rows(left, weight_rows):
    return jnp.einsum("bd,cd->bc", left, weight_rows, preferred_element_type=jnp.float32)


def on_device(
    hidden_in,
    prefill_cache,
    lengths,
    page_table,
    qkv_weight,
    out_weight,
    gate_up_weight,
    down_weight,
    norm_gains,
):
    devices = lax.axis_size(TP)
    my_index = lax.axis_index(TP)
    batch_rows = hidden_in.shape[0]
    groups = devices // PREFILL_TP
    per_group = batch_rows // groups
    local_heads = KV_HEADS // PREFILL_TP
    head_share = HEADS // KV_HEADS
    layer_count = prefill_cache.shape[1]
    page_width = prefill_cache.shape[5]
    score_scale = (D / HEADS) ** (-0.5)
    q_cols = HEADS * HEAD_DIM
    k_cols = KV_HEADS * HEAD_DIM
    my_group = my_index // PREFILL_TP
    my_slot = my_index % PREFILL_TP
    group_rows = lax.dynamic_slice_in_dim(page_table, my_group * per_group, per_group, 0)
    group_lengths = lax.dynamic_slice_in_dim(lengths, my_group * per_group, per_group, 0)
    local_cache = prefill_cache[0]
    page_ids = jnp.arange(devices, dtype=jnp.int32)
    onehot = (group_rows[:, :, None] == page_ids[None, None, :]).astype(jnp.int32)
    inverse = jnp.sum(onehot * page_ids[None, :, None], axis=1)
    arranged = jax.vmap(take_pages, in_axes=(2, 0), out_axes=2)(local_cache, inverse)
    relaid = exchange_by_chip(arranged, (("tp_0", "tp_1"), "tp_2"), (1, 0), 3, 3)
    relaid = relaid.reshape(
        layer_count, 2, per_group, groups, PREFILL_TP, page_width, local_heads, HEAD_DIM
    )
    decode_local = relaid.transpose(0, 1, 3, 2, 5, 4, 6, 7).reshape(
        layer_count, 2, batch_rows, page_width, k_cols
    )
    my_pos = my_index * page_width + jnp.arange(page_width, dtype=jnp.int32)
    fresh_slot = my_pos[None, :] == lengths[:, None]
    kept_cache = local_cache.reshape(
        layer_count, 2, per_group, devices, page_width, local_heads, HEAD_DIM
    )
    cache_pos = (
        group_rows[:, :, None] * page_width + jnp.arange(page_width, dtype=jnp.int32)[None, None, :]
    )
    kept_visible = cache_pos < group_lengths[:, None, None]
    stream = hidden_in
    normed = rms_scale(stream, norm_gains[0, 0]).astype(jnp.bfloat16)
    column_part = project_rows(normed, qkv_weight[0]).astype(jnp.bfloat16)
    projected = joined_along(gather_all(column_part), 1)
    queries = rotate(
        projected[:, :q_cols].astype(jnp.float32).reshape(batch_rows, HEADS, HEAD_DIM), lengths
    ).astype(jnp.bfloat16)
    new_key = rotate(
        projected[:, q_cols : q_cols + k_cols]
        .astype(jnp.float32)
        .reshape(batch_rows, KV_HEADS, HEAD_DIM),
        lengths,
    ).astype(jnp.bfloat16)
    new_value = projected[:, q_cols + k_cols :]
    key_layer = jnp.where(
        fresh_slot[:, :, None], new_key.reshape(batch_rows, 1, k_cols), decode_local[0, 0]
    )
    value_layer = jnp.where(
        fresh_slot[:, :, None], new_value.reshape(batch_rows, 1, k_cols), decode_local[0, 1]
    )
    written = [jnp.stack([key_layer, value_layer], axis=0)]
    flat_q = queries.reshape(batch_rows, KV_HEADS, head_share, HEAD_DIM)
    flat_k = new_key.reshape(batch_rows, KV_HEADS, 1, HEAD_DIM)
    flat_v = new_value.reshape(batch_rows, KV_HEADS, 1, HEAD_DIM)
    own_weight = jnp.exp(
        capped(
            jnp.sum(flat_q.astype(jnp.float32) * flat_k.astype(jnp.float32), axis=-1) * score_scale
        )
    )
    own_term = round_back(own_weight)[..., None] * flat_v.astype(jnp.float32)
    shaped_q = flat_q.reshape(groups, per_group, PREFILL_TP, local_heads, head_share, HEAD_DIM)
    shaped_own = own_weight.reshape(groups, per_group, PREFILL_TP, local_heads, head_share)
    shaped_term = own_term.reshape(groups, per_group, PREFILL_TP, local_heads, head_share, HEAD_DIM)
    my_queries = pick_slot(shaped_q, my_group, my_slot)
    cached_keys = kept_cache[0, 0]
    cached_values = kept_cache[0, 1]
    raw_scores = (
        jnp.einsum("ramd,rjcad->ramjc", my_queries, cached_keys, preferred_element_type=jnp.float32)
        * score_scale
    )
    weights = jnp.where(kept_visible[:, None, None, :, :], jnp.exp(capped(raw_scores)), 0.0)
    numerator = jnp.einsum(
        "ramjc,rjcad->ramd",
        weights.astype(jnp.bfloat16),
        cached_values,
        preferred_element_type=jnp.float32,
    )
    numerator = numerator + pick_slot(shaped_term, my_group, my_slot)
    denominator = jnp.sum(weights, axis=(-2, -1)) + pick_slot(shaped_own, my_group, my_slot)
    mine = (
        (numerator / denominator[..., None])
        .astype(jnp.bfloat16)
        .reshape(1, per_group, local_heads * head_share * HEAD_DIM)
    )
    gathered = gather_all(mine[0])
    attended = (
        gathered.reshape(groups, PREFILL_TP, per_group, local_heads * head_share * HEAD_DIM)
        .transpose(0, 2, 1, 3)
        .reshape(batch_rows, q_cols)
    )
    mixed_part = project_rows(attended, out_weight[0]).astype(jnp.bfloat16)
    mixed_out = joined_along(gather_all(mixed_part), 1)
    stream = stream + rms_scale(mixed_out.astype(jnp.float32), norm_gains[0, 1])
    ffn_in = rms_scale(stream, norm_gains[0, 2]).astype(jnp.bfloat16)
    gate_proj = project_rows(ffn_in, gate_up_weight[0, 0])
    up_proj = project_rows(ffn_in, gate_up_weight[0, 1])
    active = (jax.nn.gelu(gate_proj, approximate=True) * up_proj).astype(jnp.bfloat16)
    branch = jnp.dot(active, down_weight[0], preferred_element_type=jnp.float32)
    column_count = branch.shape[1] // devices
    portion = scatter_sum(cut_along(branch, 1, devices))
    local_squares = jnp.sum(portion * portion, axis=-1)
    squares = jnp.sum(gather_chips(local_squares + core_swap(local_squares)), axis=0)
    gain_part = lax.dynamic_slice_in_dim(norm_gains[0, 3], my_index * column_count, column_count, 0)
    stream_part = lax.dynamic_slice_in_dim(stream, my_index * column_count, column_count, 1)
    result = stream_part + portion * lax.rsqrt(squares[:, None] / D + EPSILON) * (1.0 + gain_part)
    decode_cache = jnp.stack(written, axis=0)[None]
    return (result, decode_cache)


def solution(mesh):
    torus = Mesh(mesh.devices.reshape(mesh.shape["grp"], 8, 8, 2), ("grp", "tp_0", "tp_1", "tp_2"))
    return jax.shard_map(
        on_device,
        mesh=torus,
        in_specs=(
            P("grp", None),
            P(TP, None, None, "grp", None, None, None),
            P("grp"),
            P("grp", None),
            P(None, TP, None),
            P(None, TP, None),
            P(None, None, TP, None),
            P(None, TP, None),
            P(),
        ),
        out_specs=(P("grp", TP), P(TP, None, None, "grp", None, None)),
        check_vma=False,
    )
```

```python
import functools

import jax
import jax.numpy as jnp
from jax import lax
from jax.experimental import pallas as pl
from jax.experimental.pallas import tpu as pltpu
from jax.sharding import Mesh
from jax.sharding import PartitionSpec as P

D = 4608
HEADS = 32
KV_HEADS = 16
HEAD_DIM = 128
PREFILL_TP = 8
TP = ("tp_0", "tp_1", "tp_2")
XY = ("tp_0", "tp_1")

EPSILON = 1e-06
SOFTCAP = 50.0
LANES = 128
ROWS = 8
BF16 = jnp.bfloat16
F32 = jnp.float32

CHIPS = 64
QUARTERS = PREFILL_TP // 2
GROUPS = CHIPS // QUARTERS
SHARE = D // (2 * CHIPS)
BLOCKS = D // LANES
BATCH = 32
PER_GROUP = 2
PAGE_TILES = 2 * PER_GROUP * 2
BULK_TILES = 2 * PAGE_TILES + 1
VMEM_LIMIT = 48 * 1024 * 1024


def smem():
    return pl.BlockSpec(memory_space=pltpu.SMEM)


def vmem():
    return pl.BlockSpec(memory_space=pltpu.VMEM)


def anywhere():
    return pl.BlockSpec(memory_space=pl.ANY)


def call(kernel, out_shape, in_specs, out_specs, name, **more):
    return pl.pallas_call(
        kernel,
        out_shape=out_shape,
        in_specs=in_specs,
        out_specs=out_specs,
        name=name,
        compiler_params=pltpu.CompilerParams(vmem_limit_bytes=VMEM_LIMIT),
        **more,
    )


def shaped(shape, dtype):
    return jax.ShapeDtypeStruct(shape, dtype)


def nt_dot(left, right):
    return lax.dot_general(left, right, (((1,), (1,)), ((), ())), preferred_element_type=F32)


def nn_dot(left, right):
    return lax.dot_general(left, right, (((1,), (0,)), ((), ())), preferred_element_type=F32)


def iota(shape, dim):
    return lax.broadcasted_iota(jnp.int32, shape, dim)


def capped(raw_scores):
    return SOFTCAP * jnp.tanh(raw_scores / SOFTCAP)


def pages_kernel(me_ref, table_ref, cache_ref, out_ref):
    me = me_ref[0]
    core = me & 1
    group = me >> 3

    def place(j, carry):
        for e in range(PER_GROUP):
            block = table_ref[PER_GROUP * group + e, j]
            chip = block >> 1
            base = ((block & 1) ^ core) * PAGE_TILES + e * 2
            for kv in range(2):
                page = cache_ref[kv, e, j]
                out_ref[chip, base + kv * 4] = page[:, :LANES]
                out_ref[chip, base + kv * 4 + 1] = page[:, LANES:]
        return carry

    lax.fori_loop(0, 2 * CHIPS, place, 0, unroll=4)


def qkv_kernel(
    me_ref, hidden_ref, gain_ref, own_ref, other_ref, cos_ref, sin_ref, buf_ref, out_ref, tile_ref, sem
):
    me = me_ref[0]
    first = (me & 1) == 0
    head = me >> 1
    x = hidden_ref[...]
    meansq = jnp.sum(x * x, axis=-1, keepdims=True) * (1.0 / D)
    normed = (x * lax.rsqrt(meansq + EPSILON) * (1.0 + gain_ref[0, 0:1, :])).astype(BF16)
    own = nt_dot(normed, own_ref[0]).astype(BF16).astype(F32)
    other = nt_dot(normed, other_ref[0]).astype(BF16).astype(F32)
    front = jnp.where(first, own, other)
    back = jnp.where(first, other, own)
    cosine = cos_ref[...]
    sine = sin_ref[...]
    turned = head < HEADS + KV_HEADS
    new_front = jnp.where(turned, front * cosine - back * sine, front)
    new_back = jnp.where(turned, back * cosine + front * sine, back)
    whole = jnp.concatenate([new_front, new_back], axis=1)
    for u in range(BATCH // ROWS):
        rows = whole[ROWS * u : ROWS * u + ROWS, :].astype(BF16)
        per = CHIPS * ROWS // BATCH
        tile_ref[per * u : per * u + per] = jnp.broadcast_to(rows[None], (per, ROWS, LANES))
    copy = pltpu.make_async_copy(tile_ref, out_ref.at[:, BULK_TILES - 1], sem)
    copy.start()
    copy.wait()


def attend_kernel(me_ref, got_ref, seen_ref, cache_ref, out_ref):
    me = me_ref[0]
    group = me >> 3
    slot = me & 7
    rows_at = (group & 3) * PER_GROUP
    n_src = CHIPS * ROWS
    o = iota((32, n_src), 0)
    n = iota((32, n_src), 1)
    e = o & 1
    m = (o >> 1) & 3
    kind = o >> 3
    q_head = slot * 4 + m
    k_head = HEADS + slot * 2 + (m >> 1)
    v_head = k_head + KV_HEADS
    fix_head = HEADS + slot * 2 + (m & 1) + KV_HEADS * (m >> 1)
    chosen = jnp.where(kind == 0, q_head, jnp.where(kind == 1, k_head, jnp.where(kind == 2, v_head, fix_head)))
    pick = jnp.where(n == chosen * ROWS + rows_at + e, 1.0, 0.0).astype(BF16)
    source = got_ref[:, 0].astype(F32).reshape(n_src, LANES).astype(BF16)
    picked = nn_dot(pick, source)
    q = picked[0:8]
    new_k = picked[8:16]
    new_v = picked[16:24]
    q16 = q.astype(BF16)
    scale = (D / HEADS) ** (-0.5)
    row = iota((ROWS, 1), 0)
    scores = jnp.zeros((ROWS, 8 * 2 * CHIPS), F32)
    for ee in range(PER_GROUP):
        for a in range(2):
            keys = cache_ref[0, ee, :, a * LANES : a * LANES + LANES]
            part = nt_dot(q16, keys)
            scores = jnp.where(((row & 1) == ee) & ((row >> 2) == a), part, scores)
    weights = jnp.where(seen_ref[...] > 0.5, jnp.exp(capped(scores * scale)), 0.0)
    own = jnp.exp(capped(jnp.sum(q * new_k, axis=-1, keepdims=True) * scale))
    denominator = jnp.sum(weights, axis=-1, keepdims=True) + own
    w16 = weights.astype(BF16)
    numerator = own.astype(BF16).astype(F32) * new_v
    for ee in range(PER_GROUP):
        for a in range(2):
            values = cache_ref[1, ee, :, a * LANES : a * LANES + LANES]
            part = nn_dot(w16, values)
            numerator = numerator + jnp.where(((row & 1) == ee) & ((row >> 2) == a), part, 0.0)
    attended = numerator / denominator
    payload = jnp.concatenate([attended, picked[24:32]], axis=0).astype(BF16)
    out_ref[...] = jnp.broadcast_to(payload[None], (CHIPS, 2 * ROWS, LANES))


def mix_kernel(me_ref, own_ref, other_ref, weight_ref, out_ref):
    me = me_ref[0]
    first = (me & 1) == 0
    n_src = CHIPS * ROWS
    o = iota((n_src, n_src), 0)
    n = iota((n_src, n_src), 1)
    quarter = o >> 7
    m = (o >> 5) & 3
    group = (o >> 1) & 15
    source_row = (group * QUARTERS + quarter) * ROWS + m * 2 + (o & 1)
    pick = jnp.where(n == source_row, 1.0, 0.0).astype(BF16)
    own = own_ref[...][:, :ROWS].astype(F32)
    other = other_ref[...][:, :ROWS].astype(F32)
    mixed = jnp.zeros((BATCH, SHARE), F32)
    for c in range(2):
        mine = jnp.where(first, own, other) if c == 0 else jnp.where(first, other, own)
        rows = nn_dot(pick, mine.reshape(n_src, LANES).astype(BF16)).astype(BF16)
        left = jnp.concatenate([rows[BATCH * b : BATCH * b + BATCH] for b in range(16)], axis=1)
        right = jnp.concatenate(
            [weight_ref[0, :, (2 * y + c) * 512 : (2 * y + c) * 512 + 512] for y in range(QUARTERS)], axis=1
        )
        mixed = mixed + nt_dot(left, right)
    wide = jnp.concatenate(
        [mixed.astype(BF16).astype(F32), jnp.zeros((BATCH, LANES - SHARE), F32)], axis=1
    )
    turned = pltpu.roll(wide, (me * SHARE) % LANES, 1).astype(BF16)
    out_ref[...] = jnp.broadcast_to(turned[None], (CHIPS, BATCH, LANES))


def window(blocks, j):
    lane = iota((BATCH, LANES), 1)
    v, off = divmod(j * SHARE, LANES)
    here = blocks(v)
    if off + SHARE > LANES:
        here = jnp.where(lane >= off, here, blocks(v + 1))
    return here


def ffn_kernel(
    me_ref,
    own_ref,
    other_ref,
    hidden_ref,
    gain_ref,
    gate_up_ref,
    down_ref,
    keep_ref,
    send_ref,
    stream_ref,
    wide_ref,
    blocks_ref,
    ffn_ref,
):
    me = me_ref[0]
    first = (me & 1) == 0
    lane = iota((BATCH, LANES), 1)
    total = jnp.zeros((BATCH, LANES), F32)
    for v in range(BLOCKS):
        block = jnp.zeros((BATCH, LANES), F32)
        for j in range((LANES * v) // SHARE, (LANES * v + LANES - 1) // SHARE + 1):
            own = own_ref[j >> 1]
            other = other_ref[j >> 1]
            piece = (jnp.where(first, own, other) if j % 2 == 0 else jnp.where(first, other, own)).astype(F32)
            start = j * SHARE - LANES * v
            block = piece if start <= 0 else jnp.where(lane >= start, piece, block)
        blocks_ref[v] = block
        total = total + block * block
    scale = lax.rsqrt(jnp.sum(total, axis=-1, keepdims=True) * (1.0 / D) + EPSILON)
    total = jnp.zeros((BATCH, LANES), F32)
    for v in range(BLOCKS):
        cols = slice(LANES * v, LANES * v + LANES)
        block = hidden_ref[:, cols] + blocks_ref[v] * scale * (1.0 + gain_ref[0, 1:2, cols])
        wide_ref[v] = block
        total = total + block * block
    scale = lax.rsqrt(jnp.sum(total, axis=-1, keepdims=True) * (1.0 / D) + EPSILON)
    for v in range(BLOCKS):
        cols = slice(LANES * v, LANES * v + LANES)
        ffn_ref[:, cols] = (wide_ref[v] * scale * (1.0 + gain_ref[0, 2:3, cols])).astype(BF16)
    ffn_in = ffn_ref[...]
    gate = nt_dot(ffn_in, gate_up_ref[0, 0])
    up = nt_dot(ffn_in, gate_up_ref[0, 1])
    active = (jax.nn.gelu(gate, approximate=True) * up).astype(BF16)
    for v in range(BLOCKS):
        blocks_ref[v] = nn_dot(active, down_ref[0, :, LANES * v : LANES * v + LANES])
    for p in range(CHIPS):
        even = window(lambda v: blocks_ref[v], 2 * p)
        odd = window(lambda v: blocks_ref[v], 2 * p + 1)
        keep_ref[p] = jnp.where(first, even, odd).astype(BF16)
        send_ref[p] = jnp.where(first, odd, even).astype(BF16)
    start = me * SHARE
    at = start // LANES
    off = start % LANES
    after = jnp.minimum(at + 1, BLOCKS - 1)
    stream_ref[...] = jnp.where(lane >= off, wide_ref[at], wide_ref[after])


def to_front(x, me):
    off = (me * SHARE) % LANES
    return pltpu.roll(x, (LANES - off) % LANES, 1)


def portion_kernel(me_ref, got_ref, portion_ref, square_ref):
    me = me_ref[0]
    total = jnp.zeros((BATCH, LANES), F32)
    for p in range(CHIPS):
        total = total + got_ref[p].astype(F32)
    mine = to_front(total, me)
    portion_ref[...] = mine
    lane = iota((BATCH, LANES), 1)
    square = jnp.sum(jnp.where(lane < SHARE, mine * mine, 0.0), axis=-1, keepdims=True)
    square_ref[...] = jnp.sum(jnp.where(iota((BATCH, LANES), 0) == lane, square, 0.0), axis=0, keepdims=True)


def finish_kernel(me_ref, portion_ref, stream_ref, squares_ref, gain_ref, out_ref):
    me = me_ref[0]
    squares = jnp.sum(squares_ref[...], axis=0)
    lane = iota((BATCH, LANES), 1)
    column = jnp.sum(jnp.where(iota((BATCH, LANES), 0) == lane, squares, 0.0), axis=-1, keepdims=True)
    scale = lax.rsqrt(column * (1.0 / D) + EPSILON)
    done = to_front(stream_ref[...], me) + portion_ref[...] * scale * (1.0 + gain_ref[...])
    out_ref[...] = done[:, :SHARE]


def decode_kernel(me_ref, lengths_ref, got_ref, other_ref, own_new_ref, other_new_ref, out_ref):
    me = me_ref[0]
    core = me & 1

    def place(first_core):
        def body(g, carry):
            for y in range(QUARTERS):
                s = g * QUARTERS + y
                for side, ref in ((0, got_ref), (1, other_ref)):
                    slot = 2 * y + (first_core if side == 0 else 1 - first_core)
                    for kv in range(2):
                        for e in range(PER_GROUP):
                            for h in range(2):
                                cols = slice((2 * slot + h) * LANES, (2 * slot + h) * LANES + LANES)
                                out_ref[kv, g * PER_GROUP + e, :, cols] = ref[s, kv * 4 + e * 2 + h]
            return carry

        lax.fori_loop(0, GROUPS, body, 0)

    @pl.when(core == 0)
    def _():
        place(0)

    @pl.when(core == 1)
    def _():
        place(1)

    def fresh(r, carry):
        length = lengths_ref[r]

        @pl.when((length >> 3) == me)
        def _():
            g = r >> 1
            e = r & 1
            token = iota((ROWS, LANES), 0) == (length & 7)
            which = iota((2 * ROWS, LANES), 0)
            for y in range(QUARTERS):
                s = g * QUARTERS + y
                own = own_new_ref[s].astype(F32)
                other = other_new_ref[s].astype(F32)
                for c in range(2):
                    rows = jnp.where(core == c, own, other)
                    for kv in range(2):
                        for a in range(2):
                            at = ROWS + kv * 4 + a * 2 + e
                            line = jnp.sum(jnp.where(which == at, rows, 0.0), axis=0, keepdims=True)
                            slot = 2 * (2 * y + c) + a
                            cols = slice(slot * LANES, slot * LANES + LANES)
                            old = out_ref[kv, r, :, cols].astype(F32)
                            out_ref[kv, r, :, cols] = jnp.where(token, line, old).astype(BF16)

        return carry

    lax.fori_loop(0, BATCH, fresh, 0)


def core_swap(shard):
    return lax.ppermute(shard, "tp_2", [(0, 1), (1, 0)])


def to_chips(tiles):
    return lax.all_to_all(tiles, XY, 0, 0, tiled=True)


def pages_call(me, table, cache):
    return call(
        pages_kernel,
        shaped((CHIPS, BULK_TILES, ROWS, LANES), BF16),
        [smem(), smem(), vmem()],
        vmem(),
        "pages",
    )(me, table, cache)


def qkv_call(me, hidden, gains, own, other, cosine, sine, buf):
    return call(
        qkv_kernel,
        shaped(buf.shape, BF16),
        [smem()] + [vmem()] * 6 + [anywhere()],
        anywhere(),
        "qkv",
        scratch_shapes=[pltpu.VMEM((CHIPS, ROWS, LANES), BF16), pltpu.SemaphoreType.DMA],
        input_output_aliases={7: 0},
    )(me, hidden, gains, own, other, cosine, sine, buf)


def attend_call(me, got, seen, cache):
    return pl.pallas_call(
        attend_kernel,
        grid=(1,),
        out_shape=shaped((CHIPS, 2 * ROWS, LANES), BF16),
        in_specs=[
            smem(),
            pl.BlockSpec((CHIPS, 1, ROWS, LANES), lambda i: (0, BULK_TILES - 1, 0, 0)),
            vmem(),
            vmem(),
        ],
        out_specs=vmem(),
        name="attend",
        compiler_params=pltpu.CompilerParams(vmem_limit_bytes=VMEM_LIMIT),
    )(me, got, seen, cache)


def mix_call(me, own, other, weight):
    return call(mix_kernel, shaped((CHIPS, BATCH, LANES), BF16), [smem()] + [vmem()] * 3, vmem(), "mix")(
        me, own, other, weight
    )


def ffn_call(me, own, other, hidden, gains, gate_up, down):
    wide = shaped((CHIPS, BATCH, LANES), BF16)
    return call(
        ffn_kernel,
        (wide, wide, shaped((BATCH, LANES), F32)),
        [smem()] + [vmem()] * 6,
        (vmem(), vmem(), vmem()),
        "ffn",
        scratch_shapes=[
            pltpu.VMEM((BLOCKS, BATCH, LANES), F32),
            pltpu.VMEM((BLOCKS, BATCH, LANES), F32),
            pltpu.VMEM((BATCH, D), BF16),
        ],
    )(me, own, other, hidden, gains, gate_up, down)


def portion_call(me, got):
    return call(
        portion_kernel,
        (shaped((BATCH, LANES), F32), shaped((1, LANES), F32)),
        [smem(), vmem()],
        (vmem(), vmem()),
        "portion",
    )(me, got)


def finish_call(me, portion, stream, squares, gain):
    return call(finish_kernel, shaped((BATCH, SHARE), F32), [smem()] + [vmem()] * 4, vmem(), "finish")(
        me, portion, stream, squares, gain
    )


def decode_call(me, lengths, got, other, own_new, other_new):
    return pl.pallas_call(
        decode_kernel,
        grid=(1,),
        out_shape=shaped((2, BATCH, ROWS, KV_HEADS * HEAD_DIM), BF16),
        in_specs=[
            smem(),
            smem(),
            pl.BlockSpec((CHIPS, PAGE_TILES, ROWS, LANES), lambda i: (0, 0, 0, 0)),
            vmem(),
            vmem(),
            vmem(),
        ],
        out_specs=vmem(),
        name="decode",
        compiler_params=pltpu.CompilerParams(vmem_limit_bytes=VMEM_LIMIT),
    )(me, lengths, got, other, own_new, other_new)


def rope_tables(lengths):
    half_dim = HEAD_DIM // 2
    exponent = jnp.arange(half_dim, dtype=F32) * (-2.0 / HEAD_DIM)
    frequency = jnp.power(jnp.float32(10000.0), exponent)
    angles = lengths.astype(F32)[:, None] * frequency
    return jnp.cos(angles), jnp.sin(angles)


def on_device(
    hidden_in,
    prefill_cache,
    lengths,
    page_table,
    qkv_weight,
    out_weight,
    gate_up_weight,
    down_weight,
    norm_gains,
):
    my_index = lax.axis_index(TP)
    me = jnp.full((1,), my_index, jnp.int32)
    group = my_index // PREFILL_TP
    cache = prefill_cache[0, 0]
    other_rows = core_swap(qkv_weight)
    buf = pages_call(me, page_table, cache)
    cosine, sine = rope_tables(lengths)
    buf = qkv_call(me, hidden_in, norm_gains, qkv_weight, other_rows, cosine, sine, buf)
    with jax.named_scope("bulk"):
        got = to_chips(buf)
    rows = lax.dynamic_slice_in_dim(page_table, group * PER_GROUP, PER_GROUP, 0)
    limits = lax.dynamic_slice_in_dim(lengths, group * PER_GROUP, PER_GROUP, 0)
    position = rows[:, :, None] * ROWS + jnp.arange(ROWS, dtype=jnp.int32)
    seen = (position < limits[:, None, None]).astype(F32).reshape(PER_GROUP, -1)
    seen = jnp.tile(seen, (4, 1))
    gain = lax.dynamic_slice_in_dim(norm_gains[0, 3], my_index * SHARE, SHARE, 0)
    gain = jnp.pad(gain, (0, LANES - SHARE))[None]
    payload = attend_call(me, got, seen, cache.reshape(2, PER_GROUP, -1, 2 * HEAD_DIM))
    with jax.named_scope("attended"):
        own_att = to_chips(payload)
    other_att = core_swap(own_att)
    other_pages = core_swap(got[:, PAGE_TILES : 2 * PAGE_TILES])
    payload = mix_call(me, own_att, other_att, out_weight)
    with jax.named_scope("mixed"):
        own_mix = to_chips(payload)
    other_mix = core_swap(own_mix)
    keep, send, stream = ffn_call(me, own_mix, other_mix, hidden_in, norm_gains, gate_up_weight, down_weight)
    chip = (keep.astype(F32) + core_swap(send).astype(F32)).astype(BF16)
    with jax.named_scope("branch"):
        got_branch = to_chips(chip)
    portion, square = portion_call(me, got_branch)
    square = square + core_swap(square)
    with jax.named_scope("squares"):
        squares = to_chips(jnp.broadcast_to(square[None], (CHIPS, 1, LANES)))
    result = finish_call(me, portion, stream, squares, gain)
    decoded = decode_call(me, lengths, got, other_pages, own_att, other_att)
    return result, decoded[None, None]


def solution(mesh):
    torus = Mesh(mesh.devices.reshape(mesh.shape["grp"], 8, 8, 2), ("grp", "tp_0", "tp_1", "tp_2"))
    return jax.shard_map(
        on_device,
        mesh=torus,
        in_specs=(
            P("grp", None),
            P(TP, None, None, "grp", None, None, None),
            P("grp"),
            P("grp", None),
            P(None, TP, None),
            P(None, TP, None),
            P(None, None, TP, None),
            P(None, TP, None),
            P(),
        ),
        out_specs=(P("grp", TP), P(TP, None, None, "grp", None, None)),
        check_vma=False,
    )
```

```python
import jax
import jax.numpy as jnp
from jax import lax
from jax.experimental import pallas as pl
from jax.experimental.pallas import tpu as pltpu
from jax.sharding import Mesh
from jax.sharding import PartitionSpec as P

D = 4608
HEADS = 32
KV_HEADS = 16
HEAD_DIM = 128
PREFILL_TP = 8
TP = ("tp_0", "tp_1", "tp_2")
XY = ("tp_0", "tp_1")

EPSILON = 1e-06
SOFTCAP = 50.0
LANES = 128
ROWS = 8
BF16 = jnp.bfloat16
F32 = jnp.float32

CHIPS = 64
QUARTERS = PREFILL_TP // 2
GROUPS = CHIPS // QUARTERS
SHARE = D // (2 * CHIPS)
BLOCKS = D // LANES
BATCH = 32
HALF = BATCH // 2
PER_GROUP = 2
PAGE_TILES = 2 * PER_GROUP * 2
BULK_TILES = 2 * PAGE_TILES + 1
VMEM_LIMIT = 24 * 1024 * 1024


def smem():
    return pl.BlockSpec(memory_space=pltpu.SMEM)


def vmem():
    return pl.BlockSpec(memory_space=pltpu.VMEM)


def call(kernel, out_shape, in_specs, out_specs, **more):
    return pl.pallas_call(
        kernel,
        out_shape=out_shape,
        in_specs=in_specs,
        out_specs=out_specs,
        compiler_params=pltpu.CompilerParams(vmem_limit_bytes=VMEM_LIMIT),
        **more,
    )


def shaped(shape, dtype):
    return jax.ShapeDtypeStruct(shape, dtype)


def nt_dot(left, right):
    return lax.dot_general(left, right, (((1,), (1,)), ((), ())), preferred_element_type=F32)


def nn_dot(left, right):
    return lax.dot_general(left, right, (((1,), (0,)), ((), ())), preferred_element_type=F32)


def iota(shape, dim):
    return lax.broadcasted_iota(jnp.int32, shape, dim)


def capped(raw_scores):
    return SOFTCAP * jnp.tanh(raw_scores / SOFTCAP)


def pages_kernel(me_ref, table_ref, cache_ref, out_ref, held_ref, sem):
    me = me_ref[0]
    core = me & 1
    group = me >> 3
    keep = pltpu.make_async_copy(cache_ref, held_ref, sem)
    keep.start()

    def place(j, carry):
        for e in range(PER_GROUP):
            block = table_ref[PER_GROUP * group + e, j]
            chip = block >> 1
            base = ((block & 1) ^ core) * PAGE_TILES + e * 2
            for kv in range(2):
                page = cache_ref[kv, e, j]
                out_ref[chip, base + kv * 4] = page[:, :LANES]
                out_ref[chip, base + kv * 4 + 1] = page[:, LANES:]
        return carry

    lax.fori_loop(0, 2 * CHIPS, place, 0, unroll=4)
    keep.wait()


def qkv_kernel(
    me_ref, hidden_ref, gain_ref, own_ref, other_ref, cos_ref, sin_ref, buf_ref, out_ref, tile_ref, sem
):
    me = me_ref[0]
    first = (me & 1) == 0
    head = me >> 1
    x = hidden_ref[...]
    meansq = jnp.sum(x * x, axis=-1, keepdims=True) * (1.0 / D)
    normed = (x * lax.rsqrt(meansq + EPSILON) * (1.0 + gain_ref[0, 0:1, :])).astype(BF16)
    own = nt_dot(normed, own_ref[0]).astype(BF16).astype(F32)
    other = nt_dot(normed, other_ref[0]).astype(BF16).astype(F32)
    front = jnp.where(first, own, other)
    back = jnp.where(first, other, own)
    cosine = cos_ref[...]
    sine = sin_ref[...]
    turned = head < HEADS + KV_HEADS
    new_front = jnp.where(turned, front * cosine - back * sine, front)
    new_back = jnp.where(turned, back * cosine + front * sine, back)
    whole = jnp.concatenate([new_front, new_back], axis=1)
    for u in range(BATCH // ROWS):
        rows = whole[ROWS * u : ROWS * u + ROWS, :].astype(BF16)
        per = CHIPS * ROWS // BATCH
        tile_ref[per * u : per * u + per] = jnp.broadcast_to(rows[None], (per, ROWS, LANES))
    copy = pltpu.make_async_copy(tile_ref, out_ref.at[:, BULK_TILES - 1], sem)
    copy.start()
    copy.wait()


def attend_kernel(me_ref, lengths_ref, got_ref, table_ref, cache_ref, out_ref):
    me = me_ref[0]
    group = me >> 3
    slot = me & 7
    rows_at = (group & 3) * PER_GROUP
    n_src = CHIPS * ROWS
    o = iota((32, n_src), 0)
    n = iota((32, n_src), 1)
    e = o & 1
    m = (o >> 1) & 3
    kind = o >> 3
    q_head = slot * 4 + m
    k_head = HEADS + slot * 2 + (m >> 1)
    v_head = k_head + KV_HEADS
    fix_head = HEADS + slot * 2 + (m & 1) + KV_HEADS * (m >> 1)
    chosen = jnp.where(kind == 0, q_head, jnp.where(kind == 1, k_head, jnp.where(kind == 2, v_head, fix_head)))
    pick = jnp.where(n == chosen * ROWS + rows_at + e, 1.0, 0.0).astype(BF16)
    source = got_ref[:, 0].astype(F32).reshape(n_src, LANES).astype(BF16)
    picked = nn_dot(pick, source)
    q = picked[0:8]
    new_k = picked[8:16]
    new_v = picked[16:24]
    q16 = q.astype(BF16)
    scale = (D / HEADS) ** (-0.5)
    row = iota((ROWS, 1), 0)
    scores = jnp.zeros((ROWS, 8 * 2 * CHIPS), F32)
    for ee in range(PER_GROUP):
        for a in range(2):
            keys = cache_ref[0, ee, :, a * LANES : a * LANES + LANES]
            part = nt_dot(q16, keys)
            scores = jnp.where(((row & 1) == ee) & ((row >> 2) == a), part, scores)
    pages = 2 * CHIPS
    table_row = iota((BATCH, pages), 0)
    lines = []
    for ee in range(PER_GROUP):
        chosen_row = jnp.where(table_row == group * PER_GROUP + ee, table_ref[...], 0)
        lines.append(jnp.sum(chosen_row, axis=0, keepdims=True))
    blocks = jnp.where((row & 1) == 0, lines[0], lines[1]).astype(F32).astype(BF16)
    spread = jnp.where(iota((pages, ROWS * pages), 1) >> 3 == iota((pages, ROWS * pages), 0), 1.0, 0.0)
    position = nn_dot(blocks, spread.astype(BF16)).astype(jnp.int32) * ROWS + (iota((ROWS, ROWS * pages), 1) & 7)
    limit = jnp.where((row & 1) == 0, lengths_ref[group * PER_GROUP], lengths_ref[group * PER_GROUP + 1])
    weights = jnp.where(position < limit, jnp.exp(capped(scores * scale)), 0.0)
    own = jnp.exp(capped(jnp.sum(q * new_k, axis=-1, keepdims=True) * scale))
    denominator = jnp.sum(weights, axis=-1, keepdims=True) + own
    w16 = weights.astype(BF16)
    numerator = own.astype(BF16).astype(F32) * new_v
    for ee in range(PER_GROUP):
        for a in range(2):
            values = cache_ref[1, ee, :, a * LANES : a * LANES + LANES]
            part = nn_dot(w16, values)
            numerator = numerator + jnp.where(((row & 1) == ee) & ((row >> 2) == a), part, 0.0)
    attended = numerator / denominator
    payload = jnp.concatenate([attended, picked[24:32]], axis=0).astype(BF16)
    out_ref[...] = jnp.broadcast_to(payload[None], (CHIPS, 2 * ROWS, LANES))


def mix_kernel(me_ref, own_ref, other_ref, weight_ref, out_ref):
    me = me_ref[0]
    first = (me & 1) == 0
    n_src = CHIPS * ROWS
    o = iota((n_src, n_src), 0)
    n = iota((n_src, n_src), 1)
    quarter = o >> 7
    m = (o >> 5) & 3
    group = (o >> 1) & 15
    source_row = (group * QUARTERS + quarter) * ROWS + m * 2 + (o & 1)
    pick = jnp.where(n == source_row, 1.0, 0.0).astype(BF16)
    own = own_ref[...][:, :ROWS].astype(F32)
    other = other_ref[...][:, :ROWS].astype(F32)
    mixed = jnp.zeros((BATCH, SHARE), F32)
    for c in range(2):
        mine = jnp.where(first, own, other) if c == 0 else jnp.where(first, other, own)
        rows = nn_dot(pick, mine.reshape(n_src, LANES).astype(BF16)).astype(BF16)
        left = jnp.concatenate([rows[BATCH * b : BATCH * b + BATCH] for b in range(16)], axis=1)
        right = jnp.concatenate(
            [weight_ref[0, :, (2 * y + c) * 512 : (2 * y + c) * 512 + 512] for y in range(QUARTERS)], axis=1
        )
        mixed = mixed + nt_dot(left, right)
    values = mixed.astype(BF16).astype(F32)
    gap = jnp.zeros((HALF, LANES // 2 - SHARE), F32)
    packed = jnp.concatenate([values[:HALF], gap, values[HALF:], gap], axis=1)
    turned = pltpu.roll(packed, (me * SHARE) % LANES, 1).astype(BF16)
    out_ref[...] = jnp.broadcast_to(turned[None], (CHIPS, HALF, LANES))


def window(low_ref, high_ref, j):
    lane = iota((HALF, LANES), 1)
    far = (lane + LANES // 2) % LANES
    v, off = divmod(j * SHARE, LANES)
    low = low_ref[v]
    high = high_ref[v]
    if off + SHARE > LANES:
        low = jnp.where(lane >= off, low, low_ref[v + 1])
        high = jnp.where(far >= off, high, high_ref[v + 1])
    return jnp.where((lane - off) % LANES < LANES // 2, low, high)


def ffn_kernel(
    me_ref,
    own_ref,
    other_ref,
    hidden_ref,
    gain_ref,
    gate_up_ref,
    down_ref,
    keep_ref,
    send_ref,
    stream_ref,
    wide_ref,
    low_ref,
    high_ref,
    ffn_ref,
):
    me = me_ref[0]
    first = (me & 1) == 0
    lane = iota((BATCH, LANES), 1)
    near = iota((HALF, LANES), 1)
    far = (near + LANES // 2) % LANES
    total = jnp.zeros((BATCH, LANES), F32)
    for v in range(BLOCKS):
        low = high = None
        for j in range((LANES * v) // SHARE, (LANES * v + LANES - 1) // SHARE + 1):
            own = own_ref[j >> 1]
            other = other_ref[j >> 1]
            piece = (jnp.where(first, own, other) if j % 2 == 0 else jnp.where(first, other, own)).astype(F32)
            start = j * SHARE - LANES * v
            low = piece if low is None else jnp.where(near >= start, piece, low)
            high = piece if high is None else jnp.where(far >= start, piece, high)
        block = jnp.concatenate([low, pltpu.roll(high, LANES // 2, 1)], axis=0)
        wide_ref[v] = block
        total = total + block * block
    scale = lax.rsqrt(jnp.sum(total, axis=-1, keepdims=True) * (1.0 / D) + EPSILON)
    total = jnp.zeros((BATCH, LANES), F32)
    for v in range(BLOCKS):
        cols = slice(LANES * v, LANES * v + LANES)
        block = hidden_ref[:, cols] + wide_ref[v] * scale * (1.0 + gain_ref[0, 1:2, cols])
        wide_ref[v] = block
        total = total + block * block
    scale = lax.rsqrt(jnp.sum(total, axis=-1, keepdims=True) * (1.0 / D) + EPSILON)
    for v in range(BLOCKS):
        cols = slice(LANES * v, LANES * v + LANES)
        ffn_ref[:, cols] = (wide_ref[v] * scale * (1.0 + gain_ref[0, 2:3, cols])).astype(BF16)
    ffn_in = ffn_ref[...]
    gate = nt_dot(ffn_in, gate_up_ref[0, 0])
    up = nt_dot(ffn_in, gate_up_ref[0, 1])
    active = (jax.nn.gelu(gate, approximate=True) * up).astype(BF16)
    for v in range(BLOCKS):
        block = nn_dot(active, down_ref[0, :, LANES * v : LANES * v + LANES])
        low_ref[v] = block[:HALF]
        high_ref[v] = pltpu.roll(block[HALF:], LANES // 2, 1)
    for p in range(CHIPS):
        even = window(low_ref, high_ref, 2 * p)
        odd = window(low_ref, high_ref, 2 * p + 1)
        keep_ref[p] = jnp.where(first, even, odd).astype(BF16)
        send_ref[p] = jnp.where(first, odd, even).astype(BF16)
    start = me * SHARE
    at = start // LANES
    off = start % LANES
    after = jnp.minimum(at + 1, BLOCKS - 1)
    stream_ref[...] = jnp.where(lane >= off, wide_ref[at], wide_ref[after])


def to_front(x, me):
    off = (me * SHARE) % LANES
    return pltpu.roll(x, (LANES - off) % LANES, 1)


def portion_kernel(me_ref, got_ref, portion_ref, square_ref):
    me = me_ref[0]
    total = jnp.zeros((HALF, LANES), F32)
    for p in range(CHIPS):
        total = total + got_ref[p].astype(F32)
    packed = to_front(total, me)
    mine = jnp.concatenate([packed, pltpu.roll(packed, LANES // 2, 1)], axis=0)
    portion_ref[...] = mine
    lane = iota((BATCH, LANES), 1)
    square = jnp.sum(jnp.where(lane < SHARE, mine * mine, 0.0), axis=-1, keepdims=True)
    line = jnp.sum(jnp.where(iota((BATCH, LANES), 0) == lane, square, 0.0), axis=0, keepdims=True)
    square_ref[...] = jnp.broadcast_to(line[None], (CHIPS, 1, LANES))


def finish_kernel(me_ref, portion_ref, stream_ref, own_ref, other_ref, gain_ref, out_ref):
    me = me_ref[0]
    squares = jnp.sum(own_ref[...] + other_ref[...], axis=0)
    lane = iota((BATCH, LANES), 1)
    column = jnp.sum(jnp.where(iota((BATCH, LANES), 0) == lane, squares, 0.0), axis=-1, keepdims=True)
    scale = lax.rsqrt(column * (1.0 / D) + EPSILON)
    at = (me * SHARE) // LANES
    after = jnp.minimum(at + 1, BLOCKS - 1)
    here = gain_ref[0, 3:4, pl.ds(pl.multiple_of(at * LANES, LANES), LANES)]
    there = gain_ref[0, 3:4, pl.ds(pl.multiple_of(after * LANES, LANES), LANES)]
    gain = jnp.where(lane >= (me * SHARE) % LANES, here, there)
    done = to_front(stream_ref[...], me) + portion_ref[...] * scale * (1.0 + to_front(gain, me))
    out_ref[...] = done[:, :SHARE]


def decode_kernel(me_ref, lengths_ref, got_ref, other_ref, own_new_ref, other_new_ref, out_ref):
    me = me_ref[0]
    core = me & 1

    def place(first_core):
        def body(g, carry):
            for y in range(QUARTERS):
                s = g * QUARTERS + y
                for side, ref in ((0, got_ref), (1, other_ref)):
                    slot = 2 * y + (first_core if side == 0 else 1 - first_core)
                    for kv in range(2):
                        for e in range(PER_GROUP):
                            for h in range(2):
                                cols = slice((2 * slot + h) * LANES, (2 * slot + h) * LANES + LANES)
                                out_ref[kv, g * PER_GROUP + e, :, cols] = ref[s, kv * 4 + e * 2 + h]
            return carry

        lax.fori_loop(0, GROUPS, body, 0)

    @pl.when(core == 0)
    def _():
        place(0)

    @pl.when(core == 1)
    def _():
        place(1)

    def fresh(r, carry):
        length = lengths_ref[r]

        @pl.when((length >> 3) == me)
        def _():
            g = r >> 1
            e = r & 1
            token = iota((ROWS, LANES), 0) == (length & 7)
            which = iota((2 * ROWS, LANES), 0)
            for y in range(QUARTERS):
                s = g * QUARTERS + y
                own = own_new_ref[s].astype(F32)
                other = other_new_ref[s].astype(F32)
                for c in range(2):
                    rows = jnp.where(core == c, own, other)
                    for kv in range(2):
                        for a in range(2):
                            at = ROWS + kv * 4 + a * 2 + e
                            line = jnp.sum(jnp.where(which == at, rows, 0.0), axis=0, keepdims=True)
                            slot = 2 * (2 * y + c) + a
                            cols = slice(slot * LANES, slot * LANES + LANES)
                            old = out_ref[kv, r, :, cols].astype(F32)
                            out_ref[kv, r, :, cols] = jnp.where(token, line, old).astype(BF16)

        return carry

    lax.fori_loop(0, BATCH, fresh, 0)


def core_swap(shard):
    return lax.ppermute(shard, "tp_2", [(0, 1), (1, 0)])


def to_chips(tiles):
    return lax.all_to_all(tiles, XY, 0, 0, tiled=True)


def pages_call(me, table, cache):
    return call(
        pages_kernel,
        (shaped((CHIPS, BULK_TILES, ROWS, LANES), BF16), shaped(cache.shape, BF16)),
        [smem(), smem(), vmem()],
        (vmem(), vmem()),
        scratch_shapes=[pltpu.SemaphoreType.DMA],
    )(me, table, cache)


def qkv_call(me, hidden, gains, own, other, cosine, sine, buf):
    return call(
        qkv_kernel,
        shaped(buf.shape, BF16),
        [smem()] + [vmem()] * 6 + [pl.BlockSpec(memory_space=pl.ANY)],
        pl.BlockSpec(memory_space=pl.ANY),
        scratch_shapes=[pltpu.VMEM((CHIPS, ROWS, LANES), BF16), pltpu.SemaphoreType.DMA],
        input_output_aliases={7: 0},
    )(me, hidden, gains, own, other, cosine, sine, buf)


def attend_call(me, lengths, got, table, cache):
    return pl.pallas_call(
        attend_kernel,
        grid=(1,),
        out_shape=shaped((CHIPS, 2 * ROWS, LANES), BF16),
        in_specs=[
            smem(),
            smem(),
            pl.BlockSpec((CHIPS, 1, ROWS, LANES), lambda i: (0, BULK_TILES - 1, 0, 0)),
            vmem(),
            vmem(),
        ],
        out_specs=vmem(),
        name="attend",
        compiler_params=pltpu.CompilerParams(vmem_limit_bytes=VMEM_LIMIT),
    )(me, lengths, got, table, cache)


def mix_call(me, own, other, weight):
    return call(mix_kernel, shaped((CHIPS, HALF, LANES), BF16), [smem()] + [vmem()] * 3, vmem())(me, own, other, weight)


def ffn_call(me, own, other, hidden, gains, gate_up, down):
    wide = shaped((CHIPS, HALF, LANES), BF16)
    return call(
        ffn_kernel,
        (wide, wide, shaped((BATCH, LANES), F32)),
        [smem()] + [vmem()] * 6,
        (vmem(), vmem(), vmem()),
        scratch_shapes=[
            pltpu.VMEM((BLOCKS, BATCH, LANES), F32),
            pltpu.VMEM((BLOCKS, HALF, LANES), F32),
            pltpu.VMEM((BLOCKS, HALF, LANES), F32),
            pltpu.VMEM((BATCH, D), BF16),
        ],
    )(me, own, other, hidden, gains, gate_up, down)


def portion_call(me, got):
    return call(
        portion_kernel,
        (shaped((BATCH, LANES), F32), shaped((CHIPS, 1, LANES), F32)),
        [smem(), vmem()],
        (vmem(), vmem()),
    )(me, got)


def finish_call(me, portion, stream, own, other, gains):
    return call(finish_kernel, shaped((BATCH, SHARE), F32), [smem()] + [vmem()] * 5, vmem())(
        me, portion, stream, own, other, gains
    )


def decode_call(me, lengths, got, other, own_new, other_new):
    return pl.pallas_call(
        decode_kernel,
        grid=(1,),
        out_shape=shaped((2, BATCH, ROWS, KV_HEADS * HEAD_DIM), BF16),
        in_specs=[
            smem(),
            smem(),
            pl.BlockSpec((CHIPS, PAGE_TILES, ROWS, LANES), lambda i: (0, 0, 0, 0)),
            vmem(),
            vmem(),
            vmem(),
        ],
        out_specs=vmem(),
        name="decode",
        compiler_params=pltpu.CompilerParams(vmem_limit_bytes=VMEM_LIMIT),
    )(me, lengths, got, other, own_new, other_new)


def rope_tables(lengths):
    half_dim = HEAD_DIM // 2
    exponent = jnp.arange(half_dim, dtype=F32) * (-2.0 / HEAD_DIM)
    frequency = jnp.power(jnp.float32(10000.0), exponent)
    angles = lengths.astype(F32)[:, None] * frequency
    return jnp.cos(angles), jnp.sin(angles)


def on_device(
    hidden_in,
    prefill_cache,
    lengths,
    page_table,
    qkv_weight,
    out_weight,
    gate_up_weight,
    down_weight,
    norm_gains,
):
    me = jnp.full((1,), lax.axis_index(TP), jnp.int32)
    cache = prefill_cache[0, 0]
    other_rows = core_swap(qkv_weight)
    buf, held = pages_call(me, page_table, cache)
    cosine, sine = rope_tables(lengths)
    buf = qkv_call(me, hidden_in, norm_gains, qkv_weight, other_rows, cosine, sine, buf)
    got = to_chips(buf)
    payload = attend_call(me, lengths, got, page_table, held.reshape(2, PER_GROUP, -1, 2 * HEAD_DIM))
    own_att = to_chips(payload)
    other_att = core_swap(own_att)
    leaving = got[:, PAGE_TILES : 2 * PAGE_TILES]
    other_pages = core_swap(leaving)
    payload = mix_call(me, own_att, other_att, out_weight)
    own_mix = to_chips(payload)
    other_mix = core_swap(own_mix)
    keep, send, stream = ffn_call(me, own_mix, other_mix, hidden_in, norm_gains, gate_up_weight, down_weight)
    chip = (keep.astype(F32) + core_swap(send).astype(F32)).astype(BF16)
    got_branch = to_chips(chip)
    portion, square = portion_call(me, got_branch)
    squares = to_chips(square)
    result = finish_call(me, portion, stream, squares, core_swap(squares), norm_gains)
    decoded = decode_call(me, lengths, got, other_pages, own_att, other_att)
    return result, decoded[None, None]


def solution(mesh):
    torus = Mesh(mesh.devices.reshape(mesh.shape["grp"], 8, 8, 2), ("grp", "tp_0", "tp_1", "tp_2"))
    return jax.shard_map(
        on_device,
        mesh=torus,
        in_specs=(
            P("grp", None),
            P(TP, None, None, "grp", None, None, None),
            P("grp"),
            P("grp", None),
            P(None, TP, None),
            P(None, TP, None),
            P(None, None, TP, None),
            P(None, TP, None),
            P(),
        ),
        out_specs=(P("grp", TP), P(TP, None, None, "grp", None, None)),
        check_vma=False,
    )
```

```python
import jax
import jax.numpy as jnp
from jax import lax
from jax.experimental import pallas as pl
from jax.experimental.pallas import tpu as pltpu
from jax.sharding import Mesh
from jax.sharding import PartitionSpec as P

D = 4608
HEADS = 32
KV_HEADS = 16
HEAD_DIM = 128
PREFILL_TP = 8
TP = ("tp_0", "tp_1", "tp_2")
XY = ("tp_0", "tp_1")

EPSILON = 1e-06
SOFTCAP = 50.0
LANES = 128
ROWS = 8
BF16 = jnp.bfloat16
F32 = jnp.float32

CHIPS = 64
QUARTERS = PREFILL_TP // 2
GROUPS = CHIPS // QUARTERS
SHARE = D // (2 * CHIPS)
BLOCKS = D // LANES
BATCH = 32
HALF = BATCH // 2
PER_GROUP = 2
PAGE_TILES = 2 * PER_GROUP * 2
BULK_TILES = 2 * PAGE_TILES + 1
VMEM_LIMIT = 24 * 1024 * 1024


def smem():
    return pl.BlockSpec(memory_space=pltpu.SMEM)


def vmem():
    return pl.BlockSpec(memory_space=pltpu.VMEM)


def hbm():
    return pl.BlockSpec(memory_space=pltpu.HBM)


def call(kernel, out_shape, in_specs, out_specs, **more):
    return pl.pallas_call(
        kernel,
        out_shape=out_shape,
        in_specs=in_specs,
        out_specs=out_specs,
        compiler_params=pltpu.CompilerParams(vmem_limit_bytes=VMEM_LIMIT),
        **more,
    )


def shaped(shape, dtype):
    return jax.ShapeDtypeStruct(shape, dtype)


def nt_dot(left, right):
    return lax.dot_general(left, right, (((1,), (1,)), ((), ())), preferred_element_type=F32)


def nn_dot(left, right):
    return lax.dot_general(left, right, (((1,), (0,)), ((), ())), preferred_element_type=F32)


def iota(shape, dim):
    return lax.broadcasted_iota(jnp.int32, shape, dim)


def capped(raw_scores):
    return SOFTCAP * jnp.tanh(raw_scores / SOFTCAP)


def pages_kernel(
    me_ref,
    lengths_hbm,
    table_hbm,
    cache_hbm,
    weight_hbm,
    hidden_hbm,
    gain_hbm,
    out_ref,
    held_ref,
    weight_ref,
    hidden_ref,
    gain_ref,
    length_ref,
    position_ref,
    lengths_ref,
    table_ref,
    rows_ref,
    sems,
):
    me = me_ref[0]
    core = me & 1
    group = me >> 3
    loads = [
        (lengths_hbm, lengths_ref),
        (table_hbm, rows_ref),
        (table_hbm, table_ref),
        (cache_hbm.at[0, 0], held_ref.at[0, 0]),
        (cache_hbm.at[1, 0], held_ref.at[1, 0]),
        (cache_hbm.at[0, 1], held_ref.at[0, 1]),
        (cache_hbm.at[1, 1], held_ref.at[1, 1]),
        (hidden_hbm, hidden_ref),
        (weight_hbm, weight_ref),
        (gain_hbm, gain_ref),
    ]
    loads = [pltpu.make_async_copy(src, dst, sems.at[i]) for i, (src, dst) in enumerate(loads)]
    for load in loads:
        load.start()
    for load in loads[:3]:
        load.wait()
    row = iota((BATCH, HEAD_DIM // 2), 0)
    spread_length = jnp.zeros((BATCH, HEAD_DIM // 2), F32)
    for r in range(BATCH):
        spread_length = jnp.where(row == r, lengths_ref[r].astype(F32), spread_length)
    length_ref[...] = spread_length
    pages = 2 * CHIPS
    table_row = iota((BATCH, pages), 0)
    lines = []
    for e in range(PER_GROUP):
        chosen_row = jnp.where(table_row == group * PER_GROUP + e, rows_ref[...], 0)
        lines.append(jnp.sum(chosen_row, axis=0, keepdims=True))
    blocks = jnp.where((iota((ROWS, 1), 0) & 1) == 0, lines[0], lines[1]).astype(F32).astype(BF16)
    spread = jnp.where(iota((pages, ROWS * pages), 1) >> 3 == iota((pages, ROWS * pages), 0), 1.0, 0.0)
    inside = iota((ROWS, ROWS * pages), 1) & 7
    position_ref[...] = nn_dot(blocks, spread.astype(BF16)).astype(jnp.int32) * ROWS + inside
    for e in range(PER_GROUP):
        for kv in range(2):
            loads[3 + 2 * e + kv].wait()

            def place(j, carry):
                block = table_ref[PER_GROUP * group + e, j]
                at = ((block & 1) ^ core) * PAGE_TILES + kv * 4 + e * 2
                page = held_ref[kv, e, j]
                out_ref[block >> 1, at] = page[:, :LANES]
                out_ref[block >> 1, at + 1] = page[:, LANES:]
                return carry

            lax.fori_loop(0, pages, place, 0, unroll=8)
    for load in loads[7:]:
        load.wait()


def qkv_kernel(
    me_ref, hidden_ref, gain_ref, own_ref, other_ref, cos_ref, sin_ref, buf_ref, out_ref, tile_ref, sem
):
    me = me_ref[0]
    first = (me & 1) == 0
    head = me >> 1
    x = hidden_ref[...]
    meansq = jnp.sum(x * x, axis=-1, keepdims=True) * (1.0 / D)
    normed = (x * lax.rsqrt(meansq + EPSILON) * (1.0 + gain_ref[0, 0:1, :])).astype(BF16)
    own = nt_dot(normed, own_ref[0]).astype(BF16).astype(F32)
    other = nt_dot(normed, other_ref[0]).astype(BF16).astype(F32)
    front = jnp.where(first, own, other)
    back = jnp.where(first, other, own)
    cosine = cos_ref[...]
    sine = sin_ref[...]
    turned = head < HEADS + KV_HEADS
    new_front = jnp.where(turned, front * cosine - back * sine, front)
    new_back = jnp.where(turned, back * cosine + front * sine, back)
    whole = jnp.concatenate([new_front, new_back], axis=1)
    for u in range(BATCH // ROWS):
        rows = whole[ROWS * u : ROWS * u + ROWS, :].astype(BF16)
        per = CHIPS * ROWS // BATCH
        tile_ref[per * u : per * u + per] = jnp.broadcast_to(rows[None], (per, ROWS, LANES))
    copy = pltpu.make_async_copy(tile_ref, out_ref.at[:, BULK_TILES - 1], sem)
    copy.start()
    copy.wait()


def attend_kernel(me_ref, lengths_ref, got_ref, position_ref, cache_ref, out_ref, leaving_ref, sem):
    leave = pltpu.make_async_copy(got_ref.at[:, PAGE_TILES : 2 * PAGE_TILES], leaving_ref, sem)
    leave.start()
    me = me_ref[0]
    group = me >> 3
    slot = me & 7
    rows_at = (group & 3) * PER_GROUP
    n_src = CHIPS * ROWS
    o = iota((32, n_src), 0)
    n = iota((32, n_src), 1)
    e = o & 1
    m = (o >> 1) & 3
    kind = o >> 3
    q_head = slot * 4 + m
    k_head = HEADS + slot * 2 + (m >> 1)
    v_head = k_head + KV_HEADS
    fix_head = HEADS + slot * 2 + (m & 1) + KV_HEADS * (m >> 1)
    chosen = jnp.where(kind == 0, q_head, jnp.where(kind == 1, k_head, jnp.where(kind == 2, v_head, fix_head)))
    pick = jnp.where(n == chosen * ROWS + rows_at + e, 1.0, 0.0).astype(BF16)
    source = got_ref[:, BULK_TILES - 1].astype(F32).reshape(n_src, LANES).astype(BF16)
    picked = nn_dot(pick, source)
    q = picked[0:8]
    new_k = picked[8:16]
    new_v = picked[16:24]
    q16 = q.astype(BF16)
    scale = (D / HEADS) ** (-0.5)
    row = iota((ROWS, 1), 0)
    scores = jnp.zeros((ROWS, 8 * 2 * CHIPS), F32)
    for ee in range(PER_GROUP):
        for a in range(2):
            keys = cache_ref[0, ee, :, a * LANES : a * LANES + LANES]
            part = nt_dot(q16, keys)
            scores = jnp.where(((row & 1) == ee) & ((row >> 2) == a), part, scores)
    limit = jnp.where((row & 1) == 0, lengths_ref[group * PER_GROUP], lengths_ref[group * PER_GROUP + 1])
    weights = jnp.where(position_ref[...] < limit, jnp.exp(capped(scores * scale)), 0.0)
    own = jnp.exp(capped(jnp.sum(q * new_k, axis=-1, keepdims=True) * scale))
    denominator = jnp.sum(weights, axis=-1, keepdims=True) + own
    w16 = weights.astype(BF16)
    numerator = own.astype(BF16).astype(F32) * new_v
    for ee in range(PER_GROUP):
        for a in range(2):
            values = cache_ref[1, ee, :, a * LANES : a * LANES + LANES]
            part = nn_dot(w16, values)
            numerator = numerator + jnp.where(((row & 1) == ee) & ((row >> 2) == a), part, 0.0)
    attended = numerator / denominator
    payload = jnp.concatenate([attended, picked[24:32]], axis=0).astype(BF16)
    out_ref[...] = jnp.broadcast_to(payload[None], (CHIPS, 2 * ROWS, LANES))
    leave.wait()


def mix_kernel(me_ref, own_ref, other_ref, weight_ref, out_ref):
    me = me_ref[0]
    first = (me & 1) == 0
    n_src = CHIPS * ROWS
    o = iota((n_src, n_src), 0)
    n = iota((n_src, n_src), 1)
    quarter = o >> 7
    m = (o >> 5) & 3
    group = (o >> 1) & 15
    source_row = (group * QUARTERS + quarter) * ROWS + m * 2 + (o & 1)
    pick = jnp.where(n == source_row, 1.0, 0.0).astype(BF16)
    own = own_ref[...][:, :ROWS].astype(F32)
    other = other_ref[...][:, :ROWS].astype(F32)
    mixed = jnp.zeros((BATCH, SHARE), F32)
    for c in range(2):
        mine = jnp.where(first, own, other) if c == 0 else jnp.where(first, other, own)
        rows = nn_dot(pick, mine.reshape(n_src, LANES).astype(BF16)).astype(BF16)
        left = jnp.concatenate([rows[BATCH * b : BATCH * b + BATCH] for b in range(16)], axis=1)
        right = jnp.concatenate(
            [weight_ref[0, :, (2 * y + c) * 512 : (2 * y + c) * 512 + 512] for y in range(QUARTERS)], axis=1
        )
        mixed = mixed + nt_dot(left, right)
    values = mixed.astype(BF16).astype(F32)
    gap = jnp.zeros((HALF, LANES // 2 - SHARE), F32)
    packed = jnp.concatenate([values[:HALF], gap, values[HALF:], gap], axis=1)
    turned = pltpu.roll(packed, (me * SHARE) % LANES, 1).astype(BF16)
    out_ref[...] = jnp.broadcast_to(turned[None], (CHIPS, HALF, LANES))


def window(low_ref, high_ref, j):
    lane = iota((HALF, LANES), 1)
    far = (lane + LANES // 2) % LANES
    v, off = divmod(j * SHARE, LANES)
    low = low_ref[v]
    high = high_ref[v]
    if off + SHARE > LANES:
        low = jnp.where(lane >= off, low, low_ref[v + 1])
        high = jnp.where(far >= off, high, high_ref[v + 1])
    return jnp.where((lane - off) % LANES < LANES // 2, low, high)


def ffn_kernel(
    me_ref,
    own_ref,
    other_ref,
    hidden_ref,
    gain_ref,
    gate_up_ref,
    down_ref,
    keep_ref,
    send_ref,
    stream_ref,
    wide_ref,
    low_ref,
    high_ref,
    ffn_ref,
):
    me = me_ref[0]
    first = (me & 1) == 0
    lane = iota((BATCH, LANES), 1)
    near = iota((HALF, LANES), 1)
    far = (near + LANES // 2) % LANES
    total = jnp.zeros((BATCH, LANES), F32)
    for v in range(BLOCKS):
        low = high = None
        for j in range((LANES * v) // SHARE, (LANES * v + LANES - 1) // SHARE + 1):
            own = own_ref[j >> 1]
            other = other_ref[j >> 1]
            piece = (jnp.where(first, own, other) if j % 2 == 0 else jnp.where(first, other, own)).astype(F32)
            start = j * SHARE - LANES * v
            low = piece if low is None else jnp.where(near >= start, piece, low)
            high = piece if high is None else jnp.where(far >= start, piece, high)
        block = jnp.concatenate([low, pltpu.roll(high, LANES // 2, 1)], axis=0)
        wide_ref[v] = block
        total = total + block * block
    scale = lax.rsqrt(jnp.sum(total, axis=-1, keepdims=True) * (1.0 / D) + EPSILON)
    total = jnp.zeros((BATCH, LANES), F32)
    for v in range(BLOCKS):
        cols = slice(LANES * v, LANES * v + LANES)
        block = hidden_ref[:, cols] + wide_ref[v] * scale * (1.0 + gain_ref[0, 1:2, cols])
        wide_ref[v] = block
        total = total + block * block
    scale = lax.rsqrt(jnp.sum(total, axis=-1, keepdims=True) * (1.0 / D) + EPSILON)
    for v in range(BLOCKS):
        cols = slice(LANES * v, LANES * v + LANES)
        ffn_ref[:, cols] = (wide_ref[v] * scale * (1.0 + gain_ref[0, 2:3, cols])).astype(BF16)
    ffn_in = ffn_ref[...]
    gate = nt_dot(ffn_in, gate_up_ref[0, 0])
    up = nt_dot(ffn_in, gate_up_ref[0, 1])
    active = (jax.nn.gelu(gate, approximate=True) * up).astype(BF16)
    for v in range(BLOCKS):
        block = nn_dot(active, down_ref[0, :, LANES * v : LANES * v + LANES])
        low_ref[v] = block[:HALF]
        high_ref[v] = pltpu.roll(block[HALF:], LANES // 2, 1)
    for p in range(CHIPS):
        even = window(low_ref, high_ref, 2 * p)
        odd = window(low_ref, high_ref, 2 * p + 1)
        keep_ref[p] = jnp.where(first, even, odd).astype(BF16)
        send_ref[p] = jnp.where(first, odd, even).astype(BF16)
    start = me * SHARE
    at = start // LANES
    off = start % LANES
    after = jnp.minimum(at + 1, BLOCKS - 1)
    stream_ref[...] = jnp.where(lane >= off, wide_ref[at], wide_ref[after])


def to_front(x, me):
    off = (me * SHARE) % LANES
    return pltpu.roll(x, (LANES - off) % LANES, 1)


def portion_kernel(me_ref, got_ref, portion_ref, square_ref):
    me = me_ref[0]
    total = jnp.zeros((HALF, LANES), F32)
    for p in range(CHIPS):
        total = total + got_ref[p].astype(F32)
    packed = to_front(total, me)
    mine = jnp.concatenate([packed, pltpu.roll(packed, LANES // 2, 1)], axis=0)
    portion_ref[...] = mine
    lane = iota((BATCH, LANES), 1)
    square = jnp.sum(jnp.where(lane < SHARE, mine * mine, 0.0), axis=-1, keepdims=True)
    line = jnp.sum(jnp.where(iota((BATCH, LANES), 0) == lane, square, 0.0), axis=0, keepdims=True)
    square_ref[...] = jnp.broadcast_to(line[None], (CHIPS, 1, LANES))


def finish_kernel(me_ref, portion_ref, stream_ref, own_ref, other_ref, gain_ref, out_ref):
    me = me_ref[0]
    squares = jnp.sum(own_ref[...] + other_ref[...], axis=0)
    lane = iota((BATCH, LANES), 1)
    column = jnp.sum(jnp.where(iota((BATCH, LANES), 0) == lane, squares, 0.0), axis=-1, keepdims=True)
    scale = lax.rsqrt(column * (1.0 / D) + EPSILON)
    at = (me * SHARE) // LANES
    after = jnp.minimum(at + 1, BLOCKS - 1)
    here = gain_ref[0, 3:4, pl.ds(pl.multiple_of(at * LANES, LANES), LANES)]
    there = gain_ref[0, 3:4, pl.ds(pl.multiple_of(after * LANES, LANES), LANES)]
    gain = jnp.where(lane >= (me * SHARE) % LANES, here, there)
    done = to_front(stream_ref[...], me) + portion_ref[...] * scale * (1.0 + to_front(gain, me))
    out_ref[...] = done[:, :SHARE]


def decode_kernel(me_ref, lengths_ref, got_ref, other_ref, own_new_ref, other_new_ref, out_ref):
    me = me_ref[0]
    core = me & 1

    def place(first_core):
        def body(g, carry):
            for y in range(QUARTERS):
                s = g * QUARTERS + y
                for side, ref in ((0, got_ref), (1, other_ref)):
                    slot = 2 * y + (first_core if side == 0 else 1 - first_core)
                    for kv in range(2):
                        for e in range(PER_GROUP):
                            for h in range(2):
                                cols = slice((2 * slot + h) * LANES, (2 * slot + h) * LANES + LANES)
                                out_ref[kv, g * PER_GROUP + e, :, cols] = ref[s, kv * 4 + e * 2 + h]
            return carry

        lax.fori_loop(0, GROUPS, body, 0)

    @pl.when(core == 0)
    def _():
        place(0)

    @pl.when(core == 1)
    def _():
        place(1)

    def fresh(r, carry):
        length = lengths_ref[r]

        @pl.when((length >> 3) == me)
        def _():
            g = r >> 1
            e = r & 1
            token = iota((ROWS, LANES), 0) == (length & 7)
            which = iota((2 * ROWS, LANES), 0)
            for y in range(QUARTERS):
                s = g * QUARTERS + y
                own = own_new_ref[s].astype(F32)
                other = other_new_ref[s].astype(F32)
                for c in range(2):
                    rows = jnp.where(core == c, own, other)
                    for kv in range(2):
                        for a in range(2):
                            at = ROWS + kv * 4 + a * 2 + e
                            line = jnp.sum(jnp.where(which == at, rows, 0.0), axis=0, keepdims=True)
                            slot = 2 * (2 * y + c) + a
                            cols = slice(slot * LANES, slot * LANES + LANES)
                            old = out_ref[kv, r, :, cols].astype(F32)
                            out_ref[kv, r, :, cols] = jnp.where(token, line, old).astype(BF16)

        return carry

    lax.fori_loop(0, BATCH, fresh, 0)


def core_swap(shard):
    return lax.ppermute(shard, "tp_2", [(0, 1), (1, 0)])


def to_chips(tiles):
    return lax.all_to_all(tiles, XY, 0, 0, tiled=True)


def pages_call(me, lengths, table, cache, weight, hidden, gains):
    fixed = [pltpu.with_memory_space_constraint(x, pltpu.HBM) for x in (lengths, table, cache, weight, hidden, gains)]
    return call(
        pages_kernel,
        (
            pltpu.VMEM((CHIPS, BULK_TILES, ROWS, LANES), BF16),
            pltpu.VMEM(cache.shape, BF16),
            pltpu.VMEM(weight.shape, BF16),
            pltpu.VMEM(hidden.shape, F32),
            pltpu.VMEM(gains.shape, F32),
            pltpu.VMEM((BATCH, HEAD_DIM // 2), F32),
            pltpu.VMEM((ROWS, ROWS * 2 * CHIPS), jnp.int32),
        ),
        [smem()] + [hbm()] * 6,
        (vmem(),) * 7,
        scratch_shapes=[
            pltpu.SMEM(lengths.shape, jnp.int32),
            pltpu.SMEM(table.shape, jnp.int32),
            pltpu.VMEM(table.shape, jnp.int32),
            pltpu.SemaphoreType.DMA((10,)),
        ],
    )(me, *fixed)


def qkv_call(me, hidden, gains, own, other, cosine, sine, buf):
    return call(
        qkv_kernel,
        shaped(buf.shape, BF16),
        [smem()] + [vmem()] * 6 + [pl.BlockSpec(memory_space=pl.ANY)],
        pl.BlockSpec(memory_space=pl.ANY),
        scratch_shapes=[pltpu.VMEM((CHIPS, ROWS, LANES), BF16), pltpu.SemaphoreType.DMA],
        input_output_aliases={7: 0},
    )(me, hidden, gains, own, other, cosine, sine, buf)


def attend_call(me, lengths, got, position, cache):
    return call(
        attend_kernel,
        (
            pltpu.VMEM((CHIPS, 2 * ROWS, LANES), BF16),
            pltpu.VMEM((CHIPS, PAGE_TILES, ROWS, LANES), BF16),
        ),
        [smem(), smem()] + [vmem()] * 3,
        (vmem(), vmem()),
        scratch_shapes=[pltpu.SemaphoreType.DMA],
    )(me, lengths, got, position, cache)


def mix_call(me, own, other, weight):
    return call(mix_kernel, shaped((CHIPS, HALF, LANES), BF16), [smem()] + [vmem()] * 3, vmem())(me, own, other, weight)


def ffn_call(me, own, other, hidden, gains, gate_up, down):
    wide = shaped((CHIPS, HALF, LANES), BF16)
    return call(
        ffn_kernel,
        (wide, wide, shaped((BATCH, LANES), F32)),
        [smem()] + [vmem()] * 6,
        (vmem(), vmem(), vmem()),
        scratch_shapes=[
            pltpu.VMEM((BLOCKS, BATCH, LANES), F32),
            pltpu.VMEM((BLOCKS, HALF, LANES), F32),
            pltpu.VMEM((BLOCKS, HALF, LANES), F32),
            pltpu.VMEM((BATCH, D), BF16),
        ],
    )(me, own, other, hidden, gains, gate_up, down)


def portion_call(me, got):
    return call(
        portion_kernel,
        (shaped((BATCH, LANES), F32), shaped((CHIPS, 1, LANES), F32)),
        [smem(), vmem()],
        (vmem(), vmem()),
    )(me, got)


def finish_call(me, portion, stream, own, other, gains):
    return call(finish_kernel, shaped((BATCH, SHARE), F32), [smem()] + [vmem()] * 5, vmem())(
        me, portion, stream, own, other, gains
    )


def decode_call(me, lengths, got, other, own_new, other_new):
    return call(
        decode_kernel, pltpu.VMEM((2, BATCH, ROWS, KV_HEADS * HEAD_DIM), BF16), [smem(), smem()] + [vmem()] * 4, vmem()
    )(me, lengths, got, other, own_new, other_new)


def rope_tables(spread_length):
    half_dim = HEAD_DIM // 2
    exponent = jnp.arange(half_dim, dtype=F32) * (-2.0 / HEAD_DIM)
    angles = spread_length * jnp.power(jnp.float32(10000.0), exponent)
    return jnp.cos(angles), jnp.sin(angles)


def on_device(
    hidden_in,
    prefill_cache,
    lengths,
    page_table,
    qkv_weight,
    out_weight,
    gate_up_weight,
    down_weight,
    norm_gains,
):
    me = jnp.full((1,), lax.axis_index(TP), jnp.int32)
    other_rows = core_swap(qkv_weight)
    buf, held, own_rows, hidden, gains, spread_length, position = pages_call(
        me, lengths, page_table, prefill_cache[0, 0], qkv_weight, hidden_in, norm_gains
    )
    cosine, sine = rope_tables(spread_length)
    buf = qkv_call(me, hidden, gains, own_rows, other_rows, cosine, sine, buf)
    got = to_chips(buf)
    payload, leaving = attend_call(
        me, lengths, got, position, held.reshape(2, PER_GROUP, -1, 2 * HEAD_DIM)
    )
    own_att = to_chips(payload)
    other_att = core_swap(own_att)
    other_pages = core_swap(leaving)
    payload = mix_call(me, own_att, other_att, out_weight)
    own_mix = to_chips(payload)
    other_mix = core_swap(own_mix)
    keep, send, stream = ffn_call(me, own_mix, other_mix, hidden, gains, gate_up_weight, down_weight)
    sent = core_swap(send)
    chip = (keep.astype(F32) + sent.astype(F32)).astype(BF16)
    got_branch = to_chips(chip)
    portion, square = portion_call(me, got_branch)
    squares = to_chips(square)
    result = finish_call(me, portion, stream, squares, core_swap(squares), gains)
    decoded = decode_call(me, lengths, got, other_pages, own_att, other_att)
    return result, decoded[None, None]


def solution(mesh):
    torus = Mesh(mesh.devices.reshape(mesh.shape["grp"], 8, 8, 2), ("grp", "tp_0", "tp_1", "tp_2"))
    return jax.shard_map(
        on_device,
        mesh=torus,
        in_specs=(
            P("grp", None),
            P(TP, None, None, "grp", None, None, None),
            P("grp"),
            P("grp", None),
            P(None, TP, None),
            P(None, TP, None),
            P(None, None, TP, None),
            P(None, TP, None),
            P(),
        ),
        out_specs=(P("grp", TP), P(TP, None, None, "grp", None, None)),
        check_vma=False,
    )
```

```python
import jax
import jax.numpy as jnp
from jax import lax
from jax.experimental import pallas as pl
from jax.experimental.pallas import tpu as pltpu
from jax.sharding import Mesh
from jax.sharding import PartitionSpec as P

D = 4608
HEADS = 32
KV_HEADS = 16
HEAD_DIM = 128
PREFILL_TP = 8
TP = ("tp_0", "tp_1", "tp_2")
XY = ("tp_0", "tp_1")

EPSILON = 1e-06
SOFTCAP = 50.0
LANES = 128
ROWS = 8
BF16 = jnp.bfloat16
F32 = jnp.float32

CHIPS = 64
QUARTERS = PREFILL_TP // 2
GROUPS = CHIPS // QUARTERS
SHARE = D // (2 * CHIPS)
BLOCKS = D // LANES
BATCH = 32
HALF = BATCH // 2
PER_GROUP = 2
PAGE_TILES = 2 * PER_GROUP * 2
BULK_TILES = 2 * PAGE_TILES + 1
VMEM_LIMIT = 24 * 1024 * 1024


def smem():
    return pl.BlockSpec(memory_space=pltpu.SMEM)


def vmem():
    return pl.BlockSpec(memory_space=pltpu.VMEM)


def hbm():
    return pl.BlockSpec(memory_space=pltpu.HBM)


def call(kernel, out_shape, in_specs, out_specs, **more):
    return pl.pallas_call(
        kernel,
        out_shape=out_shape,
        in_specs=in_specs,
        out_specs=out_specs,
        compiler_params=pltpu.CompilerParams(vmem_limit_bytes=VMEM_LIMIT),
        **more,
    )


def shaped(shape, dtype):
    return jax.ShapeDtypeStruct(shape, dtype)


def nt_dot(left, right):
    return lax.dot_general(left, right, (((1,), (1,)), ((), ())), preferred_element_type=F32)


def nn_dot(left, right):
    return lax.dot_general(left, right, (((1,), (0,)), ((), ())), preferred_element_type=F32)


def iota(shape, dim):
    return lax.broadcasted_iota(jnp.int32, shape, dim)


def bulk_place(chip):
    return ((chip & 7) << 3) | (chip >> 3)


def capped(raw_scores):
    return SOFTCAP * jnp.tanh(raw_scores / SOFTCAP)


def pages_kernel(
    me_ref,
    lengths_hbm,
    table_hbm,
    cache_hbm,
    weight_hbm,
    hidden_hbm,
    gain_hbm,
    out_ref,
    held_ref,
    weight_ref,
    hidden_ref,
    gain_ref,
    length_ref,
    position_ref,
    lengths_ref,
    table_ref,
    rows_ref,
    sems,
):
    me = me_ref[0]
    core = me & 1
    group = me >> 3
    loads = [
        (lengths_hbm, lengths_ref),
        (table_hbm, rows_ref),
        (table_hbm, table_ref),
        (cache_hbm.at[0, 0], held_ref.at[0, 0]),
        (cache_hbm.at[1, 0], held_ref.at[1, 0]),
        (cache_hbm.at[0, 1], held_ref.at[0, 1]),
        (cache_hbm.at[1, 1], held_ref.at[1, 1]),
        (hidden_hbm, hidden_ref),
        (weight_hbm, weight_ref),
        (gain_hbm, gain_ref),
    ]
    loads = [pltpu.make_async_copy(src, dst, sems.at[i]) for i, (src, dst) in enumerate(loads)]
    for load in loads:
        load.start()
    for load in loads[:3]:
        load.wait()
    row = iota((BATCH, HEAD_DIM // 2), 0)
    spread_length = jnp.zeros((BATCH, HEAD_DIM // 2), F32)
    for r in range(BATCH):
        spread_length = jnp.where(row == r, lengths_ref[r].astype(F32), spread_length)
    length_ref[...] = spread_length
    pages = 2 * CHIPS
    table_row = iota((BATCH, pages), 0)
    lines = []
    for e in range(PER_GROUP):
        chosen_row = jnp.where(table_row == group * PER_GROUP + e, rows_ref[...], 0)
        lines.append(jnp.sum(chosen_row, axis=0, keepdims=True))
    blocks = jnp.where((iota((ROWS, 1), 0) & 1) == 0, lines[0], lines[1]).astype(F32).astype(BF16)
    spread = jnp.where(iota((pages, ROWS * pages), 1) >> 3 == iota((pages, ROWS * pages), 0), 1.0, 0.0)
    inside = iota((ROWS, ROWS * pages), 1) & 7
    position_ref[...] = nn_dot(blocks, spread.astype(BF16)).astype(jnp.int32) * ROWS + inside
    for e in range(PER_GROUP):
        for kv in range(2):
            loads[3 + 2 * e + kv].wait()

            def place(j, carry):
                block = table_ref[PER_GROUP * group + e, j]
                at = ((block & 1) ^ core) * PAGE_TILES + kv * 4 + e * 2
                page = held_ref[kv, e, j]
                chip = bulk_place(block >> 1)
                out_ref[chip, at] = page[:, :LANES]
                out_ref[chip, at + 1] = page[:, LANES:]
                return carry

            lax.fori_loop(0, pages, place, 0, unroll=8)
    for load in loads[7:]:
        load.wait()


def qkv_kernel(
    me_ref, hidden_ref, gain_ref, own_ref, other_ref, cos_ref, sin_ref, buf_ref, out_ref, tile_ref, sem
):
    me = me_ref[0]
    first = (me & 1) == 0
    head = me >> 1
    x = hidden_ref[...]
    meansq = jnp.sum(x * x, axis=-1, keepdims=True) * (1.0 / D)
    normed = (x * lax.rsqrt(meansq + EPSILON) * (1.0 + gain_ref[0, 0:1, :])).astype(BF16)
    own = nt_dot(normed, own_ref[0]).astype(BF16).astype(F32)
    other = nt_dot(normed, other_ref[0]).astype(BF16).astype(F32)
    front = jnp.where(first, own, other)
    back = jnp.where(first, other, own)
    cosine = cos_ref[...]
    sine = sin_ref[...]
    turned = head < HEADS + KV_HEADS
    new_front = jnp.where(turned, front * cosine - back * sine, front)
    new_back = jnp.where(turned, back * cosine + front * sine, back)
    whole = jnp.concatenate([new_front, new_back], axis=1)
    rows = [whole[ROWS * u : ROWS * u + ROWS, :].astype(BF16) for u in range(BATCH // ROWS)]
    for chip in range(CHIPS):
        tile_ref[bulk_place(chip)] = rows[chip * BATCH // (CHIPS * ROWS)]
    copy = pltpu.make_async_copy(tile_ref, out_ref.at[:, BULK_TILES - 1], sem)
    copy.start()
    copy.wait()


def attend_kernel(me_ref, lengths_ref, got_ref, position_ref, cache_ref, out_ref, leaving_ref, sem):
    leave = pltpu.make_async_copy(got_ref.at[:, PAGE_TILES : 2 * PAGE_TILES], leaving_ref, sem)
    leave.start()
    me = me_ref[0]
    group = me >> 3
    slot = me & 7
    rows_at = (group & 3) * PER_GROUP
    n_src = CHIPS * ROWS
    o = iota((32, n_src), 0)
    n = iota((32, n_src), 1)
    e = o & 1
    m = (o >> 1) & 3
    kind = o >> 3
    q_head = slot * 4 + m
    k_head = HEADS + slot * 2 + (m >> 1)
    v_head = k_head + KV_HEADS
    fix_head = HEADS + slot * 2 + (m & 1) + KV_HEADS * (m >> 1)
    chosen = jnp.where(kind == 0, q_head, jnp.where(kind == 1, k_head, jnp.where(kind == 2, v_head, fix_head)))
    pick = jnp.where(n == bulk_place(chosen) * ROWS + rows_at + e, 1.0, 0.0).astype(BF16)
    source = got_ref[:, BULK_TILES - 1].astype(F32).reshape(n_src, LANES).astype(BF16)
    picked = nn_dot(pick, source)
    q = picked[0:8]
    new_k = picked[8:16]
    new_v = picked[16:24]
    q16 = q.astype(BF16)
    scale = (D / HEADS) ** (-0.5)
    row = iota((ROWS, 1), 0)
    scores = jnp.zeros((ROWS, 8 * 2 * CHIPS), F32)
    for ee in range(PER_GROUP):
        for a in range(2):
            keys = cache_ref[0, ee, :, a * LANES : a * LANES + LANES]
            part = nt_dot(q16, keys)
            scores = jnp.where(((row & 1) == ee) & ((row >> 2) == a), part, scores)
    limit = jnp.where((row & 1) == 0, lengths_ref[group * PER_GROUP], lengths_ref[group * PER_GROUP + 1])
    weights = jnp.where(position_ref[...] < limit, jnp.exp(capped(scores * scale)), 0.0)
    own = jnp.exp(capped(jnp.sum(q * new_k, axis=-1, keepdims=True) * scale))
    denominator = jnp.sum(weights, axis=-1, keepdims=True) + own
    w16 = weights.astype(BF16)
    numerator = own.astype(BF16).astype(F32) * new_v
    for ee in range(PER_GROUP):
        for a in range(2):
            values = cache_ref[1, ee, :, a * LANES : a * LANES + LANES]
            part = nn_dot(w16, values)
            numerator = numerator + jnp.where(((row & 1) == ee) & ((row >> 2) == a), part, 0.0)
    attended = numerator / denominator
    payload = jnp.concatenate([attended, picked[24:32]], axis=0).astype(BF16)
    out_ref[...] = jnp.broadcast_to(payload[None], (CHIPS, 2 * ROWS, LANES))
    leave.wait()


def mix_kernel(me_ref, own_ref, other_ref, weight_ref, out_ref):
    me = me_ref[0]
    first = (me & 1) == 0
    n_src = CHIPS * ROWS
    o = iota((n_src, n_src), 0)
    n = iota((n_src, n_src), 1)
    quarter = o >> 7
    m = (o >> 5) & 3
    group = (o >> 1) & 15
    source_row = (group * QUARTERS + quarter) * ROWS + m * 2 + (o & 1)
    pick = jnp.where(n == source_row, 1.0, 0.0).astype(BF16)
    own = own_ref[...][:, :ROWS].astype(F32)
    other = other_ref[...][:, :ROWS].astype(F32)
    mixed = jnp.zeros((BATCH, SHARE), F32)
    for c in range(2):
        mine = jnp.where(first, own, other) if c == 0 else jnp.where(first, other, own)
        rows = nn_dot(pick, mine.reshape(n_src, LANES).astype(BF16)).astype(BF16)
        left = jnp.concatenate([rows[BATCH * b : BATCH * b + BATCH] for b in range(16)], axis=1)
        right = jnp.concatenate(
            [weight_ref[0, :, (2 * y + c) * 512 : (2 * y + c) * 512 + 512] for y in range(QUARTERS)], axis=1
        )
        mixed = mixed + nt_dot(left, right)
    values = mixed.astype(BF16).astype(F32)
    gap = jnp.zeros((HALF, LANES // 2 - SHARE), F32)
    packed = jnp.concatenate([values[:HALF], gap, values[HALF:], gap], axis=1)
    turned = pltpu.roll(packed, (me * SHARE) % LANES, 1).astype(BF16)
    out_ref[...] = jnp.broadcast_to(turned[None], (CHIPS, HALF, LANES))


def window(low_ref, high_ref, j):
    lane = iota((HALF, LANES), 1)
    far = (lane + LANES // 2) % LANES
    v, off = divmod(j * SHARE, LANES)
    low = low_ref[v]
    high = high_ref[v]
    if off + SHARE > LANES:
        low = jnp.where(lane >= off, low, low_ref[v + 1])
        high = jnp.where(far >= off, high, high_ref[v + 1])
    return jnp.where((lane - off) % LANES < LANES // 2, low, high)


def ffn_kernel(
    me_ref,
    own_ref,
    other_ref,
    hidden_ref,
    gain_ref,
    gate_up_ref,
    down_ref,
    keep_ref,
    send_ref,
    stream_ref,
    wide_ref,
    low_ref,
    high_ref,
    ffn_ref,
):
    me = me_ref[0]
    first = (me & 1) == 0
    lane = iota((BATCH, LANES), 1)
    near = iota((HALF, LANES), 1)
    far = (near + LANES // 2) % LANES
    total = jnp.zeros((BATCH, LANES), F32)
    for v in range(BLOCKS):
        low = high = None
        for j in range((LANES * v) // SHARE, (LANES * v + LANES - 1) // SHARE + 1):
            own = own_ref[j >> 1]
            other = other_ref[j >> 1]
            piece = (jnp.where(first, own, other) if j % 2 == 0 else jnp.where(first, other, own)).astype(F32)
            start = j * SHARE - LANES * v
            low = piece if low is None else jnp.where(near >= start, piece, low)
            high = piece if high is None else jnp.where(far >= start, piece, high)
        block = jnp.concatenate([low, pltpu.roll(high, LANES // 2, 1)], axis=0)
        wide_ref[v] = block
        total = total + block * block
    scale = lax.rsqrt(jnp.sum(total, axis=-1, keepdims=True) * (1.0 / D) + EPSILON)
    total = jnp.zeros((BATCH, LANES), F32)
    for v in range(BLOCKS):
        cols = slice(LANES * v, LANES * v + LANES)
        block = hidden_ref[:, cols] + wide_ref[v] * scale * (1.0 + gain_ref[0, 1:2, cols])
        wide_ref[v] = block
        total = total + block * block
    scale = lax.rsqrt(jnp.sum(total, axis=-1, keepdims=True) * (1.0 / D) + EPSILON)
    for v in range(BLOCKS):
        cols = slice(LANES * v, LANES * v + LANES)
        ffn_ref[:, cols] = (wide_ref[v] * scale * (1.0 + gain_ref[0, 2:3, cols])).astype(BF16)
    ffn_in = ffn_ref[...]
    gate = nt_dot(ffn_in, gate_up_ref[0, 0])
    up = nt_dot(ffn_in, gate_up_ref[0, 1])
    active = (jax.nn.gelu(gate, approximate=True) * up).astype(BF16)
    for v in range(BLOCKS):
        block = nn_dot(active, down_ref[0, :, LANES * v : LANES * v + LANES])
        low_ref[v] = block[:HALF]
        high_ref[v] = pltpu.roll(block[HALF:], LANES // 2, 1)
    for p in range(CHIPS):
        even = window(low_ref, high_ref, 2 * p)
        odd = window(low_ref, high_ref, 2 * p + 1)
        keep_ref[p] = jnp.where(first, even, odd).astype(BF16)
        send_ref[p] = jnp.where(first, odd, even).astype(BF16)
    start = me * SHARE
    at = start // LANES
    off = start % LANES
    after = jnp.minimum(at + 1, BLOCKS - 1)
    stream_ref[...] = jnp.where(lane >= off, wide_ref[at], wide_ref[after])


def to_front(x, me):
    off = (me * SHARE) % LANES
    return pltpu.roll(x, (LANES - off) % LANES, 1)


def portion_kernel(me_ref, got_ref, portion_ref, square_ref):
    me = me_ref[0]
    total = jnp.zeros((HALF, LANES), F32)
    for p in range(CHIPS):
        total = total + got_ref[p].astype(F32)
    packed = to_front(total, me)
    mine = jnp.concatenate([packed, pltpu.roll(packed, LANES // 2, 1)], axis=0)
    portion_ref[...] = mine
    lane = iota((BATCH, LANES), 1)
    square = jnp.sum(jnp.where(lane < SHARE, mine * mine, 0.0), axis=-1, keepdims=True)
    line = jnp.sum(jnp.where(iota((BATCH, LANES), 0) == lane, square, 0.0), axis=0, keepdims=True)
    square_ref[...] = jnp.broadcast_to(line[None], (CHIPS, 1, LANES))


def finish_kernel(me_ref, portion_ref, stream_ref, own_ref, other_ref, gain_ref, out_ref):
    me = me_ref[0]
    squares = jnp.sum(own_ref[...] + other_ref[...], axis=0)
    lane = iota((BATCH, LANES), 1)
    column = jnp.sum(jnp.where(iota((BATCH, LANES), 0) == lane, squares, 0.0), axis=-1, keepdims=True)
    scale = lax.rsqrt(column * (1.0 / D) + EPSILON)
    at = (me * SHARE) // LANES
    after = jnp.minimum(at + 1, BLOCKS - 1)
    here = gain_ref[0, 3:4, pl.ds(pl.multiple_of(at * LANES, LANES), LANES)]
    there = gain_ref[0, 3:4, pl.ds(pl.multiple_of(after * LANES, LANES), LANES)]
    gain = jnp.where(lane >= (me * SHARE) % LANES, here, there)
    done = to_front(stream_ref[...], me) + portion_ref[...] * scale * (1.0 + to_front(gain, me))
    out_ref[...] = done[:, :SHARE]


def decode_kernel(me_ref, lengths_ref, got_ref, other_ref, own_new_ref, other_new_ref, out_ref):
    me = me_ref[0]
    core = me & 1

    def place(first_core):
        def body(g, carry):
            for y in range(QUARTERS):
                s = bulk_place(g * QUARTERS + y)
                for side, ref in ((0, got_ref), (1, other_ref)):
                    slot = 2 * y + (first_core if side == 0 else 1 - first_core)
                    for kv in range(2):
                        for e in range(PER_GROUP):
                            for h in range(2):
                                cols = slice((2 * slot + h) * LANES, (2 * slot + h) * LANES + LANES)
                                out_ref[kv, g * PER_GROUP + e, :, cols] = ref[s, kv * 4 + e * 2 + h]
            return carry

        lax.fori_loop(0, GROUPS, body, 0)

    @pl.when(core == 0)
    def _():
        place(0)

    @pl.when(core == 1)
    def _():
        place(1)

    def fresh(r, carry):
        length = lengths_ref[r]

        @pl.when((length >> 3) == me)
        def _():
            g = r >> 1
            e = r & 1
            token = iota((ROWS, LANES), 0) == (length & 7)
            which = iota((2 * ROWS, LANES), 0)
            for y in range(QUARTERS):
                s = g * QUARTERS + y
                own = own_new_ref[s].astype(F32)
                other = other_new_ref[s].astype(F32)
                for c in range(2):
                    rows = jnp.where(core == c, own, other)
                    for kv in range(2):
                        for a in range(2):
                            at = ROWS + kv * 4 + a * 2 + e
                            line = jnp.sum(jnp.where(which == at, rows, 0.0), axis=0, keepdims=True)
                            slot = 2 * (2 * y + c) + a
                            cols = slice(slot * LANES, slot * LANES + LANES)
                            old = out_ref[kv, r, :, cols].astype(F32)
                            out_ref[kv, r, :, cols] = jnp.where(token, line, old).astype(BF16)

        return carry

    lax.fori_loop(0, BATCH, fresh, 0)


def core_swap(shard):
    return lax.ppermute(shard, "tp_2", [(0, 1), (1, 0)])


def to_chips(tiles):
    return lax.all_to_all(tiles, XY, 0, 0, tiled=True)


def pages_call(me, lengths, table, cache, weight, hidden, gains):
    fixed = [pltpu.with_memory_space_constraint(x, pltpu.HBM) for x in (lengths, table, cache, weight, hidden, gains)]
    return call(
        pages_kernel,
        (
            pltpu.VMEM((CHIPS, BULK_TILES, ROWS, LANES), BF16),
            pltpu.VMEM(cache.shape, BF16),
            pltpu.VMEM(weight.shape, BF16),
            pltpu.VMEM(hidden.shape, F32),
            pltpu.VMEM(gains.shape, F32),
            pltpu.VMEM((BATCH, HEAD_DIM // 2), F32),
            pltpu.VMEM((ROWS, ROWS * 2 * CHIPS), jnp.int32),
        ),
        [smem()] + [hbm()] * 6,
        (vmem(),) * 7,
        scratch_shapes=[
            pltpu.SMEM(lengths.shape, jnp.int32),
            pltpu.SMEM(table.shape, jnp.int32),
            pltpu.VMEM(table.shape, jnp.int32),
            pltpu.SemaphoreType.DMA((10,)),
        ],
    )(me, *fixed)


def qkv_call(me, hidden, gains, own, other, cosine, sine, buf):
    return call(
        qkv_kernel,
        shaped(buf.shape, BF16),
        [smem()] + [vmem()] * 6 + [pl.BlockSpec(memory_space=pl.ANY)],
        pl.BlockSpec(memory_space=pl.ANY),
        scratch_shapes=[pltpu.VMEM((CHIPS, ROWS, LANES), BF16), pltpu.SemaphoreType.DMA],
        input_output_aliases={7: 0},
    )(me, hidden, gains, own, other, cosine, sine, buf)


def attend_call(me, lengths, got, position, cache):
    return call(
        attend_kernel,
        (
            pltpu.VMEM((CHIPS, 2 * ROWS, LANES), BF16),
            pltpu.VMEM((CHIPS, PAGE_TILES, ROWS, LANES), BF16),
        ),
        [smem(), smem()] + [vmem()] * 3,
        (vmem(), vmem()),
        scratch_shapes=[pltpu.SemaphoreType.DMA],
    )(me, lengths, got, position, cache)


def mix_call(me, own, other, weight):
    return call(mix_kernel, shaped((CHIPS, HALF, LANES), BF16), [smem()] + [vmem()] * 3, vmem())(me, own, other, weight)


def ffn_call(me, own, other, hidden, gains, gate_up, down):
    wide = shaped((CHIPS, HALF, LANES), BF16)
    return call(
        ffn_kernel,
        (wide, wide, shaped((BATCH, LANES), F32)),
        [smem()] + [vmem()] * 6,
        (vmem(), vmem(), vmem()),
        scratch_shapes=[
            pltpu.VMEM((BLOCKS, BATCH, LANES), F32),
            pltpu.VMEM((BLOCKS, HALF, LANES), F32),
            pltpu.VMEM((BLOCKS, HALF, LANES), F32),
            pltpu.VMEM((BATCH, D), BF16),
        ],
    )(me, own, other, hidden, gains, gate_up, down)


def portion_call(me, got):
    return call(
        portion_kernel,
        (shaped((BATCH, LANES), F32), shaped((CHIPS, 1, LANES), F32)),
        [smem(), vmem()],
        (vmem(), vmem()),
    )(me, got)


def finish_call(me, portion, stream, own, other, gains):
    return call(finish_kernel, shaped((BATCH, SHARE), F32), [smem()] + [vmem()] * 5, vmem())(
        me, portion, stream, own, other, gains
    )


def decode_call(me, lengths, got, other, own_new, other_new):
    return call(
        decode_kernel, pltpu.VMEM((2, BATCH, ROWS, KV_HEADS * HEAD_DIM), BF16), [smem(), smem()] + [vmem()] * 4, vmem()
    )(me, lengths, got, other, own_new, other_new)


def rope_tables(spread_length):
    half_dim = HEAD_DIM // 2
    exponent = jnp.arange(half_dim, dtype=F32) * (-2.0 / HEAD_DIM)
    angles = spread_length * jnp.power(jnp.float32(10000.0), exponent)
    return jnp.cos(angles), jnp.sin(angles)


def on_device(
    hidden_in,
    prefill_cache,
    lengths,
    page_table,
    qkv_weight,
    out_weight,
    gate_up_weight,
    down_weight,
    norm_gains,
):
    me = jnp.full((1,), lax.axis_index(TP), jnp.int32)
    other_rows = core_swap(qkv_weight)
    buf, held, own_rows, hidden, gains, spread_length, position = pages_call(
        me, lengths, page_table, prefill_cache[0, 0], qkv_weight, hidden_in, norm_gains
    )
    cosine, sine = rope_tables(spread_length)
    buf = qkv_call(me, hidden, gains, own_rows, other_rows, cosine, sine, buf)
    got = lax.all_to_all(buf, XY[::-1], 0, 0, tiled=True)
    payload, leaving = attend_call(
        me, lengths, got, position, held.reshape(2, PER_GROUP, -1, 2 * HEAD_DIM)
    )
    own_att = to_chips(payload)
    other_att = core_swap(own_att)
    other_pages = core_swap(leaving)
    payload = mix_call(me, own_att, other_att, out_weight)
    own_mix = to_chips(payload)
    other_mix = core_swap(own_mix)
    keep, send, stream = ffn_call(me, own_mix, other_mix, hidden, gains, gate_up_weight, down_weight)
    sent = core_swap(send)
    chip = (keep.astype(F32) + sent.astype(F32)).astype(BF16)
    got_branch = to_chips(chip)
    portion, square = portion_call(me, got_branch)
    squares = to_chips(square)
    result = finish_call(me, portion, stream, squares, core_swap(squares), gains)
    decoded = decode_call(me, lengths, got, other_pages, own_att, other_att)
    return result, decoded[None, None]


def solution(mesh):
    torus = Mesh(mesh.devices.reshape(mesh.shape["grp"], 8, 8, 2), ("grp", "tp_0", "tp_1", "tp_2"))
    return jax.shard_map(
        on_device,
        mesh=torus,
        in_specs=(
            P("grp", None),
            P(TP, None, None, "grp", None, None, None),
            P("grp"),
            P("grp", None),
            P(None, TP, None),
            P(None, TP, None),
            P(None, None, TP, None),
            P(None, TP, None),
            P(),
        ),
        out_specs=(P("grp", TP), P(TP, None, None, "grp", None, None)),
        check_vma=False,
    )
```

```python
import jax
import jax.numpy as jnp
from jax import lax
from jax.experimental import pallas as pl
from jax.experimental.pallas import tpu as pltpu
from jax.sharding import Mesh
from jax.sharding import PartitionSpec as P

D = 4608
HEADS = 32
KV_HEADS = 16
HEAD_DIM = 128
PREFILL_TP = 8
TP = ("tp_0", "tp_1", "tp_2")
XY = ("tp_0", "tp_1")

EPSILON = 1e-06
SOFTCAP = 50.0
LANES = 128
ROWS = 8
BF16 = jnp.bfloat16
F32 = jnp.float32

CHIPS = 64
QUARTERS = PREFILL_TP // 2
GROUPS = CHIPS // QUARTERS
SHARE = D // (2 * CHIPS)
BLOCKS = D // LANES
BATCH = 32
HALF = BATCH // 2
PER_GROUP = 2
PAGE_TILES = 2 * PER_GROUP * 2
BULK_TILES = 2 * PAGE_TILES + 1
VMEM_LIMIT = 24 * 1024 * 1024


def smem():
    return pl.BlockSpec(memory_space=pltpu.SMEM)


def vmem():
    return pl.BlockSpec(memory_space=pltpu.VMEM)


def hbm():
    return pl.BlockSpec(memory_space=pltpu.HBM)


def call(kernel, out_shape, in_specs, out_specs, **more):
    return pl.pallas_call(
        kernel,
        out_shape=out_shape,
        in_specs=in_specs,
        out_specs=out_specs,
        compiler_params=pltpu.CompilerParams(vmem_limit_bytes=VMEM_LIMIT),
        **more,
    )


def shaped(shape, dtype):
    return jax.ShapeDtypeStruct(shape, dtype)


def nt_dot(left, right):
    return lax.dot_general(left, right, (((1,), (1,)), ((), ())), preferred_element_type=F32)


def nn_dot(left, right):
    return lax.dot_general(left, right, (((1,), (0,)), ((), ())), preferred_element_type=F32)


def iota(shape, dim):
    return lax.broadcasted_iota(jnp.int32, shape, dim)


def bulk_place(chip):
    return ((chip & 7) << 3) | (chip >> 3)


def capped(raw_scores):
    return SOFTCAP * jnp.tanh(raw_scores / SOFTCAP)


def pages_kernel(
    me_ref,
    lengths_hbm,
    table_hbm,
    cache_hbm,
    weight_hbm,
    hidden_hbm,
    gain_hbm,
    out_ref,
    held_ref,
    weight_ref,
    hidden_ref,
    gain_ref,
    length_ref,
    position_ref,
    lengths_ref,
    table_ref,
    rows_ref,
    sems,
):
    me = me_ref[0]
    core = me & 1
    group = me >> 3
    loads = [
        (lengths_hbm, lengths_ref),
        (table_hbm, rows_ref),
        (table_hbm, table_ref),
        *[
            (cache_hbm.at[:, e, pl.ds(CHIPS * half, CHIPS)], held_ref.at[:, e, pl.ds(CHIPS * half, CHIPS)])
            for e in range(PER_GROUP)
            for half in range(2)
        ],
        (hidden_hbm, hidden_ref),
        (weight_hbm, weight_ref),
        (gain_hbm, gain_ref),
    ]
    loads = [pltpu.make_async_copy(src, dst, sems.at[i]) for i, (src, dst) in enumerate(loads)]
    for load in loads:
        load.start()
    for load in loads[:3]:
        load.wait()
    row = iota((BATCH, HEAD_DIM // 2), 0)
    spread_length = jnp.zeros((BATCH, HEAD_DIM // 2), F32)
    for r in range(BATCH):
        spread_length = jnp.where(row == r, lengths_ref[r].astype(F32), spread_length)
    length_ref[...] = spread_length
    pages = 2 * CHIPS
    table_row = iota((BATCH, pages), 0)
    lines = []
    for e in range(PER_GROUP):
        chosen_row = jnp.where(table_row == group * PER_GROUP + e, rows_ref[...], 0)
        lines.append(jnp.sum(chosen_row, axis=0, keepdims=True))
    blocks = jnp.where((iota((ROWS, 1), 0) & 1) == 0, lines[0], lines[1]).astype(F32).astype(BF16)
    spread = jnp.where(iota((pages, ROWS * pages), 1) >> 3 == iota((pages, ROWS * pages), 0), 1.0, 0.0)
    inside = iota((ROWS, ROWS * pages), 1) & 7
    position_ref[...] = nn_dot(blocks, spread.astype(BF16)).astype(jnp.int32) * ROWS + inside
    for e in range(PER_GROUP):
        for half in range(2):
            loads[3 + 2 * e + half].wait()

            def place(j, carry):
                block = table_ref[PER_GROUP * group + e, j]
                chip = bulk_place(block >> 1)
                at = ((block & 1) ^ core) * PAGE_TILES + e * 2
                for kv in range(2):
                    page = held_ref[kv, e, j]
                    out_ref[chip, at + kv * 4] = page[:, :LANES]
                    out_ref[chip, at + kv * 4 + 1] = page[:, LANES:]
                return carry

            lax.fori_loop(CHIPS * half, CHIPS * half + CHIPS, place, 0, unroll=8)
    for load in loads[7:]:
        load.wait()


def qkv_kernel(
    me_ref, hidden_ref, gain_ref, own_ref, other_ref, cos_ref, sin_ref, buf_ref, out_ref, tile_ref, sem
):
    me = me_ref[0]
    first = (me & 1) == 0
    head = me >> 1
    x = hidden_ref[...]
    meansq = jnp.sum(x * x, axis=-1, keepdims=True) * (1.0 / D)
    normed = (x * lax.rsqrt(meansq + EPSILON) * (1.0 + gain_ref[0, 0:1, :])).astype(BF16)
    own = nt_dot(normed, own_ref[0]).astype(BF16).astype(F32)
    other = nt_dot(normed, other_ref[0]).astype(BF16).astype(F32)
    front = jnp.where(first, own, other)
    back = jnp.where(first, other, own)
    cosine = cos_ref[...]
    sine = sin_ref[...]
    turned = head < HEADS + KV_HEADS
    new_front = jnp.where(turned, front * cosine - back * sine, front)
    new_back = jnp.where(turned, back * cosine + front * sine, back)
    whole = jnp.concatenate([new_front, new_back], axis=1)
    rows = [whole[ROWS * u : ROWS * u + ROWS, :].astype(BF16) for u in range(BATCH // ROWS)]
    for chip in range(CHIPS):
        tile_ref[bulk_place(chip)] = rows[chip * BATCH // (CHIPS * ROWS)]
    copy = pltpu.make_async_copy(tile_ref, out_ref.at[:, BULK_TILES - 1], sem)
    copy.start()
    copy.wait()


def attend_kernel(me_ref, lengths_ref, got_ref, position_ref, cache_ref, out_ref, leaving_ref, sem):
    leave = pltpu.make_async_copy(got_ref.at[:, pl.ds(PAGE_TILES, PAGE_TILES // 2)], leaving_ref, sem)
    leave.start()
    me = me_ref[0]
    group = me >> 3
    slot = me & 7
    rows_at = (group & 3) * PER_GROUP
    n_src = CHIPS * ROWS
    o = iota((32, n_src), 0)
    n = iota((32, n_src), 1)
    e = o & 1
    m = (o >> 1) & 3
    kind = o >> 3
    q_head = slot * 4 + m
    k_head = HEADS + slot * 2 + (m >> 1)
    v_head = k_head + KV_HEADS
    fix_head = HEADS + slot * 2 + (m & 1) + KV_HEADS * (m >> 1)
    chosen = jnp.where(kind == 0, q_head, jnp.where(kind == 1, k_head, jnp.where(kind == 2, v_head, fix_head)))
    pick = jnp.where(n == bulk_place(chosen) * ROWS + rows_at + e, 1.0, 0.0).astype(BF16)
    source = got_ref[:, BULK_TILES - 1].astype(F32).reshape(n_src, LANES).astype(BF16)
    picked = nn_dot(pick, source)
    q = picked[0:8]
    new_k = picked[8:16]
    new_v = picked[16:24]
    q16 = q.astype(BF16)
    scale = (D / HEADS) ** (-0.5)
    row = iota((ROWS, 1), 0)
    scores = jnp.zeros((ROWS, 8 * 2 * CHIPS), F32)
    for ee in range(PER_GROUP):
        for a in range(2):
            keys = cache_ref[0, ee, :, a * LANES : a * LANES + LANES]
            part = nt_dot(q16, keys)
            scores = jnp.where(((row & 1) == ee) & ((row >> 2) == a), part, scores)
    limit = jnp.where((row & 1) == 0, lengths_ref[group * PER_GROUP], lengths_ref[group * PER_GROUP + 1])
    weights = jnp.where(position_ref[...] < limit, jnp.exp(capped(scores * scale)), 0.0)
    own = jnp.exp(capped(jnp.sum(q * new_k, axis=-1, keepdims=True) * scale))
    denominator = jnp.sum(weights, axis=-1, keepdims=True) + own
    w16 = weights.astype(BF16)
    numerator = own.astype(BF16).astype(F32) * new_v
    for ee in range(PER_GROUP):
        for a in range(2):
            values = cache_ref[1, ee, :, a * LANES : a * LANES + LANES]
            part = nn_dot(w16, values)
            numerator = numerator + jnp.where(((row & 1) == ee) & ((row >> 2) == a), part, 0.0)
    attended = numerator / denominator
    payload = jnp.concatenate([attended, picked[24:32]], axis=0).astype(BF16)
    out_ref[...] = jnp.broadcast_to(payload[None], (CHIPS, 2 * ROWS, LANES))
    leave.wait()


def mix_kernel(me_ref, own_ref, other_ref, weight_ref, got_ref, out_ref, leaving_ref, sem):
    leave = pltpu.make_async_copy(
        got_ref.at[:, pl.ds(PAGE_TILES + PAGE_TILES // 2, PAGE_TILES // 2)], leaving_ref, sem
    )
    leave.start()
    me = me_ref[0]
    first = (me & 1) == 0
    n_src = CHIPS * ROWS
    o = iota((n_src, n_src), 0)
    n = iota((n_src, n_src), 1)
    quarter = o >> 7
    m = (o >> 5) & 3
    group = (o >> 1) & 15
    source_row = (group * QUARTERS + quarter) * ROWS + m * 2 + (o & 1)
    pick = jnp.where(n == source_row, 1.0, 0.0).astype(BF16)
    own = own_ref[...][:, :ROWS].astype(F32)
    other = other_ref[...][:, :ROWS].astype(F32)
    mixed = jnp.zeros((BATCH, SHARE), F32)
    for c in range(2):
        mine = jnp.where(first, own, other) if c == 0 else jnp.where(first, other, own)
        rows = nn_dot(pick, mine.reshape(n_src, LANES).astype(BF16)).astype(BF16)
        left = jnp.concatenate([rows[BATCH * b : BATCH * b + BATCH] for b in range(16)], axis=1)
        right = jnp.concatenate(
            [weight_ref[0, :, (2 * y + c) * 512 : (2 * y + c) * 512 + 512] for y in range(QUARTERS)], axis=1
        )
        mixed = mixed + nt_dot(left, right)
    values = mixed.astype(BF16).astype(F32)
    gap = jnp.zeros((HALF, LANES // 2 - SHARE), F32)
    packed = jnp.concatenate([values[:HALF], gap, values[HALF:], gap], axis=1)
    turned = pltpu.roll(packed, (me * SHARE) % LANES, 1).astype(BF16)
    out_ref[...] = jnp.broadcast_to(turned[None], (CHIPS, HALF, LANES))
    leave.wait()


def window(low_ref, high_ref, j):
    lane = iota((HALF, LANES), 1)
    far = (lane + LANES // 2) % LANES
    v, off = divmod(j * SHARE, LANES)
    low = low_ref[v]
    high = high_ref[v]
    if off + SHARE > LANES:
        low = jnp.where(lane >= off, low, low_ref[v + 1])
        high = jnp.where(far >= off, high, high_ref[v + 1])
    return jnp.where((lane - off) % LANES < LANES // 2, low, high)


def ffn_kernel(
    me_ref,
    own_ref,
    other_ref,
    hidden_ref,
    gain_ref,
    gate_up_ref,
    down_ref,
    keep_ref,
    send_ref,
    stream_ref,
    wide_ref,
    low_ref,
    high_ref,
    ffn_ref,
):
    me = me_ref[0]
    first = (me & 1) == 0
    lane = iota((BATCH, LANES), 1)
    near = iota((HALF, LANES), 1)
    far = (near + LANES // 2) % LANES
    total = jnp.zeros((BATCH, LANES), F32)
    for v in range(BLOCKS):
        low = high = None
        for j in range((LANES * v) // SHARE, (LANES * v + LANES - 1) // SHARE + 1):
            own = own_ref[j >> 1]
            other = other_ref[j >> 1]
            piece = (jnp.where(first, own, other) if j % 2 == 0 else jnp.where(first, other, own)).astype(F32)
            start = j * SHARE - LANES * v
            low = piece if low is None else jnp.where(near >= start, piece, low)
            high = piece if high is None else jnp.where(far >= start, piece, high)
        block = jnp.concatenate([low, pltpu.roll(high, LANES // 2, 1)], axis=0)
        wide_ref[v] = block
        total = total + block * block
    scale = lax.rsqrt(jnp.sum(total, axis=-1, keepdims=True) * (1.0 / D) + EPSILON)
    total = jnp.zeros((BATCH, LANES), F32)
    for v in range(BLOCKS):
        cols = slice(LANES * v, LANES * v + LANES)
        block = hidden_ref[:, cols] + wide_ref[v] * scale * (1.0 + gain_ref[0, 1:2, cols])
        wide_ref[v] = block
        total = total + block * block
    scale = lax.rsqrt(jnp.sum(total, axis=-1, keepdims=True) * (1.0 / D) + EPSILON)
    for v in range(BLOCKS):
        cols = slice(LANES * v, LANES * v + LANES)
        ffn_ref[:, cols] = (wide_ref[v] * scale * (1.0 + gain_ref[0, 2:3, cols])).astype(BF16)
    ffn_in = ffn_ref[...]
    gate = nt_dot(ffn_in, gate_up_ref[0, 0])
    up = nt_dot(ffn_in, gate_up_ref[0, 1])
    active = (jax.nn.gelu(gate, approximate=True) * up).astype(BF16)
    for v in range(BLOCKS):
        block = nn_dot(active, down_ref[0, :, LANES * v : LANES * v + LANES])
        low_ref[v] = block[:HALF]
        high_ref[v] = pltpu.roll(block[HALF:], LANES // 2, 1)
    for p in range(CHIPS):
        even = window(low_ref, high_ref, 2 * p)
        odd = window(low_ref, high_ref, 2 * p + 1)
        keep_ref[p] = jnp.where(first, even, odd).astype(BF16)
        send_ref[p] = jnp.where(first, odd, even).astype(BF16)
    start = me * SHARE
    at = start // LANES
    off = start % LANES
    after = jnp.minimum(at + 1, BLOCKS - 1)
    stream_ref[...] = jnp.where(lane >= off, wide_ref[at], wide_ref[after])


def to_front(x, me):
    off = (me * SHARE) % LANES
    return pltpu.roll(x, (LANES - off) % LANES, 1)


def portion_kernel(me_ref, got_ref, portion_ref, square_ref):
    me = me_ref[0]
    total = jnp.zeros((HALF, LANES), F32)
    for p in range(CHIPS):
        total = total + got_ref[p].astype(F32)
    packed = to_front(total, me)
    mine = jnp.concatenate([packed, pltpu.roll(packed, LANES // 2, 1)], axis=0)
    portion_ref[...] = mine
    lane = iota((BATCH, LANES), 1)
    square = jnp.sum(jnp.where(lane < SHARE, mine * mine, 0.0), axis=-1, keepdims=True)
    line = jnp.sum(jnp.where(iota((BATCH, LANES), 0) == lane, square, 0.0), axis=0, keepdims=True)
    square_ref[...] = jnp.broadcast_to(line[None], (CHIPS, 1, LANES))


def finish_kernel(me_ref, portion_ref, stream_ref, own_ref, other_ref, gain_ref, out_ref):
    me = me_ref[0]
    squares = jnp.sum(own_ref[...] + other_ref[...], axis=0)
    lane = iota((BATCH, LANES), 1)
    column = jnp.sum(jnp.where(iota((BATCH, LANES), 0) == lane, squares, 0.0), axis=-1, keepdims=True)
    scale = lax.rsqrt(column * (1.0 / D) + EPSILON)
    at = (me * SHARE) // LANES
    after = jnp.minimum(at + 1, BLOCKS - 1)
    here = gain_ref[0, 3:4, pl.ds(pl.multiple_of(at * LANES, LANES), LANES)]
    there = gain_ref[0, 3:4, pl.ds(pl.multiple_of(after * LANES, LANES), LANES)]
    gain = jnp.where(lane >= (me * SHARE) % LANES, here, there)
    done = to_front(stream_ref[...], me) + portion_ref[...] * scale * (1.0 + to_front(gain, me))
    out_ref[...] = done[:, :SHARE]


def decode_kernel(
    me_ref, lengths_ref, got_ref, keys_ref, values_ref, own_new_ref, other_new_ref, out_ref
):
    me = me_ref[0]
    core = me & 1

    def place(first_core):
        def body(g, carry):
            for y in range(QUARTERS):
                s = bulk_place(g * QUARTERS + y)
                for side in range(2):
                    slot = 2 * y + (first_core if side == 0 else 1 - first_core)
                    for kv in range(2):
                        for e in range(PER_GROUP):
                            for h in range(2):
                                cols = slice((2 * slot + h) * LANES, (2 * slot + h) * LANES + LANES)
                                if side == 0:
                                    tile = got_ref[s, kv * 4 + e * 2 + h]
                                else:
                                    tile = (keys_ref, values_ref)[kv][s, e * 2 + h]
                                out_ref[kv, g * PER_GROUP + e, :, cols] = tile
            return carry

        lax.fori_loop(0, GROUPS, body, 0)

    @pl.when(core == 0)
    def _():
        place(0)

    @pl.when(core == 1)
    def _():
        place(1)

    def fresh(r, carry):
        length = lengths_ref[r]

        @pl.when((length >> 3) == me)
        def _():
            g = r >> 1
            e = r & 1
            token = iota((ROWS, LANES), 0) == (length & 7)
            which = iota((2 * ROWS, LANES), 0)
            for y in range(QUARTERS):
                s = g * QUARTERS + y
                own = own_new_ref[s].astype(F32)
                other = other_new_ref[s].astype(F32)
                for c in range(2):
                    rows = jnp.where(core == c, own, other)
                    for kv in range(2):
                        for a in range(2):
                            at = ROWS + kv * 4 + a * 2 + e
                            line = jnp.sum(jnp.where(which == at, rows, 0.0), axis=0, keepdims=True)
                            slot = 2 * (2 * y + c) + a
                            cols = slice(slot * LANES, slot * LANES + LANES)
                            old = out_ref[kv, r, :, cols].astype(F32)
                            out_ref[kv, r, :, cols] = jnp.where(token, line, old).astype(BF16)

        return carry

    lax.fori_loop(0, BATCH, fresh, 0)


def core_swap(shard):
    return lax.ppermute(shard, "tp_2", [(0, 1), (1, 0)])


def to_chips(tiles):
    return lax.all_to_all(tiles, XY, 0, 0, tiled=True)


def pages_call(me, lengths, table, cache, weight, hidden, gains):
    fixed = [pltpu.with_memory_space_constraint(x, pltpu.HBM) for x in (lengths, table, cache, weight, hidden, gains)]
    return call(
        pages_kernel,
        (
            pltpu.VMEM((CHIPS, BULK_TILES, ROWS, LANES), BF16),
            pltpu.VMEM(cache.shape, BF16),
            pltpu.VMEM(weight.shape, BF16),
            pltpu.VMEM(hidden.shape, F32),
            pltpu.VMEM(gains.shape, F32),
            pltpu.VMEM((BATCH, HEAD_DIM // 2), F32),
            pltpu.VMEM((ROWS, ROWS * 2 * CHIPS), jnp.int32),
        ),
        [smem()] + [hbm()] * 6,
        (vmem(),) * 7,
        scratch_shapes=[
            pltpu.SMEM(lengths.shape, jnp.int32),
            pltpu.SMEM(table.shape, jnp.int32),
            pltpu.VMEM(table.shape, jnp.int32),
            pltpu.SemaphoreType.DMA((10,)),
        ],
    )(me, *fixed)


def qkv_call(me, hidden, gains, own, other, cosine, sine, buf):
    return call(
        qkv_kernel,
        shaped(buf.shape, BF16),
        [smem()] + [vmem()] * 6 + [pl.BlockSpec(memory_space=pl.ANY)],
        pl.BlockSpec(memory_space=pl.ANY),
        scratch_shapes=[pltpu.VMEM((CHIPS, ROWS, LANES), BF16), pltpu.SemaphoreType.DMA],
        input_output_aliases={7: 0},
    )(me, hidden, gains, own, other, cosine, sine, buf)


def attend_call(me, lengths, got, position, cache):
    return call(
        attend_kernel,
        (
            pltpu.VMEM((CHIPS, 2 * ROWS, LANES), BF16),
            pltpu.VMEM((CHIPS, PAGE_TILES // 2, ROWS, LANES), BF16),
        ),
        [smem(), smem()] + [vmem()] * 3,
        (vmem(), vmem()),
        scratch_shapes=[pltpu.SemaphoreType.DMA],
    )(me, lengths, got, position, cache)


def mix_call(me, own, other, weight, got):
    return call(
        mix_kernel,
        (
            pltpu.VMEM((CHIPS, HALF, LANES), BF16),
            pltpu.VMEM((CHIPS, PAGE_TILES // 2, ROWS, LANES), BF16),
        ),
        [smem()] + [vmem()] * 4,
        (vmem(), vmem()),
        scratch_shapes=[pltpu.SemaphoreType.DMA],
    )(me, own, other, weight, got)


def ffn_call(me, own, other, hidden, gains, gate_up, down):
    wide = shaped((CHIPS, HALF, LANES), BF16)
    return call(
        ffn_kernel,
        (wide, wide, shaped((BATCH, LANES), F32)),
        [smem()] + [vmem()] * 6,
        (vmem(), vmem(), vmem()),
        scratch_shapes=[
            pltpu.VMEM((BLOCKS, BATCH, LANES), F32),
            pltpu.VMEM((BLOCKS, HALF, LANES), F32),
            pltpu.VMEM((BLOCKS, HALF, LANES), F32),
            pltpu.VMEM((BATCH, D), BF16),
        ],
    )(me, own, other, hidden, gains, gate_up, down)


def portion_call(me, got):
    return call(
        portion_kernel,
        (shaped((BATCH, LANES), F32), shaped((CHIPS, 1, LANES), F32)),
        [smem(), vmem()],
        (vmem(), vmem()),
    )(me, got)


def finish_call(me, portion, stream, own, other, gains):
    return call(finish_kernel, shaped((BATCH, SHARE), F32), [smem()] + [vmem()] * 5, vmem())(
        me, portion, stream, own, other, gains
    )


def decode_call(me, lengths, got, other_keys, other_values, own_new, other_new):
    return call(
        decode_kernel, pltpu.VMEM((2, BATCH, ROWS, KV_HEADS * HEAD_DIM), BF16), [smem(), smem()] + [vmem()] * 5, vmem()
    )(me, lengths, got, other_keys, other_values, own_new, other_new)


def rope_tables(spread_length):
    half_dim = HEAD_DIM // 2
    exponent = jnp.arange(half_dim, dtype=F32) * (-2.0 / HEAD_DIM)
    angles = spread_length * jnp.power(jnp.float32(10000.0), exponent)
    return jnp.cos(angles), jnp.sin(angles)


def on_device(
    hidden_in,
    prefill_cache,
    lengths,
    page_table,
    qkv_weight,
    out_weight,
    gate_up_weight,
    down_weight,
    norm_gains,
):
    me = jnp.full((1,), lax.axis_index(TP), jnp.int32)
    other_rows = core_swap(qkv_weight)
    buf, held, own_rows, hidden, gains, spread_length, position = pages_call(
        me, lengths, page_table, prefill_cache[0, 0], qkv_weight, hidden_in, norm_gains
    )
    cosine, sine = rope_tables(spread_length)
    buf = qkv_call(me, hidden, gains, own_rows, other_rows, cosine, sine, buf)
    got = lax.all_to_all(buf, XY[::-1], 0, 0, tiled=True)
    payload, leaving_keys = attend_call(
        me, lengths, got, position, held.reshape(2, PER_GROUP, -1, 2 * HEAD_DIM)
    )
    own_att = to_chips(payload)
    other_att = core_swap(own_att)
    other_keys = core_swap(leaving_keys)
    payload, leaving_values = mix_call(me, own_att, other_att, out_weight, got)
    own_mix = to_chips(payload)
    other_mix = core_swap(own_mix)
    other_values = core_swap(leaving_values)
    keep, send, stream = ffn_call(me, own_mix, other_mix, hidden, gains, gate_up_weight, down_weight)
    sent = core_swap(send)
    chip = (keep.astype(F32) + sent.astype(F32)).astype(BF16)
    got_branch = to_chips(chip)
    portion, square = portion_call(me, got_branch)
    squares = to_chips(square)
    result = finish_call(me, portion, stream, squares, core_swap(squares), gains)
    decoded = decode_call(me, lengths, got, other_keys, other_values, own_att, other_att)
    return result, decoded[None, None]


def solution(mesh):
    torus = Mesh(mesh.devices.reshape(mesh.shape["grp"], 8, 8, 2), ("grp", "tp_0", "tp_1", "tp_2"))
    return jax.shard_map(
        on_device,
        mesh=torus,
        in_specs=(
            P("grp", None),
            P(TP, None, None, "grp", None, None, None),
            P("grp"),
            P("grp", None),
            P(None, TP, None),
            P(None, TP, None),
            P(None, None, TP, None),
            P(None, TP, None),
            P(),
        ),
        out_specs=(P("grp", TP), P(TP, None, None, "grp", None, None)),
        check_vma=False,
    )
```

```python
import jax
import jax.numpy as jnp
from jax import lax
from jax.experimental import pallas as pl
from jax.experimental.pallas import tpu as pltpu
from jax.sharding import Mesh
from jax.sharding import PartitionSpec as P

D = 4608
HEADS = 32
KV_HEADS = 16
HEAD_DIM = 128
PREFILL_TP = 8
TP = ("tp_0", "tp_1", "tp_2")
XY = ("tp_0", "tp_1")

EPSILON = 1e-06
SOFTCAP = 50.0
LANES = 128
ROWS = 8
BF16 = jnp.bfloat16
F32 = jnp.float32

CHIPS = 64
QUARTERS = PREFILL_TP // 2
GROUPS = CHIPS // QUARTERS
SHARE = D // (2 * CHIPS)
BLOCKS = D // LANES
BATCH = 32
HALF = BATCH // 2
PER_GROUP = 2
PAGE_TILES = 2 * PER_GROUP * 2
BULK_TILES = 2 * PAGE_TILES + 1
VMEM_LIMIT = 24 * 1024 * 1024


def smem():
    return pl.BlockSpec(memory_space=pltpu.SMEM)


def vmem():
    return pl.BlockSpec(memory_space=pltpu.VMEM)


def hbm():
    return pl.BlockSpec(memory_space=pltpu.HBM)


def call(kernel, out_shape, in_specs, out_specs, **more):
    return pl.pallas_call(
        kernel,
        out_shape=out_shape,
        in_specs=in_specs,
        out_specs=out_specs,
        compiler_params=pltpu.CompilerParams(vmem_limit_bytes=VMEM_LIMIT),
        **more,
    )


def shaped(shape, dtype):
    return jax.ShapeDtypeStruct(shape, dtype)


def nt_dot(left, right):
    return lax.dot_general(left, right, (((1,), (1,)), ((), ())), preferred_element_type=F32)


def nn_dot(left, right):
    return lax.dot_general(left, right, (((1,), (0,)), ((), ())), preferred_element_type=F32)


def iota(shape, dim):
    return lax.broadcasted_iota(jnp.int32, shape, dim)


def place_of(chip):
    return ((chip & 7) << 3) | (chip >> 3)


def capped(raw_scores):
    return SOFTCAP * jnp.tanh(raw_scores / SOFTCAP)


def pages_kernel(
    me_ref,
    lengths_hbm,
    table_hbm,
    cache_hbm,
    weight_hbm,
    hidden_hbm,
    gain_hbm,
    out_ref,
    held_ref,
    weight_ref,
    hidden_ref,
    gain_ref,
    length_ref,
    position_ref,
    lengths_ref,
    table_ref,
    rows_ref,
    sems,
):
    me = me_ref[0]
    core = me & 1
    group = me >> 3
    loads = [
        (lengths_hbm, lengths_ref),
        (table_hbm, rows_ref),
        (table_hbm, table_ref),
        *[
            (cache_hbm.at[:, e, pl.ds(CHIPS * half, CHIPS)], held_ref.at[:, e, pl.ds(CHIPS * half, CHIPS)])
            for e in range(PER_GROUP)
            for half in range(2)
        ],
        (hidden_hbm, hidden_ref),
        (weight_hbm, weight_ref),
        (gain_hbm, gain_ref),
    ]
    loads = [pltpu.make_async_copy(src, dst, sems.at[i]) for i, (src, dst) in enumerate(loads)]
    for load in loads:
        load.start()
    for load in loads[:3]:
        load.wait()
    row = iota((BATCH, HEAD_DIM // 2), 0)
    spread_length = jnp.zeros((BATCH, HEAD_DIM // 2), F32)
    for r in range(BATCH):
        spread_length = jnp.where(row == r, lengths_ref[r].astype(F32), spread_length)
    length_ref[...] = spread_length
    pages = 2 * CHIPS
    table_row = iota((BATCH, pages), 0)
    lines = []
    for e in range(PER_GROUP):
        chosen_row = jnp.where(table_row == group * PER_GROUP + e, rows_ref[...], 0)
        lines.append(jnp.sum(chosen_row, axis=0, keepdims=True))
    blocks = jnp.where((iota((ROWS, 1), 0) & 1) == 0, lines[0], lines[1]).astype(F32).astype(BF16)
    spread = jnp.where(iota((pages, ROWS * pages), 1) >> 3 == iota((pages, ROWS * pages), 0), 1.0, 0.0)
    inside = iota((ROWS, ROWS * pages), 1) & 7
    position_ref[...] = nn_dot(blocks, spread.astype(BF16)).astype(jnp.int32) * ROWS + inside
    for e in range(PER_GROUP):
        for half in range(2):
            loads[3 + 2 * e + half].wait()

            def place(j, carry):
                block = table_ref[PER_GROUP * group + e, j]
                chip = place_of(block >> 1)
                at = ((block & 1) ^ core) * PAGE_TILES + e * 2
                for kv in range(2):
                    page = held_ref[kv, e, j]
                    out_ref[chip, at + kv * 4] = page[:, :LANES]
                    out_ref[chip, at + kv * 4 + 1] = page[:, LANES:]
                return carry

            lax.fori_loop(CHIPS * half, CHIPS * half + CHIPS, place, 0, unroll=8)
    for load in loads[7:]:
        load.wait()


def qkv_kernel(
    me_ref, hidden_ref, gain_ref, own_ref, other_ref, cos_ref, sin_ref, buf_ref, out_ref, tile_ref, sem
):
    me = me_ref[0]
    first = (me & 1) == 0
    head = me >> 1
    x = hidden_ref[...]
    meansq = jnp.sum(x * x, axis=-1, keepdims=True) * (1.0 / D)
    normed = (x * lax.rsqrt(meansq + EPSILON) * (1.0 + gain_ref[0, 0:1, :])).astype(BF16)
    own = nt_dot(normed, own_ref[0]).astype(BF16).astype(F32)
    other = nt_dot(normed, other_ref[0]).astype(BF16).astype(F32)
    front = jnp.where(first, own, other)
    back = jnp.where(first, other, own)
    cosine = cos_ref[...]
    sine = sin_ref[...]
    turned = head < HEADS + KV_HEADS
    new_front = jnp.where(turned, front * cosine - back * sine, front)
    new_back = jnp.where(turned, back * cosine + front * sine, back)
    whole = jnp.concatenate([new_front, new_back], axis=1)
    rows = [whole[ROWS * u : ROWS * u + ROWS, :].astype(BF16) for u in range(BATCH // ROWS)]
    for chip in range(CHIPS):
        tile_ref[place_of(chip)] = rows[chip * BATCH // (CHIPS * ROWS)]
    copy = pltpu.make_async_copy(tile_ref, out_ref.at[:, BULK_TILES - 1], sem)
    copy.start()
    copy.wait()


def attend_kernel(me_ref, lengths_ref, got_ref, position_ref, cache_ref, out_ref, leaving_ref, sem):
    leave = pltpu.make_async_copy(got_ref.at[:, pl.ds(PAGE_TILES, PAGE_TILES // 2)], leaving_ref, sem)
    leave.start()
    me = me_ref[0]
    group = me >> 3
    slot = me & 7
    rows_at = (group & 3) * PER_GROUP
    n_src = CHIPS * ROWS
    o = iota((32, n_src), 0)
    n = iota((32, n_src), 1)
    e = o & 1
    m = (o >> 1) & 3
    kind = o >> 3
    q_head = slot * 4 + m
    k_head = HEADS + slot * 2 + (m >> 1)
    v_head = k_head + KV_HEADS
    fix_head = HEADS + slot * 2 + (m & 1) + KV_HEADS * (m >> 1)
    chosen = jnp.where(kind == 0, q_head, jnp.where(kind == 1, k_head, jnp.where(kind == 2, v_head, fix_head)))
    pick = jnp.where(n == place_of(chosen) * ROWS + rows_at + e, 1.0, 0.0).astype(BF16)
    source = got_ref[:, BULK_TILES - 1].astype(F32).reshape(n_src, LANES).astype(BF16)
    picked = nn_dot(pick, source)
    q = picked[0:8]
    new_k = picked[8:16]
    new_v = picked[16:24]
    q16 = q.astype(BF16)
    scale = (D / HEADS) ** (-0.5)
    row = iota((ROWS, 1), 0)
    scores = jnp.zeros((ROWS, 8 * 2 * CHIPS), F32)
    for ee in range(PER_GROUP):
        for a in range(2):
            keys = cache_ref[0, ee, :, a * LANES : a * LANES + LANES]
            part = nt_dot(q16, keys)
            scores = jnp.where(((row & 1) == ee) & ((row >> 2) == a), part, scores)
    limit = jnp.where((row & 1) == 0, lengths_ref[group * PER_GROUP], lengths_ref[group * PER_GROUP + 1])
    weights = jnp.where(position_ref[...] < limit, jnp.exp(capped(scores * scale)), 0.0)
    own = jnp.exp(capped(jnp.sum(q * new_k, axis=-1, keepdims=True) * scale))
    denominator = jnp.sum(weights, axis=-1, keepdims=True) + own
    w16 = weights.astype(BF16)
    numerator = own.astype(BF16).astype(F32) * new_v
    for ee in range(PER_GROUP):
        for a in range(2):
            values = cache_ref[1, ee, :, a * LANES : a * LANES + LANES]
            part = nn_dot(w16, values)
            numerator = numerator + jnp.where(((row & 1) == ee) & ((row >> 2) == a), part, 0.0)
    attended = numerator / denominator
    payload = jnp.concatenate([attended, picked[24:32]], axis=0).astype(BF16)
    out_ref[...] = jnp.broadcast_to(payload[None], (CHIPS, 2 * ROWS, LANES))
    leave.wait()


def mix_kernel(me_ref, own_ref, other_ref, weight_ref, got_ref, out_ref, leaving_ref, sem):
    leave = pltpu.make_async_copy(
        got_ref.at[:, pl.ds(PAGE_TILES + PAGE_TILES // 2, PAGE_TILES // 2)], leaving_ref, sem
    )
    leave.start()
    me = me_ref[0]
    first = (me & 1) == 0
    n_src = CHIPS * ROWS
    o = iota((n_src, n_src), 0)
    n = iota((n_src, n_src), 1)
    quarter = o >> 7
    m = (o >> 5) & 3
    group = (o >> 1) & 15
    source_row = place_of(group * QUARTERS + quarter) * ROWS + m * 2 + (o & 1)
    pick = jnp.where(n == source_row, 1.0, 0.0).astype(BF16)
    own = own_ref[...][:, :ROWS].astype(F32)
    other = other_ref[...][:, :ROWS].astype(F32)
    mixed = jnp.zeros((BATCH, SHARE), F32)
    for c in range(2):
        mine = jnp.where(first, own, other) if c == 0 else jnp.where(first, other, own)
        rows = nn_dot(pick, mine.reshape(n_src, LANES).astype(BF16)).astype(BF16)
        left = jnp.concatenate([rows[BATCH * b : BATCH * b + BATCH] for b in range(16)], axis=1)
        right = jnp.concatenate(
            [weight_ref[0, :, (2 * y + c) * 512 : (2 * y + c) * 512 + 512] for y in range(QUARTERS)], axis=1
        )
        mixed = mixed + nt_dot(left, right)
    values = mixed.astype(BF16).astype(F32)
    gap = jnp.zeros((HALF, LANES // 2 - SHARE), F32)
    packed = jnp.concatenate([values[:HALF], gap, values[HALF:], gap], axis=1)
    turned = pltpu.roll(packed, (me * SHARE) % LANES, 1).astype(BF16)
    out_ref[...] = jnp.broadcast_to(turned[None], (CHIPS, HALF, LANES))
    leave.wait()


def window(low_ref, high_ref, j):
    lane = iota((HALF, LANES), 1)
    far = (lane + LANES // 2) % LANES
    v, off = divmod(j * SHARE, LANES)
    low = low_ref[v]
    high = high_ref[v]
    if off + SHARE > LANES:
        low = jnp.where(lane >= off, low, low_ref[v + 1])
        high = jnp.where(far >= off, high, high_ref[v + 1])
    return jnp.where((lane - off) % LANES < LANES // 2, low, high)


def ffn_kernel(
    me_ref,
    own_ref,
    other_ref,
    hidden_ref,
    gain_ref,
    gate_up_ref,
    down_ref,
    keep_ref,
    send_ref,
    stream_ref,
    wide_ref,
    low_ref,
    high_ref,
    ffn_ref,
):
    me = me_ref[0]
    first = (me & 1) == 0
    lane = iota((BATCH, LANES), 1)
    near = iota((HALF, LANES), 1)
    far = (near + LANES // 2) % LANES
    total = jnp.zeros((BATCH, LANES), F32)
    for v in range(BLOCKS):
        low = high = None
        for j in range((LANES * v) // SHARE, (LANES * v + LANES - 1) // SHARE + 1):
            own = own_ref[place_of(j >> 1)]
            other = other_ref[place_of(j >> 1)]
            piece = (jnp.where(first, own, other) if j % 2 == 0 else jnp.where(first, other, own)).astype(F32)
            start = j * SHARE - LANES * v
            low = piece if low is None else jnp.where(near >= start, piece, low)
            high = piece if high is None else jnp.where(far >= start, piece, high)
        block = jnp.concatenate([low, pltpu.roll(high, LANES // 2, 1)], axis=0)
        wide_ref[v] = block
        total = total + block * block
    scale = lax.rsqrt(jnp.sum(total, axis=-1, keepdims=True) * (1.0 / D) + EPSILON)
    total = jnp.zeros((BATCH, LANES), F32)
    for v in range(BLOCKS):
        cols = slice(LANES * v, LANES * v + LANES)
        block = hidden_ref[:, cols] + wide_ref[v] * scale * (1.0 + gain_ref[0, 1:2, cols])
        wide_ref[v] = block
        total = total + block * block
    scale = lax.rsqrt(jnp.sum(total, axis=-1, keepdims=True) * (1.0 / D) + EPSILON)
    for v in range(BLOCKS):
        cols = slice(LANES * v, LANES * v + LANES)
        ffn_ref[:, cols] = (wide_ref[v] * scale * (1.0 + gain_ref[0, 2:3, cols])).astype(BF16)
    ffn_in = ffn_ref[...]
    gate = nt_dot(ffn_in, gate_up_ref[0, 0])
    up = nt_dot(ffn_in, gate_up_ref[0, 1])
    active = (jax.nn.gelu(gate, approximate=True) * up).astype(BF16)
    for v in range(BLOCKS):
        block = nn_dot(active, down_ref[0, :, LANES * v : LANES * v + LANES])
        low_ref[v] = block[:HALF]
        high_ref[v] = pltpu.roll(block[HALF:], LANES // 2, 1)
    for p in range(CHIPS):
        even = window(low_ref, high_ref, 2 * p)
        odd = window(low_ref, high_ref, 2 * p + 1)
        keep_ref[place_of(p)] = jnp.where(first, even, odd).astype(BF16)
        send_ref[place_of(p)] = jnp.where(first, odd, even).astype(BF16)
    start = me * SHARE
    at = start // LANES
    off = start % LANES
    after = jnp.minimum(at + 1, BLOCKS - 1)
    stream_ref[...] = jnp.where(lane >= off, wide_ref[at], wide_ref[after])


def to_front(x, me):
    off = (me * SHARE) % LANES
    return pltpu.roll(x, (LANES - off) % LANES, 1)


def portion_kernel(me_ref, got_ref, portion_ref, square_ref):
    me = me_ref[0]
    total = jnp.zeros((HALF, LANES), F32)
    for p in range(CHIPS):
        total = total + got_ref[p].astype(F32)
    packed = to_front(total, me)
    mine = jnp.concatenate([packed, pltpu.roll(packed, LANES // 2, 1)], axis=0)
    portion_ref[...] = mine
    lane = iota((BATCH, LANES), 1)
    square = jnp.sum(jnp.where(lane < SHARE, mine * mine, 0.0), axis=-1, keepdims=True)
    line = jnp.sum(jnp.where(iota((BATCH, LANES), 0) == lane, square, 0.0), axis=0, keepdims=True)
    square_ref[...] = jnp.broadcast_to(line[None], (CHIPS, 1, LANES))


def finish_kernel(me_ref, portion_ref, stream_ref, own_ref, other_ref, gain_ref, out_ref):
    me = me_ref[0]
    squares = jnp.sum(own_ref[...] + other_ref[...], axis=0)
    lane = iota((BATCH, LANES), 1)
    column = jnp.sum(jnp.where(iota((BATCH, LANES), 0) == lane, squares, 0.0), axis=-1, keepdims=True)
    scale = lax.rsqrt(column * (1.0 / D) + EPSILON)
    at = (me * SHARE) // LANES
    after = jnp.minimum(at + 1, BLOCKS - 1)
    here = gain_ref[0, 3:4, pl.ds(pl.multiple_of(at * LANES, LANES), LANES)]
    there = gain_ref[0, 3:4, pl.ds(pl.multiple_of(after * LANES, LANES), LANES)]
    gain = jnp.where(lane >= (me * SHARE) % LANES, here, there)
    done = to_front(stream_ref[...], me) + portion_ref[...] * scale * (1.0 + to_front(gain, me))
    out_ref[...] = done[:, :SHARE]


def decode_kernel(
    me_ref, lengths_ref, got_ref, keys_ref, values_ref, own_new_ref, other_new_ref, out_ref
):
    me = me_ref[0]
    core = me & 1

    def place(first_core):
        def body(g, carry):
            for y in range(QUARTERS):
                s = place_of(g * QUARTERS + y)
                for side in range(2):
                    slot = 2 * y + (first_core if side == 0 else 1 - first_core)
                    for kv in range(2):
                        for e in range(PER_GROUP):
                            for h in range(2):
                                cols = slice((2 * slot + h) * LANES, (2 * slot + h) * LANES + LANES)
                                if side == 0:
                                    tile = got_ref[s, kv * 4 + e * 2 + h]
                                else:
                                    tile = (keys_ref, values_ref)[kv][s, e * 2 + h]
                                out_ref[kv, g * PER_GROUP + e, :, cols] = tile
            return carry

        lax.fori_loop(0, GROUPS, body, 0)

    @pl.when(core == 0)
    def _():
        place(0)

    @pl.when(core == 1)
    def _():
        place(1)

    def fresh(r, carry):
        length = lengths_ref[r]

        @pl.when((length >> 3) == me)
        def _():
            g = r >> 1
            e = r & 1
            token = iota((ROWS, LANES), 0) == (length & 7)
            which = iota((2 * ROWS, LANES), 0)
            for y in range(QUARTERS):
                s = place_of(g * QUARTERS + y)
                own = own_new_ref[s].astype(F32)
                other = other_new_ref[s].astype(F32)
                for c in range(2):
                    rows = jnp.where(core == c, own, other)
                    for kv in range(2):
                        for a in range(2):
                            at = ROWS + kv * 4 + a * 2 + e
                            line = jnp.sum(jnp.where(which == at, rows, 0.0), axis=0, keepdims=True)
                            slot = 2 * (2 * y + c) + a
                            cols = slice(slot * LANES, slot * LANES + LANES)
                            old = out_ref[kv, r, :, cols].astype(F32)
                            out_ref[kv, r, :, cols] = jnp.where(token, line, old).astype(BF16)

        return carry

    lax.fori_loop(0, BATCH, fresh, 0)


def core_swap(shard):
    return lax.ppermute(shard, "tp_2", [(0, 1), (1, 0)])


def to_chips(tiles):
    return lax.all_to_all(tiles, XY[::-1], 0, 0, tiled=True)


def pages_call(me, lengths, table, cache, weight, hidden, gains):
    fixed = [pltpu.with_memory_space_constraint(x, pltpu.HBM) for x in (lengths, table, cache, weight, hidden, gains)]
    return call(
        pages_kernel,
        (
            pltpu.VMEM((CHIPS, BULK_TILES, ROWS, LANES), BF16),
            pltpu.VMEM(cache.shape, BF16),
            pltpu.VMEM(weight.shape, BF16),
            pltpu.VMEM(hidden.shape, F32),
            pltpu.VMEM(gains.shape, F32),
            pltpu.VMEM((BATCH, HEAD_DIM // 2), F32),
            pltpu.VMEM((ROWS, ROWS * 2 * CHIPS), jnp.int32),
        ),
        [smem()] + [hbm()] * 6,
        (vmem(),) * 7,
        scratch_shapes=[
            pltpu.SMEM(lengths.shape, jnp.int32),
            pltpu.SMEM(table.shape, jnp.int32),
            pltpu.VMEM(table.shape, jnp.int32),
            pltpu.SemaphoreType.DMA((10,)),
        ],
    )(me, *fixed)


def qkv_call(me, hidden, gains, own, other, cosine, sine, buf):
    return call(
        qkv_kernel,
        shaped(buf.shape, BF16),
        [smem()] + [vmem()] * 6 + [pl.BlockSpec(memory_space=pl.ANY)],
        pl.BlockSpec(memory_space=pl.ANY),
        scratch_shapes=[pltpu.VMEM((CHIPS, ROWS, LANES), BF16), pltpu.SemaphoreType.DMA],
        input_output_aliases={7: 0},
    )(me, hidden, gains, own, other, cosine, sine, buf)


def attend_call(me, lengths, got, position, cache):
    return call(
        attend_kernel,
        (
            pltpu.VMEM((CHIPS, 2 * ROWS, LANES), BF16),
            pltpu.VMEM((CHIPS, PAGE_TILES // 2, ROWS, LANES), BF16),
        ),
        [smem(), smem()] + [vmem()] * 3,
        (vmem(), vmem()),
        scratch_shapes=[pltpu.SemaphoreType.DMA],
    )(me, lengths, got, position, cache)


def mix_call(me, own, other, weight, got):
    return call(
        mix_kernel,
        (
            pltpu.VMEM((CHIPS, HALF, LANES), BF16),
            pltpu.VMEM((CHIPS, PAGE_TILES // 2, ROWS, LANES), BF16),
        ),
        [smem()] + [vmem()] * 4,
        (vmem(), vmem()),
        scratch_shapes=[pltpu.SemaphoreType.DMA],
    )(me, own, other, weight, got)


def ffn_call(me, own, other, hidden, gains, gate_up, down):
    wide = shaped((CHIPS, HALF, LANES), BF16)
    return call(
        ffn_kernel,
        (wide, wide, shaped((BATCH, LANES), F32)),
        [smem()] + [vmem()] * 6,
        (vmem(), vmem(), vmem()),
        scratch_shapes=[
            pltpu.VMEM((BLOCKS, BATCH, LANES), F32),
            pltpu.VMEM((BLOCKS, HALF, LANES), F32),
            pltpu.VMEM((BLOCKS, HALF, LANES), F32),
            pltpu.VMEM((BATCH, D), BF16),
        ],
    )(me, own, other, hidden, gains, gate_up, down)


def portion_call(me, got):
    return call(
        portion_kernel,
        (shaped((BATCH, LANES), F32), shaped((CHIPS, 1, LANES), F32)),
        [smem(), vmem()],
        (vmem(), vmem()),
    )(me, got)


def finish_call(me, portion, stream, own, other, gains):
    return call(finish_kernel, shaped((BATCH, SHARE), F32), [smem()] + [vmem()] * 5, vmem())(
        me, portion, stream, own, other, gains
    )


def decode_call(me, lengths, got, other_keys, other_values, own_new, other_new):
    return call(
        decode_kernel, pltpu.VMEM((2, BATCH, ROWS, KV_HEADS * HEAD_DIM), BF16), [smem(), smem()] + [vmem()] * 5, vmem()
    )(me, lengths, got, other_keys, other_values, own_new, other_new)


def rope_tables(spread_length):
    half_dim = HEAD_DIM // 2
    exponent = jnp.arange(half_dim, dtype=F32) * (-2.0 / HEAD_DIM)
    angles = spread_length * jnp.power(jnp.float32(10000.0), exponent)
    return jnp.cos(angles), jnp.sin(angles)


def on_device(
    hidden_in,
    prefill_cache,
    lengths,
    page_table,
    qkv_weight,
    out_weight,
    gate_up_weight,
    down_weight,
    norm_gains,
):
    me = jnp.full((1,), lax.axis_index(TP), jnp.int32)
    other_rows = core_swap(qkv_weight)
    buf, held, own_rows, hidden, gains, spread_length, position = pages_call(
        me, lengths, page_table, prefill_cache[0, 0], qkv_weight, hidden_in, norm_gains
    )
    cosine, sine = rope_tables(spread_length)
    buf = qkv_call(me, hidden, gains, own_rows, other_rows, cosine, sine, buf)
    got = to_chips(buf)
    payload, leaving_keys = attend_call(
        me, lengths, got, position, held.reshape(2, PER_GROUP, -1, 2 * HEAD_DIM)
    )
    own_att = to_chips(payload)
    other_att = core_swap(own_att)
    other_keys = core_swap(leaving_keys)
    payload, leaving_values = mix_call(me, own_att, other_att, out_weight, got)
    own_mix = to_chips(payload)
    other_mix = core_swap(own_mix)
    other_values = core_swap(leaving_values)
    keep, send, stream = ffn_call(me, own_mix, other_mix, hidden, gains, gate_up_weight, down_weight)
    sent = core_swap(send)
    chip = (keep.astype(F32) + sent.astype(F32)).astype(BF16)
    got_branch = to_chips(chip)
    portion, square = portion_call(me, got_branch)
    squares = to_chips(square)
    result = finish_call(me, portion, stream, squares, core_swap(squares), gains)
    decoded = decode_call(me, lengths, got, other_keys, other_values, own_att, other_att)
    return result, decoded[None, None]


def solution(mesh):
    torus = Mesh(mesh.devices.reshape(mesh.shape["grp"], 8, 8, 2), ("grp", "tp_0", "tp_1", "tp_2"))
    return jax.shard_map(
        on_device,
        mesh=torus,
        in_specs=(
            P("grp", None),
            P(TP, None, None, "grp", None, None, None),
            P("grp"),
            P("grp", None),
            P(None, TP, None),
            P(None, TP, None),
            P(None, None, TP, None),
            P(None, TP, None),
            P(),
        ),
        out_specs=(P("grp", TP), P(TP, None, None, "grp", None, None)),
        check_vma=False,
    )
```

```python
import jax
import jax.numpy as jnp
from jax import lax
from jax.experimental import pallas as pl
from jax.experimental.pallas import tpu as pltpu
from jax.sharding import Mesh
from jax.sharding import PartitionSpec as P

D = 4608
HEADS = 32
KV_HEADS = 16
HEAD_DIM = 128
PREFILL_TP = 8
TP = ("tp_0", "tp_1", "tp_2")
XY = ("tp_0", "tp_1")

EPSILON = 1e-06
SOFTCAP = 50.0
LANES = 128
ROWS = 8
BF16 = jnp.bfloat16
F32 = jnp.float32

CHIPS = 64
QUARTERS = PREFILL_TP // 2
GROUPS = CHIPS // QUARTERS
SHARE = D // (2 * CHIPS)
BLOCKS = D // LANES
BATCH = 32
HALF = BATCH // 2
PER_GROUP = 2
PAGE_TILES = 2 * PER_GROUP * 2
BULK_TILES = 2 * PAGE_TILES + 1
VMEM_LIMIT = 24 * 1024 * 1024


def smem():
    return pl.BlockSpec(memory_space=pltpu.SMEM)


def vmem():
    return pl.BlockSpec(memory_space=pltpu.VMEM)


def hbm():
    return pl.BlockSpec(memory_space=pltpu.HBM)


def call(kernel, out_shape, in_specs, out_specs, **more):
    return pl.pallas_call(
        kernel,
        out_shape=out_shape,
        in_specs=in_specs,
        out_specs=out_specs,
        compiler_params=pltpu.CompilerParams(vmem_limit_bytes=VMEM_LIMIT),
        **more,
    )


def shaped(shape, dtype):
    return jax.ShapeDtypeStruct(shape, dtype)


def nt_dot(left, right):
    return lax.dot_general(left, right, (((1,), (1,)), ((), ())), preferred_element_type=F32)


def nn_dot(left, right):
    return lax.dot_general(left, right, (((1,), (0,)), ((), ())), preferred_element_type=F32)


def iota(shape, dim):
    return lax.broadcasted_iota(jnp.int32, shape, dim)


def place_of(chip):
    return ((chip & 7) << 3) | (chip >> 3)


def capped(raw_scores):
    return SOFTCAP * jnp.tanh(raw_scores / SOFTCAP)


def pages_kernel(
    me_ref,
    lengths_hbm,
    table_hbm,
    cache_hbm,
    weight_hbm,
    hidden_hbm,
    gain_hbm,
    out_ref,
    held_ref,
    weight_ref,
    hidden_ref,
    gain_ref,
    length_ref,
    position_ref,
    lengths_ref,
    table_ref,
    rows_ref,
    sems,
):
    me = me_ref[0]
    core = me & 1
    group = me >> 3
    loads = [
        (lengths_hbm, lengths_ref),
        (table_hbm, rows_ref),
        (table_hbm, table_ref),
        *[
            (cache_hbm.at[:, e, pl.ds(CHIPS * half, CHIPS)], held_ref.at[:, e, pl.ds(CHIPS * half, CHIPS)])
            for e in range(PER_GROUP)
            for half in range(2)
        ],
        (hidden_hbm, hidden_ref),
        (weight_hbm, weight_ref),
        (gain_hbm, gain_ref),
    ]
    loads = [pltpu.make_async_copy(src, dst, sems.at[i]) for i, (src, dst) in enumerate(loads)]
    for load in loads:
        load.start()
    for load in loads[:3]:
        load.wait()
    row = iota((BATCH, HEAD_DIM // 2), 0)
    spread_length = jnp.zeros((BATCH, HEAD_DIM // 2), F32)
    for r in range(BATCH):
        spread_length = jnp.where(row == r, lengths_ref[r].astype(F32), spread_length)
    length_ref[...] = spread_length
    pages = 2 * CHIPS
    table_row = iota((BATCH, pages), 0)
    lines = []
    for e in range(PER_GROUP):
        chosen_row = jnp.where(table_row == group * PER_GROUP + e, rows_ref[...], 0)
        lines.append(jnp.sum(chosen_row, axis=0, keepdims=True))
    blocks = jnp.where((iota((ROWS, 1), 0) & 1) == 0, lines[0], lines[1]).astype(F32).astype(BF16)
    spread = jnp.where(iota((pages, ROWS * pages), 1) >> 3 == iota((pages, ROWS * pages), 0), 1.0, 0.0)
    inside = iota((ROWS, ROWS * pages), 1) & 7
    position_ref[...] = nn_dot(blocks, spread.astype(BF16)).astype(jnp.int32) * ROWS + inside
    for e in range(PER_GROUP):
        for half in range(2):
            loads[3 + 2 * e + half].wait()

            def place(j, carry):
                block = table_ref[PER_GROUP * group + e, j]
                chip = place_of(block >> 1)
                at = ((block & 1) ^ core) * PAGE_TILES + e * 2
                for kv in range(2):
                    page = held_ref[kv, e, j]
                    out_ref[chip, at + kv * 4] = page[:, :LANES]
                    out_ref[chip, at + kv * 4 + 1] = page[:, LANES:]
                return carry

            lax.fori_loop(CHIPS * half, CHIPS * half + CHIPS, place, 0, unroll=8)
    for load in loads[7:]:
        load.wait()


def qkv_kernel(
    me_ref, hidden_ref, gain_ref, own_ref, other_ref, cos_ref, sin_ref, buf_ref, out_ref, tile_ref, sem
):
    me = me_ref[0]
    first = (me & 1) == 0
    head = me >> 1
    x = hidden_ref[...]
    meansq = jnp.sum(x * x, axis=-1, keepdims=True) * (1.0 / D)
    normed = (x * lax.rsqrt(meansq + EPSILON) * (1.0 + gain_ref[0, 0:1, :])).astype(BF16)
    own = nt_dot(normed, own_ref[0]).astype(BF16).astype(F32)
    other = nt_dot(normed, other_ref[0]).astype(BF16).astype(F32)
    front = jnp.where(first, own, other)
    back = jnp.where(first, other, own)
    cosine = cos_ref[...]
    sine = sin_ref[...]
    turned = head < HEADS + KV_HEADS
    new_front = jnp.where(turned, front * cosine - back * sine, front)
    new_back = jnp.where(turned, back * cosine + front * sine, back)
    whole = jnp.concatenate([new_front, new_back], axis=1)
    rows = [whole[ROWS * u : ROWS * u + ROWS, :].astype(BF16) for u in range(BATCH // ROWS)]
    for chip in range(CHIPS):
        tile_ref[place_of(chip)] = rows[chip * BATCH // (CHIPS * ROWS)]
    copy = pltpu.make_async_copy(tile_ref, out_ref.at[:, BULK_TILES - 1], sem)
    copy.start()
    copy.wait()


def attend_kernel(me_ref, lengths_ref, got_ref, position_ref, cache_ref, out_ref, leaving_ref, sem):
    leave = pltpu.make_async_copy(got_ref.at[:, pl.ds(PAGE_TILES, PAGE_TILES // 2)], leaving_ref, sem)
    leave.start()
    me = me_ref[0]
    group = me >> 3
    slot = me & 7
    rows_at = (group & 3) * PER_GROUP
    n_src = CHIPS * ROWS
    o = iota((32, n_src), 0)
    n = iota((32, n_src), 1)
    e = o & 1
    m = (o >> 1) & 3
    kind = o >> 3
    q_head = slot * 4 + m
    k_head = HEADS + slot * 2 + (m >> 1)
    v_head = k_head + KV_HEADS
    fix_head = HEADS + slot * 2 + (m & 1) + KV_HEADS * (m >> 1)
    chosen = jnp.where(kind == 0, q_head, jnp.where(kind == 1, k_head, jnp.where(kind == 2, v_head, fix_head)))
    pick = jnp.where(n == place_of(chosen) * ROWS + rows_at + e, 1.0, 0.0).astype(BF16)
    source = got_ref[:, BULK_TILES - 1].astype(F32).reshape(n_src, LANES).astype(BF16)
    picked = nn_dot(pick, source)
    q = picked[0:8]
    new_k = picked[8:16]
    new_v = picked[16:24]
    q16 = q.astype(BF16)
    scale = (D / HEADS) ** (-0.5)
    row = iota((ROWS, 1), 0)
    scores = jnp.zeros((ROWS, 8 * 2 * CHIPS), F32)
    for ee in range(PER_GROUP):
        for a in range(2):
            keys = cache_ref[0, ee, :, a * LANES : a * LANES + LANES]
            part = nt_dot(q16, keys)
            scores = jnp.where(((row & 1) == ee) & ((row >> 2) == a), part, scores)
    limit = jnp.where((row & 1) == 0, lengths_ref[group * PER_GROUP], lengths_ref[group * PER_GROUP + 1])
    weights = jnp.where(position_ref[...] < limit, jnp.exp(capped(scores * scale)), 0.0)
    own = jnp.exp(capped(jnp.sum(q * new_k, axis=-1, keepdims=True) * scale))
    denominator = jnp.sum(weights, axis=-1, keepdims=True) + own
    w16 = weights.astype(BF16)
    numerator = own.astype(BF16).astype(F32) * new_v
    for ee in range(PER_GROUP):
        for a in range(2):
            values = cache_ref[1, ee, :, a * LANES : a * LANES + LANES]
            part = nn_dot(w16, values)
            numerator = numerator + jnp.where(((row & 1) == ee) & ((row >> 2) == a), part, 0.0)
    attended = numerator / denominator
    payload = jnp.concatenate([attended, picked[24:32]], axis=0).astype(BF16)
    out_ref[...] = jnp.broadcast_to(payload[None], (CHIPS, 2 * ROWS, LANES))
    leave.wait()


def mixed_half(pieces, weight_ref, core, pick):
    rows = nn_dot(pick, pieces[:, :ROWS].astype(F32).reshape(CHIPS * ROWS, LANES).astype(BF16)).astype(BF16)
    left = jnp.concatenate([rows[BATCH * b : BATCH * b + BATCH] for b in range(16)], axis=1)
    wide = 4 * HEAD_DIM
    right = jnp.concatenate(
        [weight_ref[0, :, pl.ds(pl.multiple_of((2 * y + core) * wide, wide), wide)] for y in range(QUARTERS)],
        axis=1,
    )
    return nt_dot(left, right)


def mix_own_kernel(me_ref, own_ref, weight_ref, got_ref, part_ref, pick_ref, leaving_ref, sem):
    leave = pltpu.make_async_copy(
        got_ref.at[:, pl.ds(PAGE_TILES + PAGE_TILES // 2, PAGE_TILES // 2)], leaving_ref, sem
    )
    leave.start()
    n_src = CHIPS * ROWS
    o = iota((n_src, n_src), 0)
    n = iota((n_src, n_src), 1)
    quarter = o >> 7
    m = (o >> 5) & 3
    group = (o >> 1) & 15
    source_row = place_of(group * QUARTERS + quarter) * ROWS + m * 2 + (o & 1)
    pick_ref[...] = jnp.where(n == source_row, 1.0, 0.0).astype(BF16)
    part_ref[...] = mixed_half(own_ref[...], weight_ref, me_ref[0] & 1, pick_ref[...])
    leave.wait()


def mix_kernel(me_ref, other_ref, weight_ref, part_ref, pick_ref, out_ref):
    me = me_ref[0]
    mixed = part_ref[...] + mixed_half(other_ref[...], weight_ref, 1 - (me & 1), pick_ref[...])
    values = mixed.astype(BF16).astype(F32)
    gap = jnp.zeros((HALF, LANES // 2 - SHARE), F32)
    packed = jnp.concatenate([values[:HALF], gap, values[HALF:], gap], axis=1)
    turned = pltpu.roll(packed, (me * SHARE) % LANES, 1).astype(BF16)
    out_ref[...] = jnp.broadcast_to(turned[None], (CHIPS, HALF, LANES))


def window(low_ref, high_ref, j):
    lane = iota((HALF, LANES), 1)
    far = (lane + LANES // 2) % LANES
    v, off = divmod(j * SHARE, LANES)
    low = low_ref[v]
    high = high_ref[v]
    if off + SHARE > LANES:
        low = jnp.where(lane >= off, low, low_ref[v + 1])
        high = jnp.where(far >= off, high, high_ref[v + 1])
    return jnp.where((lane - off) % LANES < LANES // 2, low, high)


def placed(pieces_ref, parity, v):
    near = iota((HALF, LANES), 1)
    far = (near + LANES // 2) % LANES
    low = high = jnp.zeros((HALF, LANES), F32)
    for j in range((LANES * v) // SHARE, (LANES * v + LANES - 1) // SHARE + 1):
        if j % 2 == parity:
            piece = pieces_ref[place_of(j >> 1)].astype(F32)
            start = j * SHARE - LANES * v
            low = jnp.where((near >= start) & (near < start + SHARE), piece, low)
            high = jnp.where((far >= start) & (far < start + SHARE), piece, high)
    return jnp.concatenate([low, pltpu.roll(high, LANES // 2, 1)], axis=0)


def place_own_kernel(me_ref, own_ref, out_ref):
    for parity in range(2):

        @pl.when((me_ref[0] & 1) == parity)
        def _():
            for v in range(BLOCKS):
                out_ref[v] = placed(own_ref, parity, v)


def ffn_kernel(
    me_ref,
    placed_ref,
    other_ref,
    hidden_ref,
    gain_ref,
    gate_up_ref,
    down_ref,
    keep_ref,
    send_ref,
    stream_ref,
    wide_ref,
    low_ref,
    high_ref,
    ffn_ref,
):
    me = me_ref[0]
    first = (me & 1) == 0
    lane = iota((BATCH, LANES), 1)
    for parity in range(2):

        @pl.when((me & 1) != parity)
        def _():
            for v in range(BLOCKS):
                wide_ref[v] = placed_ref[v] + placed(other_ref, parity, v)

    total = jnp.zeros((BATCH, LANES), F32)
    for v in range(BLOCKS):
        total = total + wide_ref[v] * wide_ref[v]
    scale = lax.rsqrt(jnp.sum(total, axis=-1, keepdims=True) * (1.0 / D) + EPSILON)
    total = jnp.zeros((BATCH, LANES), F32)
    for v in range(BLOCKS):
        cols = slice(LANES * v, LANES * v + LANES)
        block = hidden_ref[:, cols] + wide_ref[v] * scale * (1.0 + gain_ref[0, 1:2, cols])
        wide_ref[v] = block
        total = total + block * block
    scale = lax.rsqrt(jnp.sum(total, axis=-1, keepdims=True) * (1.0 / D) + EPSILON)
    for v in range(BLOCKS):
        cols = slice(LANES * v, LANES * v + LANES)
        ffn_ref[:, cols] = (wide_ref[v] * scale * (1.0 + gain_ref[0, 2:3, cols])).astype(BF16)
    ffn_in = ffn_ref[...]
    gate = nt_dot(ffn_in, gate_up_ref[0, 0])
    up = nt_dot(ffn_in, gate_up_ref[0, 1])
    active = (jax.nn.gelu(gate, approximate=True) * up).astype(BF16)
    for v in range(BLOCKS):
        block = nn_dot(active, down_ref[0, :, LANES * v : LANES * v + LANES])
        low_ref[v] = block[:HALF]
        high_ref[v] = pltpu.roll(block[HALF:], LANES // 2, 1)
    for p in range(CHIPS):
        even = window(low_ref, high_ref, 2 * p)
        odd = window(low_ref, high_ref, 2 * p + 1)
        keep_ref[place_of(p)] = jnp.where(first, even, odd).astype(BF16)
        send_ref[place_of(p)] = jnp.where(first, odd, even).astype(BF16)
    start = me * SHARE
    at = start // LANES
    off = start % LANES
    after = jnp.minimum(at + 1, BLOCKS - 1)
    stream_ref[...] = jnp.where(lane >= off, wide_ref[at], wide_ref[after])


def to_front(x, me):
    off = (me * SHARE) % LANES
    return pltpu.roll(x, (LANES - off) % LANES, 1)


def portion_kernel(me_ref, got_ref, portion_ref, square_ref):
    me = me_ref[0]
    total = jnp.zeros((HALF, LANES), F32)
    for p in range(CHIPS):
        total = total + got_ref[p].astype(F32)
    packed = to_front(total, me)
    mine = jnp.concatenate([packed, pltpu.roll(packed, LANES // 2, 1)], axis=0)
    portion_ref[...] = mine
    lane = iota((BATCH, LANES), 1)
    square = jnp.sum(jnp.where(lane < SHARE, mine * mine, 0.0), axis=-1, keepdims=True)
    line = jnp.sum(jnp.where(iota((BATCH, LANES), 0) == lane, square, 0.0), axis=0, keepdims=True)
    square_ref[...] = jnp.broadcast_to(line[None], (CHIPS, 1, LANES))


def finish_kernel(me_ref, portion_ref, stream_ref, own_ref, other_ref, gain_ref, out_ref):
    me = me_ref[0]
    squares = jnp.sum(own_ref[...] + other_ref[...], axis=0)
    lane = iota((BATCH, LANES), 1)
    column = jnp.sum(jnp.where(iota((BATCH, LANES), 0) == lane, squares, 0.0), axis=-1, keepdims=True)
    scale = lax.rsqrt(column * (1.0 / D) + EPSILON)
    at = (me * SHARE) // LANES
    after = jnp.minimum(at + 1, BLOCKS - 1)
    here = gain_ref[0, 3:4, pl.ds(pl.multiple_of(at * LANES, LANES), LANES)]
    there = gain_ref[0, 3:4, pl.ds(pl.multiple_of(after * LANES, LANES), LANES)]
    gain = jnp.where(lane >= (me * SHARE) % LANES, here, there)
    done = to_front(stream_ref[...], me) + portion_ref[...] * scale * (1.0 + to_front(gain, me))
    out_ref[...] = done[:, :SHARE]


def decode_kernel(
    me_ref, lengths_ref, got_ref, keys_ref, values_ref, own_new_ref, other_new_ref, out_ref
):
    me = me_ref[0]
    core = me & 1

    def place(first_core):
        def body(g, carry):
            for y in range(QUARTERS):
                s = place_of(g * QUARTERS + y)
                for side in range(2):
                    slot = 2 * y + (first_core if side == 0 else 1 - first_core)
                    for kv in range(2):
                        for e in range(PER_GROUP):
                            for h in range(2):
                                cols = slice((2 * slot + h) * LANES, (2 * slot + h) * LANES + LANES)
                                if side == 0:
                                    tile = got_ref[s, kv * 4 + e * 2 + h]
                                else:
                                    tile = (keys_ref, values_ref)[kv][s, e * 2 + h]
                                out_ref[kv, g * PER_GROUP + e, :, cols] = tile
            return carry

        lax.fori_loop(0, GROUPS, body, 0)

    @pl.when(core == 0)
    def _():
        place(0)

    @pl.when(core == 1)
    def _():
        place(1)

    def fresh(r, carry):
        length = lengths_ref[r]

        @pl.when((length >> 3) == me)
        def _():
            g = r >> 1
            e = r & 1
            token = iota((ROWS, LANES), 0) == (length & 7)
            which = iota((2 * ROWS, LANES), 0)
            for y in range(QUARTERS):
                s = place_of(g * QUARTERS + y)
                own = own_new_ref[s].astype(F32)
                other = other_new_ref[s].astype(F32)
                for c in range(2):
                    rows = jnp.where(core == c, own, other)
                    for kv in range(2):
                        for a in range(2):
                            at = ROWS + kv * 4 + a * 2 + e
                            line = jnp.sum(jnp.where(which == at, rows, 0.0), axis=0, keepdims=True)
                            slot = 2 * (2 * y + c) + a
                            cols = slice(slot * LANES, slot * LANES + LANES)
                            old = out_ref[kv, r, :, cols].astype(F32)
                            out_ref[kv, r, :, cols] = jnp.where(token, line, old).astype(BF16)

        return carry

    lax.fori_loop(0, BATCH, fresh, 0)


def core_swap(shard):
    return lax.ppermute(shard, "tp_2", [(0, 1), (1, 0)])


def to_chips(tiles):
    return lax.all_to_all(tiles, XY[::-1], 0, 0, tiled=True)


def pages_call(me, lengths, table, cache, weight, hidden, gains):
    fixed = [pltpu.with_memory_space_constraint(x, pltpu.HBM) for x in (lengths, table, cache, weight, hidden, gains)]
    return call(
        pages_kernel,
        (
            pltpu.VMEM((CHIPS, BULK_TILES, ROWS, LANES), BF16),
            pltpu.VMEM(cache.shape, BF16),
            pltpu.VMEM(weight.shape, BF16),
            pltpu.VMEM(hidden.shape, F32),
            pltpu.VMEM(gains.shape, F32),
            pltpu.VMEM((BATCH, HEAD_DIM // 2), F32),
            pltpu.VMEM((ROWS, ROWS * 2 * CHIPS), jnp.int32),
        ),
        [smem()] + [hbm()] * 6,
        (vmem(),) * 7,
        scratch_shapes=[
            pltpu.SMEM(lengths.shape, jnp.int32),
            pltpu.SMEM(table.shape, jnp.int32),
            pltpu.VMEM(table.shape, jnp.int32),
            pltpu.SemaphoreType.DMA((10,)),
        ],
    )(me, *fixed)


def qkv_call(me, hidden, gains, own, other, cosine, sine, buf):
    return call(
        qkv_kernel,
        shaped(buf.shape, BF16),
        [smem()] + [vmem()] * 6 + [pl.BlockSpec(memory_space=pl.ANY)],
        pl.BlockSpec(memory_space=pl.ANY),
        scratch_shapes=[pltpu.VMEM((CHIPS, ROWS, LANES), BF16), pltpu.SemaphoreType.DMA],
        input_output_aliases={7: 0},
    )(me, hidden, gains, own, other, cosine, sine, buf)


def attend_call(me, lengths, got, position, cache):
    return call(
        attend_kernel,
        (
            pltpu.VMEM((CHIPS, 2 * ROWS, LANES), BF16),
            pltpu.VMEM((CHIPS, PAGE_TILES // 2, ROWS, LANES), BF16),
        ),
        [smem(), smem()] + [vmem()] * 3,
        (vmem(), vmem()),
        scratch_shapes=[pltpu.SemaphoreType.DMA],
    )(me, lengths, got, position, cache)


def mix_own_call(me, own, weight, got):
    return call(
        mix_own_kernel,
        (
            pltpu.VMEM((BATCH, SHARE), F32),
            pltpu.VMEM((CHIPS * ROWS, CHIPS * ROWS), BF16),
            pltpu.VMEM((CHIPS, PAGE_TILES // 2, ROWS, LANES), BF16),
        ),
        [smem()] + [vmem()] * 3,
        (vmem(),) * 3,
        scratch_shapes=[pltpu.SemaphoreType.DMA],
    )(me, own, weight, got)


def mix_call(me, other, weight, part, pick):
    return call(
        mix_kernel, pltpu.VMEM((CHIPS, HALF, LANES), BF16), [smem()] + [vmem()] * 4, vmem()
    )(me, other, weight, part, pick)


def place_own_call(me, own):
    return call(place_own_kernel, pltpu.VMEM((BLOCKS, BATCH, LANES), F32), [smem(), vmem()], vmem())(me, own)


def ffn_call(me, own, other, hidden, gains, gate_up, down):
    wide = shaped((CHIPS, HALF, LANES), BF16)
    return call(
        ffn_kernel,
        (wide, wide, shaped((BATCH, LANES), F32)),
        [smem()] + [vmem()] * 6,
        (vmem(), vmem(), vmem()),
        scratch_shapes=[
            pltpu.VMEM((BLOCKS, BATCH, LANES), F32),
            pltpu.VMEM((BLOCKS, HALF, LANES), F32),
            pltpu.VMEM((BLOCKS, HALF, LANES), F32),
            pltpu.VMEM((BATCH, D), BF16),
        ],
    )(me, own, other, hidden, gains, gate_up, down)


def portion_call(me, got):
    return call(
        portion_kernel,
        (shaped((BATCH, LANES), F32), shaped((CHIPS, 1, LANES), F32)),
        [smem(), vmem()],
        (vmem(), vmem()),
    )(me, got)


def finish_call(me, portion, stream, own, other, gains):
    return call(finish_kernel, shaped((BATCH, SHARE), F32), [smem()] + [vmem()] * 5, vmem())(
        me, portion, stream, own, other, gains
    )


def decode_call(me, lengths, got, other_keys, other_values, own_new, other_new):
    return call(
        decode_kernel, pltpu.VMEM((2, BATCH, ROWS, KV_HEADS * HEAD_DIM), BF16), [smem(), smem()] + [vmem()] * 5, vmem()
    )(me, lengths, got, other_keys, other_values, own_new, other_new)


def rope_tables(spread_length):
    half_dim = HEAD_DIM // 2
    exponent = jnp.arange(half_dim, dtype=F32) * (-2.0 / HEAD_DIM)
    angles = spread_length * jnp.power(jnp.float32(10000.0), exponent)
    return jnp.cos(angles), jnp.sin(angles)


def on_device(
    hidden_in,
    prefill_cache,
    lengths,
    page_table,
    qkv_weight,
    out_weight,
    gate_up_weight,
    down_weight,
    norm_gains,
):
    me = jnp.full((1,), lax.axis_index(TP), jnp.int32)
    other_rows = core_swap(qkv_weight)
    buf, held, own_rows, hidden, gains, spread_length, position = pages_call(
        me, lengths, page_table, prefill_cache[0, 0], qkv_weight, hidden_in, norm_gains
    )
    cosine, sine = rope_tables(spread_length)
    buf = qkv_call(me, hidden, gains, own_rows, other_rows, cosine, sine, buf)
    got = to_chips(buf)
    payload, leaving_keys = attend_call(
        me, lengths, got, position, held.reshape(2, PER_GROUP, -1, 2 * HEAD_DIM)
    )
    own_att = to_chips(payload)
    other_att = core_swap(own_att)
    other_keys = core_swap(leaving_keys)
    part, pick, leaving_values = mix_own_call(me, own_att, out_weight, got)
    payload = mix_call(me, other_att, out_weight, part, pick)
    own_mix = to_chips(payload)
    other_mix = core_swap(own_mix)
    placed_mix = place_own_call(me, own_mix)
    other_values = core_swap(leaving_values)
    keep, send, stream = ffn_call(me, placed_mix, other_mix, hidden, gains, gate_up_weight, down_weight)
    sent = core_swap(send)
    chip = (keep.astype(F32) + sent.astype(F32)).astype(BF16)
    got_branch = to_chips(chip)
    portion, square = portion_call(me, got_branch)
    squares = to_chips(square)
    result = finish_call(me, portion, stream, squares, core_swap(squares), gains)
    decoded = decode_call(me, lengths, got, other_keys, other_values, own_att, other_att)
    return result, decoded[None, None]


def solution(mesh):
    torus = Mesh(mesh.devices.reshape(mesh.shape["grp"], 8, 8, 2), ("grp", "tp_0", "tp_1", "tp_2"))
    return jax.shard_map(
        on_device,
        mesh=torus,
        in_specs=(
            P("grp", None),
            P(TP, None, None, "grp", None, None, None),
            P("grp"),
            P("grp", None),
            P(None, TP, None),
            P(None, TP, None),
            P(None, None, TP, None),
            P(None, TP, None),
            P(),
        ),
        out_specs=(P("grp", TP), P(TP, None, None, "grp", None, None)),
        check_vma=False,
    )
```

```python
import jax
import jax.numpy as jnp
from jax import lax
from jax.experimental import pallas as pl
from jax.experimental.pallas import tpu as pltpu
from jax.sharding import Mesh
from jax.sharding import PartitionSpec as P

D = 4608
HEADS = 32
KV_HEADS = 16
HEAD_DIM = 128
PREFILL_TP = 8
TP = ("tp_0", "tp_1", "tp_2")
XY = ("tp_0", "tp_1")

EPSILON = 1e-06
SOFTCAP = 50.0
LANES = 128
ROWS = 8
BF16 = jnp.bfloat16
F32 = jnp.float32

CHIPS = 64
QUARTERS = PREFILL_TP // 2
GROUPS = CHIPS // QUARTERS
SHARE = D // (2 * CHIPS)
BLOCKS = D // LANES
BATCH = 32
HALF = BATCH // 2
PER_GROUP = 2
PAGE_TILES = 2 * PER_GROUP * 2
BULK_TILES = 2 * PAGE_TILES + 1
VMEM_LIMIT = 24 * 1024 * 1024


def smem():
    return pl.BlockSpec(memory_space=pltpu.SMEM)


def vmem():
    return pl.BlockSpec(memory_space=pltpu.VMEM)


def hbm():
    return pl.BlockSpec(memory_space=pltpu.HBM)


def call(kernel, out_shape, in_specs, out_specs, **more):
    return pl.pallas_call(
        kernel,
        out_shape=out_shape,
        in_specs=in_specs,
        out_specs=out_specs,
        compiler_params=pltpu.CompilerParams(vmem_limit_bytes=VMEM_LIMIT),
        **more,
    )


def shaped(shape, dtype):
    return jax.ShapeDtypeStruct(shape, dtype)


def nt_dot(left, right):
    return lax.dot_general(left, right, (((1,), (1,)), ((), ())), preferred_element_type=F32)


def nn_dot(left, right):
    return lax.dot_general(left, right, (((1,), (0,)), ((), ())), preferred_element_type=F32)


def iota(shape, dim):
    return lax.broadcasted_iota(jnp.int32, shape, dim)


def place_of(chip):
    return ((chip & 7) << 3) | (chip >> 3)


def capped(raw_scores):
    return SOFTCAP * jnp.tanh(raw_scores / SOFTCAP)


def pages_kernel(
    me_ref,
    lengths_hbm,
    table_hbm,
    cache_hbm,
    weight_hbm,
    hidden_hbm,
    gain_hbm,
    out_ref,
    held_ref,
    weight_ref,
    hidden_ref,
    gain_ref,
    length_ref,
    position_ref,
    lengths_ref,
    table_ref,
    rows_ref,
    sems,
):
    me = me_ref[0]
    core = me & 1
    group = me >> 3
    loads = [
        (lengths_hbm, lengths_ref),
        (table_hbm, rows_ref),
        (table_hbm, table_ref),
        *[
            (cache_hbm.at[:, e, pl.ds(CHIPS * half, CHIPS)], held_ref.at[:, e, pl.ds(CHIPS * half, CHIPS)])
            for e in range(PER_GROUP)
            for half in range(2)
        ],
        (hidden_hbm, hidden_ref),
        (weight_hbm, weight_ref),
        (gain_hbm, gain_ref),
    ]
    loads = [pltpu.make_async_copy(src, dst, sems.at[i]) for i, (src, dst) in enumerate(loads)]
    for load in loads:
        load.start()
    for load in loads[:3]:
        load.wait()
    row = iota((BATCH, HEAD_DIM // 2), 0)
    spread_length = jnp.zeros((BATCH, HEAD_DIM // 2), F32)
    for r in range(BATCH):
        spread_length = jnp.where(row == r, lengths_ref[r].astype(F32), spread_length)
    length_ref[...] = spread_length
    pages = 2 * CHIPS
    table_row = iota((BATCH, pages), 0)
    lines = []
    for e in range(PER_GROUP):
        chosen_row = jnp.where(table_row == group * PER_GROUP + e, rows_ref[...], 0)
        lines.append(jnp.sum(chosen_row, axis=0, keepdims=True))
    blocks = jnp.where((iota((ROWS, 1), 0) & 1) == 0, lines[0], lines[1]).astype(F32).astype(BF16)
    spread = jnp.where(iota((pages, ROWS * pages), 1) >> 3 == iota((pages, ROWS * pages), 0), 1.0, 0.0)
    inside = iota((ROWS, ROWS * pages), 1) & 7
    position_ref[...] = nn_dot(blocks, spread.astype(BF16)).astype(jnp.int32) * ROWS + inside
    for e in range(PER_GROUP):
        for half in range(2):
            loads[3 + 2 * e + half].wait()

            def place(j, carry):
                block = table_ref[PER_GROUP * group + e, j]
                chip = place_of(block >> 1)
                at = ((block & 1) ^ core) * PAGE_TILES + e * 2
                for kv in range(2):
                    page = held_ref[kv, e, j]
                    out_ref[chip, at + kv * 4] = page[:, :LANES]
                    out_ref[chip, at + kv * 4 + 1] = page[:, LANES:]
                return carry

            lax.fori_loop(CHIPS * half, CHIPS * half + CHIPS, place, 0, unroll=8)
    for load in loads[7:]:
        load.wait()


def qkv_kernel(
    me_ref, hidden_ref, gain_ref, own_ref, other_ref, cos_ref, sin_ref, buf_ref, out_ref, tile_ref, sem
):
    me = me_ref[0]
    first = (me & 1) == 0
    head = me >> 1
    x = hidden_ref[...]
    meansq = jnp.sum(x * x, axis=-1, keepdims=True) * (1.0 / D)
    normed = (x * lax.rsqrt(meansq + EPSILON) * (1.0 + gain_ref[0, 0:1, :])).astype(BF16)
    own = nt_dot(normed, own_ref[0]).astype(BF16).astype(F32)
    other = nt_dot(normed, other_ref[0]).astype(BF16).astype(F32)
    front = jnp.where(first, own, other)
    back = jnp.where(first, other, own)
    cosine = cos_ref[...]
    sine = sin_ref[...]
    turned = head < HEADS + KV_HEADS
    new_front = jnp.where(turned, front * cosine - back * sine, front)
    new_back = jnp.where(turned, back * cosine + front * sine, back)
    whole = jnp.concatenate([new_front, new_back], axis=1)
    rows = [whole[ROWS * u : ROWS * u + ROWS, :].astype(BF16) for u in range(BATCH // ROWS)]
    for chip in range(CHIPS):
        tile_ref[place_of(chip)] = rows[chip * BATCH // (CHIPS * ROWS)]
    copy = pltpu.make_async_copy(tile_ref, out_ref.at[:, BULK_TILES - 1], sem)
    copy.start()
    copy.wait()


def attend_kernel(me_ref, lengths_ref, got_ref, position_ref, cache_ref, out_ref):
    me = me_ref[0]
    group = me >> 3
    slot = me & 7
    rows_at = (group & 3) * PER_GROUP
    n_src = CHIPS * ROWS
    o = iota((32, n_src), 0)
    n = iota((32, n_src), 1)
    e = o & 1
    m = (o >> 1) & 3
    kind = o >> 3
    q_head = slot * 4 + m
    k_head = HEADS + slot * 2 + (m >> 1)
    v_head = k_head + KV_HEADS
    fix_head = HEADS + slot * 2 + (m & 1) + KV_HEADS * (m >> 1)
    chosen = jnp.where(kind == 0, q_head, jnp.where(kind == 1, k_head, jnp.where(kind == 2, v_head, fix_head)))
    pick = jnp.where(n == place_of(chosen) * ROWS + rows_at + e, 1.0, 0.0).astype(BF16)
    source = got_ref[:, BULK_TILES - 1].astype(F32).reshape(n_src, LANES).astype(BF16)
    picked = nn_dot(pick, source)
    q = picked[0:8]
    new_k = picked[8:16]
    new_v = picked[16:24]
    q16 = q.astype(BF16)
    scale = (D / HEADS) ** (-0.5)
    row = iota((ROWS, 1), 0)
    scores = jnp.zeros((ROWS, 8 * 2 * CHIPS), F32)
    for ee in range(PER_GROUP):
        for a in range(2):
            keys = cache_ref[0, ee, :, a * LANES : a * LANES + LANES]
            part = nt_dot(q16, keys)
            scores = jnp.where(((row & 1) == ee) & ((row >> 2) == a), part, scores)
    limit = jnp.where((row & 1) == 0, lengths_ref[group * PER_GROUP], lengths_ref[group * PER_GROUP + 1])
    weights = jnp.where(position_ref[...] < limit, jnp.exp(capped(scores * scale)), 0.0)
    own = jnp.exp(capped(jnp.sum(q * new_k, axis=-1, keepdims=True) * scale))
    denominator = jnp.sum(weights, axis=-1, keepdims=True) + own
    w16 = weights.astype(BF16)
    numerator = own.astype(BF16).astype(F32) * new_v
    for ee in range(PER_GROUP):
        for a in range(2):
            values = cache_ref[1, ee, :, a * LANES : a * LANES + LANES]
            part = nn_dot(w16, values)
            numerator = numerator + jnp.where(((row & 1) == ee) & ((row >> 2) == a), part, 0.0)
    attended = numerator / denominator
    payload = jnp.concatenate([attended, picked[24:32]], axis=0).astype(BF16)
    out_ref[...] = jnp.broadcast_to(payload[None], (CHIPS, 2 * ROWS, LANES))


def mixed_half(pieces, weight_ref, core, pick):
    rows = nn_dot(pick, pieces[:, :ROWS].astype(F32).reshape(CHIPS * ROWS, LANES).astype(BF16)).astype(BF16)
    left = jnp.concatenate([rows[BATCH * b : BATCH * b + BATCH] for b in range(16)], axis=1)
    wide = 4 * HEAD_DIM
    right = jnp.concatenate(
        [weight_ref[0, :, pl.ds(pl.multiple_of((2 * y + core) * wide, wide), wide)] for y in range(QUARTERS)],
        axis=1,
    )
    return nt_dot(left, right)


def mix_own_kernel(me_ref, own_ref, weight_ref, got_ref, part_ref, pick_ref, leaving_ref, sem):
    leave = pltpu.make_async_copy(
        got_ref.at[:, pl.ds(PAGE_TILES + PAGE_TILES // 2, PAGE_TILES // 2)], leaving_ref, sem
    )
    leave.start()
    n_src = CHIPS * ROWS
    o = iota((n_src, n_src), 0)
    n = iota((n_src, n_src), 1)
    quarter = o >> 7
    m = (o >> 5) & 3
    group = (o >> 1) & 15
    source_row = place_of(group * QUARTERS + quarter) * ROWS + m * 2 + (o & 1)
    pick_ref[...] = jnp.where(n == source_row, 1.0, 0.0).astype(BF16)
    part_ref[...] = mixed_half(own_ref[...], weight_ref, me_ref[0] & 1, pick_ref[...])
    leave.wait()


def mix_kernel(me_ref, other_ref, weight_ref, part_ref, pick_ref, out_ref):
    me = me_ref[0]
    mixed = part_ref[...] + mixed_half(other_ref[...], weight_ref, 1 - (me & 1), pick_ref[...])
    values = mixed.astype(BF16).astype(F32)
    gap = jnp.zeros((HALF, LANES // 2 - SHARE), F32)
    packed = jnp.concatenate([values[:HALF], gap, values[HALF:], gap], axis=1)
    turned = pltpu.roll(packed, (me * SHARE) % LANES, 1).astype(BF16)
    out_ref[...] = jnp.broadcast_to(turned[None], (CHIPS, HALF, LANES))


def window(low_ref, high_ref, j):
    lane = iota((HALF, LANES), 1)
    far = (lane + LANES // 2) % LANES
    v, off = divmod(j * SHARE, LANES)
    low = low_ref[v]
    high = high_ref[v]
    if off + SHARE > LANES:
        low = jnp.where(lane >= off, low, low_ref[v + 1])
        high = jnp.where(far >= off, high, high_ref[v + 1])
    return jnp.where((lane - off) % LANES < LANES // 2, low, high)


def placed(pieces_ref, parity, v):
    near = iota((HALF, LANES), 1)
    far = (near + LANES // 2) % LANES
    low = high = jnp.zeros((HALF, LANES), F32)
    for j in range((LANES * v) // SHARE, (LANES * v + LANES - 1) // SHARE + 1):
        if j % 2 == parity:
            piece = pieces_ref[place_of(j >> 1)].astype(F32)
            start = j * SHARE - LANES * v
            low = jnp.where((near >= start) & (near < start + SHARE), piece, low)
            high = jnp.where((far >= start) & (far < start + SHARE), piece, high)
    return jnp.concatenate([low, pltpu.roll(high, LANES // 2, 1)], axis=0)


def place_own_kernel(me_ref, own_ref, got_ref, out_ref, leaving_ref, sem):
    leave = pltpu.make_async_copy(got_ref.at[:, pl.ds(PAGE_TILES, PAGE_TILES // 2)], leaving_ref, sem)
    leave.start()
    for parity in range(2):

        @pl.when((me_ref[0] & 1) == parity)
        def _():
            for v in range(BLOCKS):
                out_ref[v] = placed(own_ref, parity, v)

    leave.wait()


def ffn_kernel(
    me_ref,
    placed_ref,
    other_ref,
    hidden_ref,
    gain_ref,
    gate_up_ref,
    down_ref,
    keep_ref,
    send_ref,
    stream_ref,
    wide_ref,
    low_ref,
    high_ref,
    ffn_ref,
):
    me = me_ref[0]
    first = (me & 1) == 0
    lane = iota((BATCH, LANES), 1)
    for parity in range(2):

        @pl.when((me & 1) != parity)
        def _():
            for v in range(BLOCKS):
                wide_ref[v] = placed_ref[v] + placed(other_ref, parity, v)

    total = jnp.zeros((BATCH, LANES), F32)
    for v in range(BLOCKS):
        total = total + wide_ref[v] * wide_ref[v]
    scale = lax.rsqrt(jnp.sum(total, axis=-1, keepdims=True) * (1.0 / D) + EPSILON)
    total = jnp.zeros((BATCH, LANES), F32)
    for v in range(BLOCKS):
        cols = slice(LANES * v, LANES * v + LANES)
        block = hidden_ref[:, cols] + wide_ref[v] * scale * (1.0 + gain_ref[0, 1:2, cols])
        wide_ref[v] = block
        total = total + block * block
    scale = lax.rsqrt(jnp.sum(total, axis=-1, keepdims=True) * (1.0 / D) + EPSILON)
    for v in range(BLOCKS):
        cols = slice(LANES * v, LANES * v + LANES)
        ffn_ref[:, cols] = (wide_ref[v] * scale * (1.0 + gain_ref[0, 2:3, cols])).astype(BF16)
    ffn_in = ffn_ref[...]
    gate = nt_dot(ffn_in, gate_up_ref[0, 0])
    up = nt_dot(ffn_in, gate_up_ref[0, 1])
    active = (jax.nn.gelu(gate, approximate=True) * up).astype(BF16)
    for v in range(BLOCKS):
        block = nn_dot(active, down_ref[0, :, LANES * v : LANES * v + LANES])
        low_ref[v] = block[:HALF]
        high_ref[v] = pltpu.roll(block[HALF:], LANES // 2, 1)
    for p in range(CHIPS):
        even = window(low_ref, high_ref, 2 * p)
        odd = window(low_ref, high_ref, 2 * p + 1)
        keep_ref[place_of(p)] = jnp.where(first, even, odd).astype(BF16)
        send_ref[place_of(p)] = jnp.where(first, odd, even).astype(BF16)
    start = me * SHARE
    at = start // LANES
    off = start % LANES
    after = jnp.minimum(at + 1, BLOCKS - 1)
    stream_ref[...] = jnp.where(lane >= off, wide_ref[at], wide_ref[after])


def to_front(x, me):
    off = (me * SHARE) % LANES
    return pltpu.roll(x, (LANES - off) % LANES, 1)


def portion_kernel(me_ref, got_ref, portion_ref, square_ref):
    me = me_ref[0]
    total = jnp.zeros((HALF, LANES), F32)
    for p in range(CHIPS):
        total = total + got_ref[p].astype(F32)
    packed = to_front(total, me)
    mine = jnp.concatenate([packed, pltpu.roll(packed, LANES // 2, 1)], axis=0)
    portion_ref[...] = mine
    lane = iota((BATCH, LANES), 1)
    square = jnp.sum(jnp.where(lane < SHARE, mine * mine, 0.0), axis=-1, keepdims=True)
    line = jnp.sum(jnp.where(iota((BATCH, LANES), 0) == lane, square, 0.0), axis=0, keepdims=True)
    square_ref[...] = jnp.broadcast_to(line[None], (CHIPS, 1, LANES))


def finish_kernel(me_ref, portion_ref, stream_ref, own_ref, other_ref, gain_ref, out_ref):
    me = me_ref[0]
    squares = jnp.sum(own_ref[...] + other_ref[...], axis=0)
    lane = iota((BATCH, LANES), 1)
    column = jnp.sum(jnp.where(iota((BATCH, LANES), 0) == lane, squares, 0.0), axis=-1, keepdims=True)
    scale = lax.rsqrt(column * (1.0 / D) + EPSILON)
    at = (me * SHARE) // LANES
    after = jnp.minimum(at + 1, BLOCKS - 1)
    here = gain_ref[0, 3:4, pl.ds(pl.multiple_of(at * LANES, LANES), LANES)]
    there = gain_ref[0, 3:4, pl.ds(pl.multiple_of(after * LANES, LANES), LANES)]
    gain = jnp.where(lane >= (me * SHARE) % LANES, here, there)
    done = to_front(stream_ref[...], me) + portion_ref[...] * scale * (1.0 + to_front(gain, me))
    out_ref[...] = done[:, :SHARE]


def decode_kernel(
    me_ref, lengths_ref, got_ref, keys_ref, values_ref, own_new_ref, other_new_ref, out_ref
):
    me = me_ref[0]
    core = me & 1

    def place(first_core):
        def body(g, carry):
            for y in range(QUARTERS):
                s = place_of(g * QUARTERS + y)
                for side in range(2):
                    slot = 2 * y + (first_core if side == 0 else 1 - first_core)
                    for kv in range(2):
                        for e in range(PER_GROUP):
                            for h in range(2):
                                cols = slice((2 * slot + h) * LANES, (2 * slot + h) * LANES + LANES)
                                if side == 0:
                                    tile = got_ref[s, kv * 4 + e * 2 + h]
                                else:
                                    tile = (keys_ref, values_ref)[kv][s, e * 2 + h]
                                out_ref[kv, g * PER_GROUP + e, :, cols] = tile
            return carry

        lax.fori_loop(0, GROUPS, body, 0)

    @pl.when(core == 0)
    def _():
        place(0)

    @pl.when(core == 1)
    def _():
        place(1)

    def fresh(r, carry):
        length = lengths_ref[r]

        @pl.when((length >> 3) == me)
        def _():
            g = r >> 1
            e = r & 1
            token = iota((ROWS, LANES), 0) == (length & 7)
            which = iota((2 * ROWS, LANES), 0)
            for y in range(QUARTERS):
                s = place_of(g * QUARTERS + y)
                own = own_new_ref[s].astype(F32)
                other = other_new_ref[s].astype(F32)
                for c in range(2):
                    rows = jnp.where(core == c, own, other)
                    for kv in range(2):
                        for a in range(2):
                            at = ROWS + kv * 4 + a * 2 + e
                            line = jnp.sum(jnp.where(which == at, rows, 0.0), axis=0, keepdims=True)
                            slot = 2 * (2 * y + c) + a
                            cols = slice(slot * LANES, slot * LANES + LANES)
                            old = out_ref[kv, r, :, cols].astype(F32)
                            out_ref[kv, r, :, cols] = jnp.where(token, line, old).astype(BF16)

        return carry

    lax.fori_loop(0, BATCH, fresh, 0)


def core_swap(shard):
    return lax.ppermute(shard, "tp_2", [(0, 1), (1, 0)])


def to_chips(tiles):
    return lax.all_to_all(tiles, XY[::-1], 0, 0, tiled=True)


def pages_call(me, lengths, table, cache, weight, hidden, gains):
    fixed = [pltpu.with_memory_space_constraint(x, pltpu.HBM) for x in (lengths, table, cache, weight, hidden, gains)]
    return call(
        pages_kernel,
        (
            pltpu.VMEM((CHIPS, BULK_TILES, ROWS, LANES), BF16),
            pltpu.VMEM(cache.shape, BF16),
            pltpu.VMEM(weight.shape, BF16),
            pltpu.VMEM(hidden.shape, F32),
            pltpu.VMEM(gains.shape, F32),
            pltpu.VMEM((BATCH, HEAD_DIM // 2), F32),
            pltpu.VMEM((ROWS, ROWS * 2 * CHIPS), jnp.int32),
        ),
        [smem()] + [hbm()] * 6,
        (vmem(),) * 7,
        scratch_shapes=[
            pltpu.SMEM(lengths.shape, jnp.int32),
            pltpu.SMEM(table.shape, jnp.int32),
            pltpu.VMEM(table.shape, jnp.int32),
            pltpu.SemaphoreType.DMA((10,)),
        ],
    )(me, *fixed)


def qkv_call(me, hidden, gains, own, other, cosine, sine, buf):
    return call(
        qkv_kernel,
        shaped(buf.shape, BF16),
        [smem()] + [vmem()] * 6 + [pl.BlockSpec(memory_space=pl.ANY)],
        pl.BlockSpec(memory_space=pl.ANY),
        scratch_shapes=[pltpu.VMEM((CHIPS, ROWS, LANES), BF16), pltpu.SemaphoreType.DMA],
        input_output_aliases={7: 0},
    )(me, hidden, gains, own, other, cosine, sine, buf)


def attend_call(me, lengths, got, position, cache):
    return call(
        attend_kernel,
        pltpu.VMEM((CHIPS, 2 * ROWS, LANES), BF16),
        [smem(), smem()] + [vmem()] * 3,
        vmem(),
    )(me, lengths, got, position, cache)


def mix_own_call(me, own, weight, got):
    return call(
        mix_own_kernel,
        (
            pltpu.VMEM((BATCH, SHARE), F32),
            pltpu.VMEM((CHIPS * ROWS, CHIPS * ROWS), BF16),
            pltpu.VMEM((CHIPS, PAGE_TILES // 2, ROWS, LANES), BF16),
        ),
        [smem()] + [vmem()] * 3,
        (vmem(),) * 3,
        scratch_shapes=[pltpu.SemaphoreType.DMA],
    )(me, own, weight, got)


def mix_call(me, other, weight, part, pick):
    return call(
        mix_kernel, pltpu.VMEM((CHIPS, HALF, LANES), BF16), [smem()] + [vmem()] * 4, vmem()
    )(me, other, weight, part, pick)


def place_own_call(me, own, got):
    return call(
        place_own_kernel,
        (
            pltpu.VMEM((BLOCKS, BATCH, LANES), F32),
            pltpu.VMEM((CHIPS, PAGE_TILES // 2, ROWS, LANES), BF16),
        ),
        [smem(), vmem(), vmem()],
        (vmem(), vmem()),
        scratch_shapes=[pltpu.SemaphoreType.DMA],
    )(me, own, got)


def ffn_call(me, own, other, hidden, gains, gate_up, down):
    wide = shaped((CHIPS, HALF, LANES), BF16)
    return call(
        ffn_kernel,
        (wide, wide, shaped((BATCH, LANES), F32)),
        [smem()] + [vmem()] * 6,
        (vmem(), vmem(), vmem()),
        scratch_shapes=[
            pltpu.VMEM((BLOCKS, BATCH, LANES), F32),
            pltpu.VMEM((BLOCKS, HALF, LANES), F32),
            pltpu.VMEM((BLOCKS, HALF, LANES), F32),
            pltpu.VMEM((BATCH, D), BF16),
        ],
    )(me, own, other, hidden, gains, gate_up, down)


def portion_call(me, got):
    return call(
        portion_kernel,
        (shaped((BATCH, LANES), F32), shaped((CHIPS, 1, LANES), F32)),
        [smem(), vmem()],
        (vmem(), vmem()),
    )(me, got)


def finish_call(me, portion, stream, own, other, gains):
    return call(finish_kernel, shaped((BATCH, SHARE), F32), [smem()] + [vmem()] * 5, vmem())(
        me, portion, stream, own, other, gains
    )


def decode_call(me, lengths, got, other_keys, other_values, own_new, other_new):
    return call(
        decode_kernel,
        pltpu.VMEM((2, BATCH, ROWS, KV_HEADS * HEAD_DIM), BF16),
        [smem(), smem()] + [vmem()] * 5,
        vmem(),
    )(me, lengths, got, other_keys, other_values, own_new, other_new)


def rope_tables(spread_length):
    half_dim = HEAD_DIM // 2
    exponent = jnp.arange(half_dim, dtype=F32) * (-2.0 / HEAD_DIM)
    angles = spread_length * jnp.power(jnp.float32(10000.0), exponent)
    return jnp.cos(angles), jnp.sin(angles)


def on_device(
    hidden_in,
    prefill_cache,
    lengths,
    page_table,
    qkv_weight,
    out_weight,
    gate_up_weight,
    down_weight,
    norm_gains,
):
    me = jnp.full((1,), lax.axis_index(TP), jnp.int32)
    other_rows = core_swap(qkv_weight)
    buf, held, own_rows, hidden, gains, spread_length, position = pages_call(
        me, lengths, page_table, prefill_cache[0, 0], qkv_weight, hidden_in, norm_gains
    )
    cosine, sine = rope_tables(spread_length)
    buf = qkv_call(me, hidden, gains, own_rows, other_rows, cosine, sine, buf)
    got = to_chips(buf)
    payload = attend_call(me, lengths, got, position, held.reshape(2, PER_GROUP, -1, 2 * HEAD_DIM))
    own_att = to_chips(payload)
    other_att = core_swap(own_att)
    part, pick, leaving_values = mix_own_call(me, own_att, out_weight, got)
    payload = mix_call(me, other_att, out_weight, part, pick)
    own_mix = to_chips(payload)
    other_mix = core_swap(own_mix)
    placed_mix, leaving_keys = place_own_call(me, own_mix, got)
    other_keys = core_swap(leaving_keys)
    other_values = core_swap(leaving_values)
    keep, send, stream = ffn_call(me, placed_mix, other_mix, hidden, gains, gate_up_weight, down_weight)
    sent = core_swap(send)
    chip = (keep.astype(F32) + sent.astype(F32)).astype(BF16)
    got_branch = to_chips(chip)
    portion, square = portion_call(me, got_branch)
    squares = to_chips(square)
    result = finish_call(me, portion, stream, squares, core_swap(squares), gains)
    decoded = decode_call(me, lengths, got, other_keys, other_values, own_att, other_att)
    return result, decoded[None, None]


def solution(mesh):
    torus = Mesh(mesh.devices.reshape(mesh.shape["grp"], 8, 8, 2), ("grp", "tp_0", "tp_1", "tp_2"))
    return jax.shard_map(
        on_device,
        mesh=torus,
        in_specs=(
            P("grp", None),
            P(TP, None, None, "grp", None, None, None),
            P("grp"),
            P("grp", None),
            P(None, TP, None),
            P(None, TP, None),
            P(None, None, TP, None),
            P(None, TP, None),
            P(),
        ),
        out_specs=(P("grp", TP), P(TP, None, None, "grp", None, None)),
        check_vma=False,
    )
```

```python
import jax
import jax.numpy as jnp
from jax import lax
from jax.experimental import pallas as pl
from jax.experimental.pallas import tpu as pltpu
from jax.sharding import Mesh
from jax.sharding import PartitionSpec as P

D = 4608
HEADS = 32
KV_HEADS = 16
HEAD_DIM = 128
PREFILL_TP = 8
TP = ("tp_0", "tp_1", "tp_2")
XY = ("tp_0", "tp_1")

EPSILON = 1e-06
SOFTCAP = 50.0
LANES = 128
ROWS = 8
BF16 = jnp.bfloat16
F32 = jnp.float32

CHIPS = 64
QUARTERS = PREFILL_TP // 2
GROUPS = CHIPS // QUARTERS
SHARE = D // (2 * CHIPS)
BLOCKS = D // LANES
BATCH = 32
HALF = BATCH // 2
PER_GROUP = 2
PAGE_TILES = 2 * PER_GROUP * 2
BULK_TILES = 2 * PAGE_TILES + 1
VMEM_LIMIT = 24 * 1024 * 1024


def smem():
    return pl.BlockSpec(memory_space=pltpu.SMEM)


def vmem():
    return pl.BlockSpec(memory_space=pltpu.VMEM)


def hbm():
    return pl.BlockSpec(memory_space=pltpu.HBM)


def call(kernel, out_shape, in_specs, out_specs, **more):
    return pl.pallas_call(
        kernel,
        out_shape=out_shape,
        in_specs=in_specs,
        out_specs=out_specs,
        compiler_params=pltpu.CompilerParams(vmem_limit_bytes=VMEM_LIMIT),
        **more,
    )


def shaped(shape, dtype):
    return jax.ShapeDtypeStruct(shape, dtype)


def nt_dot(left, right):
    return lax.dot_general(left, right, (((1,), (1,)), ((), ())), preferred_element_type=F32)


def nn_dot(left, right):
    return lax.dot_general(left, right, (((1,), (0,)), ((), ())), preferred_element_type=F32)


def iota(shape, dim):
    return lax.broadcasted_iota(jnp.int32, shape, dim)


def place_of(chip):
    return ((chip & 7) << 3) | (chip >> 3)


def capped(raw_scores):
    return SOFTCAP * jnp.tanh(raw_scores / SOFTCAP)


def pages_kernel(
    me_ref,
    lengths_hbm,
    table_hbm,
    cache_hbm,
    weight_hbm,
    hidden_hbm,
    gain_hbm,
    out_ref,
    held_ref,
    weight_ref,
    hidden_ref,
    gain_ref,
    length_ref,
    position_ref,
    lengths_ref,
    table_ref,
    rows_ref,
    sems,
):
    me = me_ref[0]
    core = me & 1
    group = me >> 3
    loads = [
        (lengths_hbm, lengths_ref),
        (table_hbm, rows_ref),
        (table_hbm, table_ref),
        *[
            (cache_hbm.at[:, e, pl.ds(CHIPS * half, CHIPS)], held_ref.at[:, e, pl.ds(CHIPS * half, CHIPS)])
            for e in range(PER_GROUP)
            for half in range(2)
        ],
        (hidden_hbm, hidden_ref),
        (weight_hbm, weight_ref),
        (gain_hbm, gain_ref),
    ]
    loads = [pltpu.make_async_copy(src, dst, sems.at[i]) for i, (src, dst) in enumerate(loads)]
    for load in loads:
        load.start()
    for load in loads[:3]:
        load.wait()
    row = iota((BATCH, HEAD_DIM // 2), 0)
    spread_length = jnp.zeros((BATCH, HEAD_DIM // 2), F32)
    for r in range(BATCH):
        spread_length = jnp.where(row == r, lengths_ref[r].astype(F32), spread_length)
    length_ref[...] = spread_length
    pages = 2 * CHIPS
    table_row = iota((BATCH, pages), 0)
    lines = []
    for e in range(PER_GROUP):
        chosen_row = jnp.where(table_row == group * PER_GROUP + e, rows_ref[...], 0)
        lines.append(jnp.sum(chosen_row, axis=0, keepdims=True))
    blocks = jnp.where((iota((ROWS, 1), 0) & 1) == 0, lines[0], lines[1]).astype(F32).astype(BF16)
    spread = jnp.where(iota((pages, ROWS * pages), 1) >> 3 == iota((pages, ROWS * pages), 0), 1.0, 0.0)
    inside = iota((ROWS, ROWS * pages), 1) & 7
    position_ref[...] = nn_dot(blocks, spread.astype(BF16)).astype(jnp.int32) * ROWS + inside
    for e in range(PER_GROUP):
        for half in range(2):
            loads[3 + 2 * e + half].wait()

            def place(j, carry):
                block = table_ref[PER_GROUP * group + e, j]
                chip = place_of(block >> 1)
                at = ((block & 1) ^ core) * PAGE_TILES + e * 2
                for kv in range(2):
                    page = held_ref[kv, e, j]
                    out_ref[chip, at + kv * 4] = page[:, :LANES]
                    out_ref[chip, at + kv * 4 + 1] = page[:, LANES:]
                return carry

            lax.fori_loop(CHIPS * half, CHIPS * half + CHIPS, place, 0, unroll=8)
    for load in loads[7:]:
        load.wait()


def qkv_kernel(
    me_ref, hidden_ref, gain_ref, own_ref, other_ref, cos_ref, sin_ref, buf_ref, out_ref, tile_ref, sem
):
    me = me_ref[0]
    first = (me & 1) == 0
    head = me >> 1
    x = hidden_ref[...]
    meansq = jnp.sum(x * x, axis=-1, keepdims=True) * (1.0 / D)
    normed = (x * lax.rsqrt(meansq + EPSILON) * (1.0 + gain_ref[0, 0:1, :])).astype(BF16)
    own = nt_dot(normed, own_ref[0]).astype(BF16).astype(F32)
    other = nt_dot(normed, other_ref[0]).astype(BF16).astype(F32)
    front = jnp.where(first, own, other)
    back = jnp.where(first, other, own)
    cosine = cos_ref[...]
    sine = sin_ref[...]
    turned = head < HEADS + KV_HEADS
    new_front = jnp.where(turned, front * cosine - back * sine, front)
    new_back = jnp.where(turned, back * cosine + front * sine, back)
    whole = jnp.concatenate([new_front, new_back], axis=1)
    rows = [whole[ROWS * u : ROWS * u + ROWS, :].astype(BF16) for u in range(BATCH // ROWS)]
    for chip in range(CHIPS):
        tile_ref[place_of(chip)] = rows[chip * BATCH // (CHIPS * ROWS)]
    copy = pltpu.make_async_copy(tile_ref, out_ref.at[:, BULK_TILES - 1], sem)
    copy.start()
    copy.wait()


def attend_kernel(me_ref, lengths_ref, got_ref, position_ref, cache_ref, out_ref):
    me = me_ref[0]
    group = me >> 3
    slot = me & 7
    rows_at = (group & 3) * PER_GROUP
    n_src = CHIPS * ROWS
    o = iota((32, n_src), 0)
    n = iota((32, n_src), 1)
    e = o & 1
    m = (o >> 1) & 3
    kind = o >> 3
    q_head = slot * 4 + m
    k_head = HEADS + slot * 2 + (m >> 1)
    v_head = k_head + KV_HEADS
    fix_head = HEADS + slot * 2 + (m & 1) + KV_HEADS * (m >> 1)
    chosen = jnp.where(kind == 0, q_head, jnp.where(kind == 1, k_head, jnp.where(kind == 2, v_head, fix_head)))
    pick = jnp.where(n == place_of(chosen) * ROWS + rows_at + e, 1.0, 0.0).astype(BF16)
    source = got_ref[:, BULK_TILES - 1].astype(F32).reshape(n_src, LANES).astype(BF16)
    picked = nn_dot(pick, source)
    q = picked[0:8]
    new_k = picked[8:16]
    new_v = picked[16:24]
    scale = (D / HEADS) ** (-0.5)
    row = iota((ROWS, 1), 0)
    both = jnp.concatenate([jnp.where(row < 4, q, 0.0), jnp.where(row < 4, 0.0, q)], axis=1).astype(BF16)
    even = (row & 1) == 0
    scores = jnp.where(even, nt_dot(both, cache_ref[0, 0]), nt_dot(both, cache_ref[0, 1]))
    limit = jnp.where((row & 1) == 0, lengths_ref[group * PER_GROUP], lengths_ref[group * PER_GROUP + 1])
    weights = jnp.where(position_ref[...] < limit, jnp.exp(capped(scores * scale)), 0.0)
    own = jnp.exp(capped(jnp.sum(q * new_k, axis=-1, keepdims=True) * scale))
    denominator = jnp.sum(weights, axis=-1, keepdims=True) + own
    w16 = weights.astype(BF16)
    taken = jnp.where(even, nn_dot(w16, cache_ref[1, 0]), nn_dot(w16, cache_ref[1, 1]))
    taken = jnp.where(row < 4, taken[:, :LANES], taken[:, LANES:])
    numerator = own.astype(BF16).astype(F32) * new_v + taken
    attended = numerator / denominator
    payload = jnp.concatenate([attended, picked[24:32]], axis=0).astype(BF16)
    out_ref[...] = jnp.broadcast_to(payload[None], (CHIPS, 2 * ROWS, LANES))


def mixed_half(pieces, weight_ref, core, pick):
    rows = nn_dot(pick, pieces[:, :ROWS].astype(F32).reshape(CHIPS * ROWS, LANES).astype(BF16)).astype(BF16)
    left = jnp.concatenate([rows[BATCH * b : BATCH * b + BATCH] for b in range(16)], axis=1)
    wide = 4 * HEAD_DIM
    right = jnp.concatenate(
        [weight_ref[0, :, pl.ds(pl.multiple_of((2 * y + core) * wide, wide), wide)] for y in range(QUARTERS)],
        axis=1,
    )
    return nt_dot(left, right)


def mix_own_kernel(me_ref, own_ref, weight_ref, got_ref, part_ref, pick_ref, leaving_ref, sem):
    leave = pltpu.make_async_copy(
        got_ref.at[:, pl.ds(PAGE_TILES + PAGE_TILES // 2, PAGE_TILES // 2)], leaving_ref, sem
    )
    leave.start()
    n_src = CHIPS * ROWS
    o = iota((n_src, n_src), 0)
    n = iota((n_src, n_src), 1)
    quarter = o >> 7
    m = (o >> 5) & 3
    group = (o >> 1) & 15
    source_row = place_of(group * QUARTERS + quarter) * ROWS + m * 2 + (o & 1)
    pick_ref[...] = jnp.where(n == source_row, 1.0, 0.0).astype(BF16)
    part_ref[...] = mixed_half(own_ref[...], weight_ref, me_ref[0] & 1, pick_ref[...])
    leave.wait()


def mix_kernel(me_ref, other_ref, weight_ref, part_ref, pick_ref, out_ref):
    me = me_ref[0]
    mixed = part_ref[...] + mixed_half(other_ref[...], weight_ref, 1 - (me & 1), pick_ref[...])
    values = mixed.astype(BF16).astype(F32)
    gap = jnp.zeros((HALF, LANES // 2 - SHARE), F32)
    packed = jnp.concatenate([values[:HALF], gap, values[HALF:], gap], axis=1)
    turned = pltpu.roll(packed, (me * SHARE) % LANES, 1).astype(BF16)
    out_ref[...] = jnp.broadcast_to(turned[None], (CHIPS, HALF, LANES))


def window(low_ref, high_ref, j):
    lane = iota((HALF, LANES), 1)
    far = (lane + LANES // 2) % LANES
    v, off = divmod(j * SHARE, LANES)
    low = low_ref[v]
    high = high_ref[v]
    if off + SHARE > LANES:
        low = jnp.where(lane >= off, low, low_ref[v + 1])
        high = jnp.where(far >= off, high, high_ref[v + 1])
    return jnp.where((lane - off) % LANES < LANES // 2, low, high)


def placed(pieces_ref, parity, v):
    near = iota((HALF, LANES), 1)
    far = (near + LANES // 2) % LANES
    low = high = jnp.zeros((HALF, LANES), F32)
    for j in range((LANES * v) // SHARE, (LANES * v + LANES - 1) // SHARE + 1):
        if j % 2 == parity:
            piece = pieces_ref[place_of(j >> 1)].astype(F32)
            start = j * SHARE - LANES * v
            low = jnp.where((near >= start) & (near < start + SHARE), piece, low)
            high = jnp.where((far >= start) & (far < start + SHARE), piece, high)
    return jnp.concatenate([low, pltpu.roll(high, LANES // 2, 1)], axis=0)


def place_own_kernel(me_ref, own_ref, got_ref, out_ref, leaving_ref, sem):
    leave = pltpu.make_async_copy(got_ref.at[:, pl.ds(PAGE_TILES, PAGE_TILES // 2)], leaving_ref, sem)
    leave.start()
    for parity in range(2):

        @pl.when((me_ref[0] & 1) == parity)
        def _():
            for v in range(BLOCKS):
                out_ref[v] = placed(own_ref, parity, v)

    leave.wait()


def ffn_kernel(
    me_ref,
    placed_ref,
    other_ref,
    hidden_ref,
    gain_ref,
    gate_up_ref,
    down_ref,
    keep_ref,
    send_ref,
    stream_ref,
    wide_ref,
    low_ref,
    high_ref,
    ffn_ref,
):
    me = me_ref[0]
    first = (me & 1) == 0
    lane = iota((BATCH, LANES), 1)
    for parity in range(2):

        @pl.when((me & 1) != parity)
        def _():
            for v in range(BLOCKS):
                wide_ref[v] = placed_ref[v] + placed(other_ref, parity, v)

    total = jnp.zeros((BATCH, LANES), F32)
    for v in range(BLOCKS):
        total = total + wide_ref[v] * wide_ref[v]
    scale = lax.rsqrt(jnp.sum(total, axis=-1, keepdims=True) * (1.0 / D) + EPSILON)
    total = jnp.zeros((BATCH, LANES), F32)
    for v in range(BLOCKS):
        cols = slice(LANES * v, LANES * v + LANES)
        block = hidden_ref[:, cols] + wide_ref[v] * scale * (1.0 + gain_ref[0, 1:2, cols])
        wide_ref[v] = block
        total = total + block * block
    scale = lax.rsqrt(jnp.sum(total, axis=-1, keepdims=True) * (1.0 / D) + EPSILON)
    for v in range(BLOCKS):
        cols = slice(LANES * v, LANES * v + LANES)
        ffn_ref[:, cols] = (wide_ref[v] * scale * (1.0 + gain_ref[0, 2:3, cols])).astype(BF16)
    ffn_in = ffn_ref[...]
    gate = nt_dot(ffn_in, gate_up_ref[0, 0])
    up = nt_dot(ffn_in, gate_up_ref[0, 1])
    active = (jax.nn.gelu(gate, approximate=True) * up).astype(BF16)
    for w in range(BLOCKS // 2):
        pair = nn_dot(active, down_ref[0, :, 2 * LANES * w : 2 * LANES * w + 2 * LANES])
        for side in range(2):
            block = pair[:, LANES * side : LANES * side + LANES]
            low_ref[2 * w + side] = block[:HALF]
            high_ref[2 * w + side] = pltpu.roll(block[HALF:], LANES // 2, 1)
    for p in range(CHIPS):
        even = window(low_ref, high_ref, 2 * p)
        odd = window(low_ref, high_ref, 2 * p + 1)
        keep_ref[place_of(p)] = jnp.where(first, even, odd).astype(BF16)
        send_ref[place_of(p)] = jnp.where(first, odd, even).astype(BF16)
    start = me * SHARE
    at = start // LANES
    off = start % LANES
    after = jnp.minimum(at + 1, BLOCKS - 1)
    stream_ref[...] = jnp.where(lane >= off, wide_ref[at], wide_ref[after])


def to_front(x, me):
    off = (me * SHARE) % LANES
    return pltpu.roll(x, (LANES - off) % LANES, 1)


def portion_kernel(me_ref, got_ref, portion_ref, square_ref):
    me = me_ref[0]
    total = jnp.zeros((HALF, LANES), F32)
    for p in range(CHIPS):
        total = total + got_ref[p].astype(F32)
    packed = to_front(total, me)
    mine = jnp.concatenate([packed, pltpu.roll(packed, LANES // 2, 1)], axis=0)
    portion_ref[...] = mine
    lane = iota((BATCH, LANES), 1)
    square = jnp.sum(jnp.where(lane < SHARE, mine * mine, 0.0), axis=-1, keepdims=True)
    line = jnp.sum(jnp.where(iota((BATCH, LANES), 0) == lane, square, 0.0), axis=0, keepdims=True)
    square_ref[...] = jnp.broadcast_to(line[None], (CHIPS, 1, LANES))


def finish_kernel(me_ref, portion_ref, stream_ref, own_ref, other_ref, gain_ref, out_ref):
    me = me_ref[0]
    squares = jnp.sum(own_ref[...] + other_ref[...], axis=0)
    lane = iota((BATCH, LANES), 1)
    column = jnp.sum(jnp.where(iota((BATCH, LANES), 0) == lane, squares, 0.0), axis=-1, keepdims=True)
    scale = lax.rsqrt(column * (1.0 / D) + EPSILON)
    at = (me * SHARE) // LANES
    after = jnp.minimum(at + 1, BLOCKS - 1)
    here = gain_ref[0, 3:4, pl.ds(pl.multiple_of(at * LANES, LANES), LANES)]
    there = gain_ref[0, 3:4, pl.ds(pl.multiple_of(after * LANES, LANES), LANES)]
    gain = jnp.where(lane >= (me * SHARE) % LANES, here, there)
    done = to_front(stream_ref[...], me) + portion_ref[...] * scale * (1.0 + to_front(gain, me))
    out_ref[...] = done[:, :SHARE]


def decode_kernel(
    me_ref, lengths_ref, got_ref, keys_ref, values_ref, own_new_ref, other_new_ref, out_ref
):
    me = me_ref[0]
    core = me & 1

    def place(first_core):
        def body(g, carry):
            for y in range(QUARTERS):
                s = place_of(g * QUARTERS + y)
                for side in range(2):
                    slot = 2 * y + (first_core if side == 0 else 1 - first_core)
                    for kv in range(2):
                        for e in range(PER_GROUP):
                            for h in range(2):
                                cols = slice((2 * slot + h) * LANES, (2 * slot + h) * LANES + LANES)
                                if side == 0:
                                    tile = got_ref[s, kv * 4 + e * 2 + h]
                                else:
                                    tile = (keys_ref, values_ref)[kv][s, e * 2 + h]
                                out_ref[kv, g * PER_GROUP + e, :, cols] = tile
            return carry

        lax.fori_loop(0, GROUPS, body, 0)

    @pl.when(core == 0)
    def _():
        place(0)

    @pl.when(core == 1)
    def _():
        place(1)

    def fresh(r, carry):
        length = lengths_ref[r]

        @pl.when((length >> 3) == me)
        def _():
            g = r >> 1
            e = r & 1
            token = iota((ROWS, LANES), 0) == (length & 7)
            which = iota((2 * ROWS, LANES), 0)
            for y in range(QUARTERS):
                s = place_of(g * QUARTERS + y)
                own = own_new_ref[s].astype(F32)
                other = other_new_ref[s].astype(F32)
                for c in range(2):
                    rows = jnp.where(core == c, own, other)
                    for kv in range(2):
                        for a in range(2):
                            at = ROWS + kv * 4 + a * 2 + e
                            line = jnp.sum(jnp.where(which == at, rows, 0.0), axis=0, keepdims=True)
                            slot = 2 * (2 * y + c) + a
                            cols = slice(slot * LANES, slot * LANES + LANES)
                            old = out_ref[kv, r, :, cols].astype(F32)
                            out_ref[kv, r, :, cols] = jnp.where(token, line, old).astype(BF16)

        return carry

    lax.fori_loop(0, BATCH, fresh, 0)


def core_swap(shard):
    return lax.ppermute(shard, "tp_2", [(0, 1), (1, 0)])


def to_chips(tiles):
    return lax.all_to_all(tiles, XY[::-1], 0, 0, tiled=True)


def pages_call(me, lengths, table, cache, weight, hidden, gains):
    fixed = [pltpu.with_memory_space_constraint(x, pltpu.HBM) for x in (lengths, table, cache, weight, hidden, gains)]
    return call(
        pages_kernel,
        (
            pltpu.VMEM((CHIPS, BULK_TILES, ROWS, LANES), BF16),
            pltpu.VMEM(cache.shape, BF16),
            pltpu.VMEM(weight.shape, BF16),
            pltpu.VMEM(hidden.shape, F32),
            pltpu.VMEM(gains.shape, F32),
            pltpu.VMEM((BATCH, HEAD_DIM // 2), F32),
            pltpu.VMEM((ROWS, ROWS * 2 * CHIPS), jnp.int32),
        ),
        [smem()] + [hbm()] * 6,
        (vmem(),) * 7,
        scratch_shapes=[
            pltpu.SMEM(lengths.shape, jnp.int32),
            pltpu.SMEM(table.shape, jnp.int32),
            pltpu.VMEM(table.shape, jnp.int32),
            pltpu.SemaphoreType.DMA((10,)),
        ],
    )(me, *fixed)


def qkv_call(me, hidden, gains, own, other, cosine, sine, buf):
    return call(
        qkv_kernel,
        shaped(buf.shape, BF16),
        [smem()] + [vmem()] * 6 + [pl.BlockSpec(memory_space=pl.ANY)],
        pl.BlockSpec(memory_space=pl.ANY),
        scratch_shapes=[pltpu.VMEM((CHIPS, ROWS, LANES), BF16), pltpu.SemaphoreType.DMA],
        input_output_aliases={7: 0},
    )(me, hidden, gains, own, other, cosine, sine, buf)


def attend_call(me, lengths, got, position, cache):
    return call(
        attend_kernel, pltpu.VMEM((CHIPS, 2 * ROWS, LANES), BF16), [smem(), smem()] + [vmem()] * 3, vmem()
    )(me, lengths, got, position, cache)


def mix_own_call(me, own, weight, got):
    return call(
        mix_own_kernel,
        (
            pltpu.VMEM((BATCH, SHARE), F32),
            pltpu.VMEM((CHIPS * ROWS, CHIPS * ROWS), BF16),
            pltpu.VMEM((CHIPS, PAGE_TILES // 2, ROWS, LANES), BF16),
        ),
        [smem()] + [vmem()] * 3,
        (vmem(),) * 3,
        scratch_shapes=[pltpu.SemaphoreType.DMA],
    )(me, own, weight, got)


def mix_call(me, other, weight, part, pick):
    return call(
        mix_kernel, pltpu.VMEM((CHIPS, HALF, LANES), BF16), [smem()] + [vmem()] * 4, vmem()
    )(me, other, weight, part, pick)


def place_own_call(me, own, got):
    return call(
        place_own_kernel,
        (
            pltpu.VMEM((BLOCKS, BATCH, LANES), F32),
            pltpu.VMEM((CHIPS, PAGE_TILES // 2, ROWS, LANES), BF16),
        ),
        [smem(), vmem(), vmem()],
        (vmem(), vmem()),
        scratch_shapes=[pltpu.SemaphoreType.DMA],
    )(me, own, got)


def ffn_call(me, own, other, hidden, gains, gate_up, down):
    wide = shaped((CHIPS, HALF, LANES), BF16)
    return call(
        ffn_kernel,
        (wide, wide, shaped((BATCH, LANES), F32)),
        [smem()] + [vmem()] * 6,
        (vmem(), vmem(), vmem()),
        scratch_shapes=[
            pltpu.VMEM((BLOCKS, BATCH, LANES), F32),
            pltpu.VMEM((BLOCKS, HALF, LANES), F32),
            pltpu.VMEM((BLOCKS, HALF, LANES), F32),
            pltpu.VMEM((BATCH, D), BF16),
        ],
    )(me, own, other, hidden, gains, gate_up, down)


def portion_call(me, got):
    return call(
        portion_kernel,
        (shaped((BATCH, LANES), F32), shaped((CHIPS, 1, LANES), F32)),
        [smem(), vmem()],
        (vmem(), vmem()),
    )(me, got)


def finish_call(me, portion, stream, own, other, gains):
    return call(finish_kernel, shaped((BATCH, SHARE), F32), [smem()] + [vmem()] * 5, vmem())(
        me, portion, stream, own, other, gains
    )


def decode_call(me, lengths, got, other_keys, other_values, own_new, other_new):
    return call(
        decode_kernel, pltpu.VMEM((2, BATCH, ROWS, KV_HEADS * HEAD_DIM), BF16), [smem(), smem()] + [vmem()] * 5, vmem()
    )(me, lengths, got, other_keys, other_values, own_new, other_new)


def rope_tables(spread_length):
    half_dim = HEAD_DIM // 2
    exponent = jnp.arange(half_dim, dtype=F32) * (-2.0 / HEAD_DIM)
    angles = spread_length * jnp.power(jnp.float32(10000.0), exponent)
    return jnp.cos(angles), jnp.sin(angles)


def on_device(
    hidden_in,
    prefill_cache,
    lengths,
    page_table,
    qkv_weight,
    out_weight,
    gate_up_weight,
    down_weight,
    norm_gains,
):
    me = jnp.full((1,), lax.axis_index(TP), jnp.int32)
    other_rows = core_swap(qkv_weight)
    buf, held, own_rows, hidden, gains, spread_length, position = pages_call(
        me, lengths, page_table, prefill_cache[0, 0], qkv_weight, hidden_in, norm_gains
    )
    cosine, sine = rope_tables(spread_length)
    buf = qkv_call(me, hidden, gains, own_rows, other_rows, cosine, sine, buf)
    got = to_chips(buf)
    payload = attend_call(
        me, lengths, got, position, held.reshape(2, PER_GROUP, -1, 2 * HEAD_DIM)
    )
    own_att = to_chips(payload)
    other_att = core_swap(own_att)
    part, pick, leaving_values = mix_own_call(me, own_att, out_weight, got)
    payload = mix_call(me, other_att, out_weight, part, pick)
    own_mix = to_chips(payload)
    other_mix = core_swap(own_mix)
    placed_mix, leaving_keys = place_own_call(me, own_mix, got)
    other_keys = core_swap(leaving_keys)
    other_values = core_swap(leaving_values)
    keep, send, stream = ffn_call(me, placed_mix, other_mix, hidden, gains, gate_up_weight, down_weight)
    sent = core_swap(send)
    chip = (keep.astype(F32) + sent.astype(F32)).astype(BF16)
    got_branch = to_chips(chip)
    portion, square = portion_call(me, got_branch)
    squares = to_chips(square)
    result = finish_call(me, portion, stream, squares, core_swap(squares), gains)
    decoded = decode_call(me, lengths, got, other_keys, other_values, own_att, other_att)
    return result, decoded[None, None]


def solution(mesh):
    torus = Mesh(mesh.devices.reshape(mesh.shape["grp"], 8, 8, 2), ("grp", "tp_0", "tp_1", "tp_2"))
    return jax.shard_map(
        on_device,
        mesh=torus,
        in_specs=(
            P("grp", None),
            P(TP, None, None, "grp", None, None, None),
            P("grp"),
            P("grp", None),
            P(None, TP, None),
            P(None, TP, None),
            P(None, None, TP, None),
            P(None, TP, None),
            P(),
        ),
        out_specs=(P("grp", TP), P(TP, None, None, "grp", None, None)),
        check_vma=False,
    )
```

```python
import jax
import jax.numpy as jnp
from jax import lax
from jax.experimental import pallas as pl
from jax.experimental.pallas import tpu as pltpu
from jax.sharding import Mesh
from jax.sharding import PartitionSpec as P

D = 4608
HEADS = 32
KV_HEADS = 16
HEAD_DIM = 128
PREFILL_TP = 8
TP = ("tp_0", "tp_1", "tp_2")
XY = ("tp_0", "tp_1")

EPSILON = 1e-06
SOFTCAP = 50.0
LANES = 128
ROWS = 8
BF16 = jnp.bfloat16
F32 = jnp.float32

CHIPS = 64
QUARTERS = PREFILL_TP // 2
GROUPS = CHIPS // QUARTERS
SHARE = D // (2 * CHIPS)
BLOCKS = D // LANES
BATCH = 32
HALF = BATCH // 2
PER_GROUP = 2
PAGE_TILES = 2 * PER_GROUP * 2
BULK_TILES = 2 * PAGE_TILES + 1
VMEM_LIMIT = 24 * 1024 * 1024


def smem():
    return pl.BlockSpec(memory_space=pltpu.SMEM)


def vmem():
    return pl.BlockSpec(memory_space=pltpu.VMEM)


def hbm():
    return pl.BlockSpec(memory_space=pltpu.HBM)


def call(kernel, out_shape, in_specs, out_specs, **more):
    return pl.pallas_call(
        kernel,
        out_shape=out_shape,
        in_specs=in_specs,
        out_specs=out_specs,
        compiler_params=pltpu.CompilerParams(vmem_limit_bytes=VMEM_LIMIT),
        **more,
    )


def shaped(shape, dtype):
    return jax.ShapeDtypeStruct(shape, dtype)


def nt_dot(left, right):
    return lax.dot_general(left, right, (((1,), (1,)), ((), ())), preferred_element_type=F32)


def nn_dot(left, right):
    return lax.dot_general(left, right, (((1,), (0,)), ((), ())), preferred_element_type=F32)


def iota(shape, dim):
    return lax.broadcasted_iota(jnp.int32, shape, dim)


def place_of(chip):
    return ((chip & 7) << 3) | (chip >> 3)


def capped(raw_scores):
    return SOFTCAP * jnp.tanh(raw_scores / SOFTCAP)


def pages_kernel(
    me_ref,
    lengths_hbm,
    table_hbm,
    cache_hbm,
    weight_hbm,
    hidden_hbm,
    gain_hbm,
    out_ref,
    held_ref,
    weight_ref,
    hidden_ref,
    gain_ref,
    length_ref,
    position_ref,
    lengths_ref,
    table_ref,
    rows_ref,
    sems,
):
    me = me_ref[0]
    core = me & 1
    group = me >> 3
    loads = [
        (lengths_hbm, lengths_ref),
        (table_hbm, rows_ref),
        (table_hbm, table_ref),
        *[
            (cache_hbm.at[:, e, pl.ds(CHIPS * half, CHIPS)], held_ref.at[:, e, pl.ds(CHIPS * half, CHIPS)])
            for e in range(PER_GROUP)
            for half in range(2)
        ],
        (hidden_hbm, hidden_ref),
        (weight_hbm, weight_ref),
        (gain_hbm, gain_ref),
    ]
    loads = [pltpu.make_async_copy(src, dst, sems.at[i]) for i, (src, dst) in enumerate(loads)]
    for load in loads:
        load.start()
    for load in loads[:3]:
        load.wait()
    row = iota((BATCH, HEAD_DIM // 2), 0)
    spread_length = jnp.zeros((BATCH, HEAD_DIM // 2), F32)
    for r in range(BATCH):
        spread_length = jnp.where(row == r, lengths_ref[r].astype(F32), spread_length)
    length_ref[...] = spread_length
    pages = 2 * CHIPS
    table_row = iota((BATCH, pages), 0)
    lines = []
    for e in range(PER_GROUP):
        chosen_row = jnp.where(table_row == group * PER_GROUP + e, rows_ref[...], 0)
        lines.append(jnp.sum(chosen_row, axis=0, keepdims=True))
    blocks = jnp.where((iota((ROWS, 1), 0) & 1) == 0, lines[0], lines[1]).astype(F32).astype(BF16)
    spread = jnp.where(iota((pages, ROWS * pages), 1) >> 3 == iota((pages, ROWS * pages), 0), 1.0, 0.0)
    inside = iota((ROWS, ROWS * pages), 1) & 7
    position_ref[...] = nn_dot(blocks, spread.astype(BF16)).astype(jnp.int32) * ROWS + inside
    for e in range(PER_GROUP):
        for half in range(2):
            loads[3 + 2 * e + half].wait()

            def place(j, carry):
                block = table_ref[PER_GROUP * group + e, j]
                chip = place_of(block >> 1)
                at = ((block & 1) ^ core) * PAGE_TILES + e * 2
                for kv in range(2):
                    page = held_ref[kv, e, j]
                    out_ref[chip, at + kv * 4] = page[:, :LANES]
                    out_ref[chip, at + kv * 4 + 1] = page[:, LANES:]
                return carry

            lax.fori_loop(CHIPS * half, CHIPS * half + CHIPS, place, 0, unroll=8)
    for load in loads[7:]:
        load.wait()


def qkv_kernel(
    me_ref, hidden_ref, gain_ref, own_ref, other_ref, cos_ref, sin_ref, buf_ref, out_ref, tile_ref, sem
):
    me = me_ref[0]
    first = (me & 1) == 0
    head = me >> 1
    x = hidden_ref[...]
    meansq = jnp.sum(x * x, axis=-1, keepdims=True) * (1.0 / D)
    normed = (x * lax.rsqrt(meansq + EPSILON) * (1.0 + gain_ref[0, 0:1, :])).astype(BF16)
    own = nt_dot(normed, own_ref[0]).astype(BF16).astype(F32)
    other = nt_dot(normed, other_ref[0]).astype(BF16).astype(F32)
    front = jnp.where(first, own, other)
    back = jnp.where(first, other, own)
    cosine = cos_ref[...]
    sine = sin_ref[...]
    turned = head < HEADS + KV_HEADS
    new_front = jnp.where(turned, front * cosine - back * sine, front)
    new_back = jnp.where(turned, back * cosine + front * sine, back)
    whole = jnp.concatenate([new_front, new_back], axis=1)
    rows = [whole[ROWS * u : ROWS * u + ROWS, :].astype(BF16) for u in range(BATCH // ROWS)]
    for chip in range(CHIPS):
        tile_ref[place_of(chip)] = rows[chip * BATCH // (CHIPS * ROWS)]
    copy = pltpu.make_async_copy(tile_ref, out_ref.at[:, BULK_TILES - 1], sem)
    copy.start()
    copy.wait()


def attend_kernel(me_ref, lengths_ref, got_ref, position_ref, cache_ref, out_ref):
    me = me_ref[0]
    group = me >> 3
    slot = me & 7
    rows_at = (group & 3) * PER_GROUP
    n_src = CHIPS * ROWS
    o = iota((32, n_src), 0)
    n = iota((32, n_src), 1)
    e = o & 1
    m = (o >> 1) & 3
    kind = o >> 3
    q_head = slot * 4 + m
    k_head = HEADS + slot * 2 + (m >> 1)
    v_head = k_head + KV_HEADS
    fix_head = HEADS + slot * 2 + (m & 1) + KV_HEADS * (m >> 1)
    chosen = jnp.where(kind == 0, q_head, jnp.where(kind == 1, k_head, jnp.where(kind == 2, v_head, fix_head)))
    pick = jnp.where(n == place_of(chosen) * ROWS + rows_at + e, 1.0, 0.0).astype(BF16)
    source = got_ref[:, BULK_TILES - 1].astype(F32).reshape(n_src, LANES).astype(BF16)
    picked = nn_dot(pick, source)
    q = picked[0:8]
    new_k = picked[8:16]
    new_v = picked[16:24]
    scale = (D / HEADS) ** (-0.5)
    row = iota((ROWS, 1), 0)
    both = jnp.concatenate([jnp.where(row < 4, q, 0.0), jnp.where(row < 4, 0.0, q)], axis=1).astype(BF16)
    even = (row & 1) == 0
    scores = jnp.where(even, nt_dot(both, cache_ref[0, 0]), nt_dot(both, cache_ref[0, 1]))
    limit = jnp.where((row & 1) == 0, lengths_ref[group * PER_GROUP], lengths_ref[group * PER_GROUP + 1])
    weights = jnp.where(position_ref[...] < limit, jnp.exp(capped(scores * scale)), 0.0)
    own = jnp.exp(capped(jnp.sum(q * new_k, axis=-1, keepdims=True) * scale))
    denominator = jnp.sum(weights, axis=-1, keepdims=True) + own
    w16 = weights.astype(BF16)
    taken = jnp.where(even, nn_dot(w16, cache_ref[1, 0]), nn_dot(w16, cache_ref[1, 1]))
    taken = jnp.where(row < 4, taken[:, :LANES], taken[:, LANES:])
    numerator = own.astype(BF16).astype(F32) * new_v + taken
    attended = numerator / denominator
    payload = jnp.concatenate([attended, picked[24:32]], axis=0).astype(BF16)
    out_ref[...] = jnp.broadcast_to(payload[None], (CHIPS, 2 * ROWS, LANES))


def mixed_half(pieces, weight_ref, core, pick):
    rows = nn_dot(pick, pieces[:, :ROWS].astype(F32).reshape(CHIPS * ROWS, LANES).astype(BF16)).astype(BF16)
    left = jnp.concatenate([rows[BATCH * b : BATCH * b + BATCH] for b in range(16)], axis=1)
    wide = 4 * HEAD_DIM
    right = jnp.concatenate(
        [weight_ref[0, :, pl.ds(pl.multiple_of((2 * y + core) * wide, wide), wide)] for y in range(QUARTERS)],
        axis=1,
    )
    return nt_dot(left, right)


def mix_own_kernel(me_ref, own_ref, weight_ref, got_ref, part_ref, pick_ref, leaving_ref, sem):
    leave = pltpu.make_async_copy(
        got_ref.at[:, pl.ds(PAGE_TILES + PAGE_TILES // 2, PAGE_TILES // 2)], leaving_ref, sem
    )
    leave.start()
    n_src = CHIPS * ROWS
    o = iota((n_src, n_src), 0)
    n = iota((n_src, n_src), 1)
    quarter = o >> 7
    m = (o >> 5) & 3
    group = (o >> 1) & 15
    source_row = place_of(group * QUARTERS + quarter) * ROWS + m * 2 + (o & 1)
    pick_ref[...] = jnp.where(n == source_row, 1.0, 0.0).astype(BF16)
    part_ref[...] = mixed_half(own_ref[...], weight_ref, me_ref[0] & 1, pick_ref[...])
    leave.wait()


def mix_kernel(me_ref, other_ref, weight_ref, part_ref, pick_ref, out_ref):
    me = me_ref[0]
    mixed = part_ref[...] + mixed_half(other_ref[...], weight_ref, 1 - (me & 1), pick_ref[...])
    values = mixed.astype(BF16).astype(F32)
    gap = jnp.zeros((HALF, LANES // 2 - SHARE), F32)
    packed = jnp.concatenate([values[:HALF], gap, values[HALF:], gap], axis=1)
    turned = pltpu.roll(packed, (me * SHARE) % LANES, 1).astype(BF16)
    out_ref[...] = jnp.broadcast_to(turned[None], (CHIPS, HALF, LANES))


def window(low_ref, high_ref, j):
    lane = iota((HALF, LANES), 1)
    far = (lane + LANES // 2) % LANES
    v, off = divmod(j * SHARE, LANES)
    low = low_ref[v]
    high = high_ref[v]
    if off + SHARE > LANES:
        low = jnp.where(lane >= off, low, low_ref[v + 1])
        high = jnp.where(far >= off, high, high_ref[v + 1])
    return jnp.where((lane - off) % LANES < LANES // 2, low, high)


def placed(pieces_ref, parity, v):
    near = iota((HALF, LANES), 1)
    far = (near + LANES // 2) % LANES
    low = high = jnp.zeros((HALF, LANES), F32)
    for j in range((LANES * v) // SHARE, (LANES * v + LANES - 1) // SHARE + 1):
        if j % 2 == parity:
            piece = pieces_ref[place_of(j >> 1)].astype(F32)
            start = j * SHARE - LANES * v
            low = jnp.where((near >= start) & (near < start + SHARE), piece, low)
            high = jnp.where((far >= start) & (far < start + SHARE), piece, high)
    return jnp.concatenate([low, pltpu.roll(high, LANES // 2, 1)], axis=0)


def place_own_kernel(me_ref, own_ref, got_ref, out_ref, leaving_ref, sem):
    leave = pltpu.make_async_copy(got_ref.at[:, pl.ds(PAGE_TILES, PAGE_TILES // 2)], leaving_ref, sem)
    leave.start()
    for parity in range(2):

        @pl.when((me_ref[0] & 1) == parity)
        def _():
            for v in range(BLOCKS):
                out_ref[v] = placed(own_ref, parity, v)

    leave.wait()


def ffn_kernel(
    me_ref,
    placed_ref,
    other_ref,
    hidden_ref,
    gain_ref,
    gate_up_ref,
    down_ref,
    keep_ref,
    send_ref,
    stream_ref,
    wide_ref,
    low_ref,
    high_ref,
    ffn_ref,
):
    me = me_ref[0]
    lane = iota((BATCH, LANES), 1)
    for parity in range(2):

        @pl.when((me & 1) != parity)
        def _():
            for v in range(BLOCKS):
                wide_ref[v] = placed_ref[v] + placed(other_ref, parity, v)

    total = jnp.zeros((BATCH, LANES), F32)
    for v in range(BLOCKS):
        total = total + wide_ref[v] * wide_ref[v]
    scale = lax.rsqrt(jnp.sum(total, axis=-1, keepdims=True) * (1.0 / D) + EPSILON)
    total = jnp.zeros((BATCH, LANES), F32)
    for v in range(BLOCKS):
        cols = slice(LANES * v, LANES * v + LANES)
        block = hidden_ref[:, cols] + wide_ref[v] * scale * (1.0 + gain_ref[0, 1:2, cols])
        wide_ref[v] = block
        total = total + block * block
    scale = lax.rsqrt(jnp.sum(total, axis=-1, keepdims=True) * (1.0 / D) + EPSILON)
    for v in range(BLOCKS):
        cols = slice(LANES * v, LANES * v + LANES)
        ffn_ref[:, cols] = (wide_ref[v] * scale * (1.0 + gain_ref[0, 2:3, cols])).astype(BF16)
    ffn_in = ffn_ref[...]
    gate = nt_dot(ffn_in, gate_up_ref[0, 0])
    up = nt_dot(ffn_in, gate_up_ref[0, 1])
    active = (jax.nn.gelu(gate, approximate=True) * up).astype(BF16)
    for w in range(BLOCKS // 2):
        pair = nn_dot(active, down_ref[0, :, 2 * LANES * w : 2 * LANES * w + 2 * LANES])
        for side in range(2):
            block = pair[:, LANES * side : LANES * side + LANES]
            low_ref[2 * w + side] = block[:HALF]
            high_ref[2 * w + side] = pltpu.roll(block[HALF:], LANES // 2, 1)
    for core in range(2):

        @pl.when((me & 1) == core)
        def _():
            for p in range(CHIPS):
                keep_ref[place_of(p)] = window(low_ref, high_ref, 2 * p + core).astype(BF16)
                send_ref[place_of(p)] = window(low_ref, high_ref, 2 * p + 1 - core).astype(BF16)

    start = me * SHARE
    at = start // LANES
    off = start % LANES
    after = jnp.minimum(at + 1, BLOCKS - 1)
    stream_ref[...] = jnp.where(lane >= off, wide_ref[at], wide_ref[after])


def to_front(x, me):
    off = (me * SHARE) % LANES
    return pltpu.roll(x, (LANES - off) % LANES, 1)


def portion_kernel(me_ref, got_ref, portion_ref, square_ref):
    me = me_ref[0]
    total = jnp.zeros((HALF, LANES), F32)
    for p in range(CHIPS):
        total = total + got_ref[p].astype(F32)
    packed = to_front(total, me)
    mine = jnp.concatenate([packed, pltpu.roll(packed, LANES // 2, 1)], axis=0)
    portion_ref[...] = mine
    lane = iota((BATCH, LANES), 1)
    square = jnp.sum(jnp.where(lane < SHARE, mine * mine, 0.0), axis=-1, keepdims=True)
    line = jnp.sum(jnp.where(iota((BATCH, LANES), 0) == lane, square, 0.0), axis=0, keepdims=True)
    square_ref[...] = jnp.broadcast_to(line[None], (CHIPS, 1, LANES))


def finish_kernel(me_ref, portion_ref, stream_ref, own_ref, other_ref, gain_ref, out_ref):
    me = me_ref[0]
    squares = jnp.sum(own_ref[...] + other_ref[...], axis=0)
    lane = iota((BATCH, LANES), 1)
    column = jnp.sum(jnp.where(iota((BATCH, LANES), 0) == lane, squares, 0.0), axis=-1, keepdims=True)
    scale = lax.rsqrt(column * (1.0 / D) + EPSILON)
    at = (me * SHARE) // LANES
    after = jnp.minimum(at + 1, BLOCKS - 1)
    here = gain_ref[0, 3:4, pl.ds(pl.multiple_of(at * LANES, LANES), LANES)]
    there = gain_ref[0, 3:4, pl.ds(pl.multiple_of(after * LANES, LANES), LANES)]
    gain = jnp.where(lane >= (me * SHARE) % LANES, here, there)
    done = to_front(stream_ref[...], me) + portion_ref[...] * scale * (1.0 + to_front(gain, me))
    out_ref[...] = done[:, :SHARE]


def decode_kernel(
    me_ref, lengths_ref, got_ref, keys_ref, values_ref, own_new_ref, other_new_ref, out_ref
):
    me = me_ref[0]
    core = me & 1

    def place(first_core):
        def body(g, carry):
            for y in range(QUARTERS):
                s = place_of(g * QUARTERS + y)
                for side in range(2):
                    slot = 2 * y + (first_core if side == 0 else 1 - first_core)
                    for kv in range(2):
                        for e in range(PER_GROUP):
                            for h in range(2):
                                cols = slice((2 * slot + h) * LANES, (2 * slot + h) * LANES + LANES)
                                if side == 0:
                                    tile = got_ref[s, kv * 4 + e * 2 + h]
                                else:
                                    tile = (keys_ref, values_ref)[kv][s, e * 2 + h]
                                out_ref[kv, g * PER_GROUP + e, :, cols] = tile
            return carry

        lax.fori_loop(0, GROUPS, body, 0)

    @pl.when(core == 0)
    def _():
        place(0)

    @pl.when(core == 1)
    def _():
        place(1)

    def fresh(r, carry):
        length = lengths_ref[r]

        @pl.when((length >> 3) == me)
        def _():
            g = r >> 1
            e = r & 1
            token = iota((ROWS, LANES), 0) == (length & 7)
            which = iota((2 * ROWS, LANES), 0)
            for y in range(QUARTERS):
                s = place_of(g * QUARTERS + y)
                own = own_new_ref[s].astype(F32)
                other = other_new_ref[s].astype(F32)
                for c in range(2):
                    rows = jnp.where(core == c, own, other)
                    for kv in range(2):
                        for a in range(2):
                            at = ROWS + kv * 4 + a * 2 + e
                            line = jnp.sum(jnp.where(which == at, rows, 0.0), axis=0, keepdims=True)
                            slot = 2 * (2 * y + c) + a
                            cols = slice(slot * LANES, slot * LANES + LANES)
                            old = out_ref[kv, r, :, cols].astype(F32)
                            out_ref[kv, r, :, cols] = jnp.where(token, line, old).astype(BF16)

        return carry

    lax.fori_loop(0, BATCH, fresh, 0)


def core_swap(shard):
    return lax.ppermute(shard, "tp_2", [(0, 1), (1, 0)])


def to_chips(tiles):
    return lax.all_to_all(tiles, XY[::-1], 0, 0, tiled=True)


def pages_call(me, lengths, table, cache, weight, hidden, gains):
    fixed = [pltpu.with_memory_space_constraint(x, pltpu.HBM) for x in (lengths, table, cache, weight, hidden, gains)]
    return call(
        pages_kernel,
        (
            pltpu.VMEM((CHIPS, BULK_TILES, ROWS, LANES), BF16),
            pltpu.VMEM(cache.shape, BF16),
            pltpu.VMEM(weight.shape, BF16),
            pltpu.VMEM(hidden.shape, F32),
            pltpu.VMEM(gains.shape, F32),
            pltpu.VMEM((BATCH, HEAD_DIM // 2), F32),
            pltpu.VMEM((ROWS, ROWS * 2 * CHIPS), jnp.int32),
        ),
        [smem()] + [hbm()] * 6,
        (vmem(),) * 7,
        scratch_shapes=[
            pltpu.SMEM(lengths.shape, jnp.int32),
            pltpu.SMEM(table.shape, jnp.int32),
            pltpu.VMEM(table.shape, jnp.int32),
            pltpu.SemaphoreType.DMA((10,)),
        ],
    )(me, *fixed)


def qkv_call(me, hidden, gains, own, other, cosine, sine, buf):
    return call(
        qkv_kernel,
        shaped(buf.shape, BF16),
        [smem()] + [vmem()] * 6 + [pl.BlockSpec(memory_space=pl.ANY)],
        pl.BlockSpec(memory_space=pl.ANY),
        scratch_shapes=[pltpu.VMEM((CHIPS, ROWS, LANES), BF16), pltpu.SemaphoreType.DMA],
        input_output_aliases={7: 0},
    )(me, hidden, gains, own, other, cosine, sine, buf)


def attend_call(me, lengths, got, position, cache):
    return call(
        attend_kernel, pltpu.VMEM((CHIPS, 2 * ROWS, LANES), BF16), [smem(), smem()] + [vmem()] * 3, vmem()
    )(me, lengths, got, position, cache)


def mix_own_call(me, own, weight, got):
    return call(
        mix_own_kernel,
        (
            pltpu.VMEM((BATCH, SHARE), F32),
            pltpu.VMEM((CHIPS * ROWS, CHIPS * ROWS), BF16),
            pltpu.VMEM((CHIPS, PAGE_TILES // 2, ROWS, LANES), BF16),
        ),
        [smem()] + [vmem()] * 3,
        (vmem(),) * 3,
        scratch_shapes=[pltpu.SemaphoreType.DMA],
    )(me, own, weight, got)


def mix_call(me, other, weight, part, pick):
    return call(
        mix_kernel, pltpu.VMEM((CHIPS, HALF, LANES), BF16), [smem()] + [vmem()] * 4, vmem()
    )(me, other, weight, part, pick)


def place_own_call(me, own, got):
    return call(
        place_own_kernel,
        (
            pltpu.VMEM((BLOCKS, BATCH, LANES), F32),
            pltpu.VMEM((CHIPS, PAGE_TILES // 2, ROWS, LANES), BF16),
        ),
        [smem(), vmem(), vmem()],
        (vmem(), vmem()),
        scratch_shapes=[pltpu.SemaphoreType.DMA],
    )(me, own, got)


def ffn_call(me, own, other, hidden, gains, gate_up, down):
    wide = shaped((CHIPS, HALF, LANES), BF16)
    return call(
        ffn_kernel,
        (wide, wide, shaped((BATCH, LANES), F32)),
        [smem()] + [vmem()] * 6,
        (vmem(), vmem(), vmem()),
        scratch_shapes=[
            pltpu.VMEM((BLOCKS, BATCH, LANES), F32),
            pltpu.VMEM((BLOCKS, HALF, LANES), F32),
            pltpu.VMEM((BLOCKS, HALF, LANES), F32),
            pltpu.VMEM((BATCH, D), BF16),
        ],
    )(me, own, other, hidden, gains, gate_up, down)


def portion_call(me, got):
    return call(
        portion_kernel,
        (shaped((BATCH, LANES), F32), shaped((CHIPS, 1, LANES), F32)),
        [smem(), vmem()],
        (vmem(), vmem()),
    )(me, got)


def finish_call(me, portion, stream, own, other, gains):
    return call(finish_kernel, shaped((BATCH, SHARE), F32), [smem()] + [vmem()] * 5, vmem())(
        me, portion, stream, own, other, gains
    )


def decode_call(me, lengths, got, other_keys, other_values, own_new, other_new):
    return call(
        decode_kernel, pltpu.VMEM((2, BATCH, ROWS, KV_HEADS * HEAD_DIM), BF16), [smem(), smem()] + [vmem()] * 5, vmem()
    )(me, lengths, got, other_keys, other_values, own_new, other_new)


def rope_tables(spread_length):
    half_dim = HEAD_DIM // 2
    exponent = jnp.arange(half_dim, dtype=F32) * (-2.0 / HEAD_DIM)
    angles = spread_length * jnp.power(jnp.float32(10000.0), exponent)
    return jnp.cos(angles), jnp.sin(angles)


def on_device(
    hidden_in,
    prefill_cache,
    lengths,
    page_table,
    qkv_weight,
    out_weight,
    gate_up_weight,
    down_weight,
    norm_gains,
):
    me = jnp.full((1,), lax.axis_index(TP), jnp.int32)
    other_rows = core_swap(qkv_weight)
    buf, held, own_rows, hidden, gains, spread_length, position = pages_call(
        me, lengths, page_table, prefill_cache[0, 0], qkv_weight, hidden_in, norm_gains
    )
    cosine, sine = rope_tables(spread_length)
    buf = qkv_call(me, hidden, gains, own_rows, other_rows, cosine, sine, buf)
    got = to_chips(buf)
    payload = attend_call(
        me, lengths, got, position, held.reshape(2, PER_GROUP, -1, 2 * HEAD_DIM)
    )
    own_att = to_chips(payload)
    other_att = core_swap(own_att)
    part, pick, leaving_values = mix_own_call(me, own_att, out_weight, got)
    payload = mix_call(me, other_att, out_weight, part, pick)
    own_mix = to_chips(payload)
    other_mix = core_swap(own_mix)
    placed_mix, leaving_keys = place_own_call(me, own_mix, got)
    other_keys = core_swap(leaving_keys)
    other_values = core_swap(leaving_values)
    keep, send, stream = ffn_call(me, placed_mix, other_mix, hidden, gains, gate_up_weight, down_weight)
    sent = core_swap(send)
    chip = (keep.astype(F32) + sent.astype(F32)).astype(BF16)
    got_branch = to_chips(chip)
    portion, square = portion_call(me, got_branch)
    squares = to_chips(square)
    result = finish_call(me, portion, stream, squares, core_swap(squares), gains)
    decoded = decode_call(me, lengths, got, other_keys, other_values, own_att, other_att)
    return result, decoded[None, None]


def solution(mesh):
    torus = Mesh(mesh.devices.reshape(mesh.shape["grp"], 8, 8, 2), ("grp", "tp_0", "tp_1", "tp_2"))
    return jax.shard_map(
        on_device,
        mesh=torus,
        in_specs=(
            P("grp", None),
            P(TP, None, None, "grp", None, None, None),
            P("grp"),
            P("grp", None),
            P(None, TP, None),
            P(None, TP, None),
            P(None, None, TP, None),
            P(None, TP, None),
            P(),
        ),
        out_specs=(P("grp", TP), P(TP, None, None, "grp", None, None)),
        check_vma=False,
    )
```
